32 devices in a mesh: rel: 4 (over y, x), tgt: 8 (over z, core).
Axes of the slice: x: 2, y: 2, z: 4, core: 2. Of those that a mesh axis runs over, the one named last changes fastest.
Arguments:
- features: bfloat16 [2048, 768], P('tgt'), may hold values from -6 to 6
- weights: bfloat16 [8, 768, 768], P('rel'), may hold values from -0.109375 to 0.109375
- bias: float32 [768], replicated, may hold values from -3 to 3
- cotangent: bfloat16 [2048, 768], P('tgt'), may hold values from -1.0546875 to 1.0546875
- tile_values: int32 [8, 2048, 8, 128], P('rel', 'tgt'), may hold values from 0 to 3, as said below
- tile_count: int32 [8, 16], P('rel', 'tgt'), may hold values from 1 to 8, as said below
- tile_slot: int32 [8, 16, 8], P('rel', 'tgt'), may hold values from 0 to 7, as said below
- source_blocks: int32 [8, 8], replicated, may hold values from -1 to 1, as said below
Outputs:
- output: bfloat16 [2048, 768], P('tgt', 'rel')
- grad_weights: float32 [8, 768, 768], P('rel', 'tgt')
- grad_features: float32 [16, 128, 768], P('tgt', 'rel')
The draws below stay inside these ranges and needn't reach their ends.
Inputs may be any that keep to these rules, and one draw needn't show every extreme that they name: `tile_values`: entries in tile slots at or beyond the live count are arbitrary and take no part. `tile_count`: every relation has some tile row of targets with all 8 slots live. `tile_slot`: every tile slot, live or not, names an owner for which the target block's entry of source_blocks is not -1. `source_blocks`: entry [t, o] is a block index within owner o's 2 blocks, or -1 where target block t reads nothing from o; entry [t, t] is never -1.
All inputs are finite; a program needn't handle non-finite values.
Results may differ from the reference program's by a relative error of at most 0.01.
Values may be sent and summed in bfloat16 or wider, within the bound.
A program may use at most 64 MiB of HBM per device.

```python
import jax
import jax.numpy as jnp
from jax import lax

D = 768
BLK = 128
SLOTS = 8
REL_DEV = 2
TGT_DEV = 256
REL = 8
OWNERS = 8
NODES = 2048
N_REL = 4


def source_table(key):
    picked = jax.random.randint(jax.random.fold_in(key, 11), (OWNERS, OWNERS), 0, TGT_DEV // BLK)
    keeper = jax.random.randint(jax.random.fold_in(key, 12), (OWNERS, OWNERS), 0, 4) > 0
    diagonal = jnp.eye(OWNERS, dtype=bool)
    return jnp.where(keeper | diagonal, picked, -1).astype(jnp.int32)


def draw_source_blocks(key, part):
    return source_table(key)


def draw_tile_slot(key, part):
    table = source_table(key)
    tile_rows = NODES // BLK
    wanted = jax.random.randint(jax.random.fold_in(key, 13), (REL, tile_rows, SLOTS), 0, OWNERS)
    home = (jnp.arange(tile_rows, dtype=jnp.int32) // (TGT_DEV // BLK))[None, :, None]
    home_full = jnp.broadcast_to(home, (REL, tile_rows, SLOTS))
    listed = table[home_full, wanted] >= 0
    return jnp.where(listed, wanted, home_full).astype(jnp.int32)


def draw_tile_count(key, part):
    tile_rows = NODES // BLK
    hotness = jax.random.randint(jax.random.fold_in(key, 21), (REL, OWNERS), 0, 4) == 0
    hot_rows = jnp.repeat(hotness, TGT_DEV // BLK, axis=1)
    higher = jax.random.randint(jax.random.fold_in(key, 22), (REL, tile_rows), SLOTS // 2 + 1, SLOTS + 1)
    lower_counts = jax.random.randint(jax.random.fold_in(key, 23), (REL, tile_rows), 1, SLOTS // 2 + 1)
    counts = jnp.where(hot_rows, higher, lower_counts)
    forced = jnp.arange(tile_rows)[None, :] == jnp.arange(REL)[:, None] * 5 % tile_rows
    return jnp.where(forced, SLOTS, counts).astype(jnp.int32)


def draw_tile_values(key, part):
    shape_all = (REL, NODES, SLOTS, BLK)
    uniform_ints = jax.random.randint(jax.random.fold_in(key, 31), shape_all, 0, 15)
    levels = jnp.where(uniform_ints < 9, 0, (uniform_ints - 9) // 2 + 1)
    row_alive = jax.random.randint(jax.random.fold_in(key, 33), (REL, NODES, 1, 1), 0, 16) > 0
    return (levels * row_alive).astype(jnp.int32)


def level_of(key, shape, shards, least, largest):
    factor_of, own = 1.0, jax.random.fold_in(key, 6)
    for dim, blocks in shards:
        heights = jnp.exp(jax.random.uniform(jax.random.fold_in(own, dim), (blocks,), jnp.float32, least / len(shards), largest / len(shards)))
        factor_of = factor_of * jnp.repeat(heights, shape[dim] // blocks).reshape([-1 if axis == dim else 1 for axis in range(len(shape))])
    return factor_of


def centred(stream_key, extent, deviation, reach, split=(), kind=jnp.bfloat16):
    drawn = jax.random.normal(stream_key, extent, jnp.float32) * deviation
    if len(split) > 0:
        drawn = level_of(stream_key, extent, split, -0.22, 0.18) * drawn
    return jnp.clip(drawn, min=-reach, max=reach).astype(kind)


def setup_inputs(seed: int = 0) -> dict:
    key_list = jax.random.split(jax.random.key(seed), 9)
    features = centred(key_list[0], (NODES, D), 1.0, 6.0, ((0, 8),))
    weights = centred(key_list[1], (REL, D, D), (4 * D) ** -0.5, 0.109375, ((0, 4),))
    bias = centred(key_list[2], (D,), 0.5, 3.0, (), jnp.float32)
    cotangent = centred(key_list[3], (NODES, D), (8.0 / NODES ** 0.5), 1.0546875, ((0, 8),))
    tile_values = draw_tile_values(jax.random.fold_in(key_list[8], 71), 0)
    tile_count = draw_tile_count(jax.random.fold_in(key_list[8], 71), 0)
    tile_slot = draw_tile_slot(jax.random.fold_in(key_list[8], 71), 0)
    source_blocks = draw_source_blocks(jax.random.fold_in(key_list[8], 71), 0)
    return {"features": features, "weights": weights, "bias": bias, "cotangent": cotangent, "tile_values": tile_values, "tile_count": tile_count, "tile_slot": tile_slot, "source_blocks": source_blocks}


HIGHEST = lax.Precision.HIGHEST

def silu_pair(values):
    sigmoid = jax.nn.sigmoid(values)
    return (values * sigmoid, sigmoid * (1.0 + values * (1.0 - sigmoid)))

def reference(features, weights, bias, cotangent, tile_values, tile_count, tile_slot, source_blocks):
    sections = TGT_DEV // BLK
    own_blocks = features.reshape(OWNERS, sections, BLK, D)
    weights_wide = weights.astype(jnp.float32)
    owner_ids = jnp.arange(OWNERS, dtype=jnp.int32)
    section_ids = jnp.arange(sections, dtype=jnp.int32)
    slot_ids = jnp.arange(SLOTS, dtype=jnp.int32)

    def one_block(state_pair, target):
        weight_sum, feature_sum = state_pair
        values = lax.dynamic_slice_in_dim(tile_values, target * TGT_DEV, TGT_DEV, 1)
        counts = lax.dynamic_slice_in_dim(tile_count, target * sections, sections, 1)
        slots_here = lax.dynamic_slice_in_dim(tile_slot, target * sections, sections, 1)
        requested = lax.dynamic_index_in_dim(source_blocks, target, 0, keepdims=False)
        cot_rows = lax.dynamic_slice_in_dim(cotangent, target * TGT_DEV, TGT_DEV, 0)
        chosen = own_blocks[owner_ids, jnp.maximum(requested, 0)]
        fetched = jnp.where((requested >= 0)[:, None, None], chosen, jnp.zeros_like(chosen))
        live_mask = (slot_ids[None, None, :] < counts[:, :, None]).astype(jnp.int32)
        counted = values.reshape(REL, sections, BLK, SLOTS, BLK) * live_mask[:, :, None, :, None]
        degree = lax.optimization_barrier(jnp.sum(counted, axis=(3, 4))).astype(jnp.float32)
        adjacency = (counted.astype(jnp.float32) / jnp.sqrt(jnp.maximum(degree, 1.0))[..., None, None]).astype(jnp.bfloat16)
        adj_wide = adjacency.astype(jnp.float32)
        sources = fetched[slots_here].astype(jnp.float32)
        messages = jnp.einsum('rqisc,rqscd->rqid', adj_wide, sources, precision=HIGHEST).astype(jnp.bfloat16)
        msg_wide = messages.reshape(REL, TGT_DEV, D).astype(jnp.float32)
        preact = jnp.einsum('rnd,rde->ne', msg_wide, weights_wide, precision=HIGHEST) + bias
        activated, derivative = silu_pair(preact)
        grad_pre = (cot_rows.astype(jnp.float32) * derivative).astype(jnp.bfloat16)
        grad_wide = grad_pre.astype(jnp.float32)
        grad_messages = jnp.einsum('ne,rde->rnd', grad_wide, weights_wide, precision=HIGHEST).astype(jnp.bfloat16)
        weight_sum = weight_sum + jnp.einsum('rnd,ne->rde', msg_wide, grad_wide, precision=HIGHEST)
        grads_blocked = grad_messages.astype(jnp.float32).reshape(REL, sections, BLK, D)
        contrib = jnp.einsum('rqisc,rqid->rqscd', adj_wide, grads_blocked, precision=HIGHEST)
        selector = (slots_here[..., None] == owner_ids).astype(jnp.float32)
        grouped = jnp.einsum('grqso,grqscd->gocd', selector.reshape(N_REL, REL_DEV, sections, SLOTS, OWNERS), contrib.reshape(N_REL, REL_DEV, sections, SLOTS, BLK, D), precision=HIGHEST)
        rounded = lax.optimization_barrier(grouped.astype(jnp.bfloat16)).astype(jnp.float32)
        per_owner = lax.optimization_barrier(jnp.sum(rounded, axis=0))
        placed = (requested[:, None] == section_ids[None, :]).astype(jnp.float32)
        feature_sum = feature_sum + jnp.einsum('ok,ocd->okcd', placed, per_owner, precision=HIGHEST)
        return ((weight_sum, feature_sum), activated.astype(jnp.bfloat16))
    initial = (jnp.zeros((REL, D, D), jnp.float32), jnp.zeros((OWNERS, sections, BLK, D), jnp.float32))
    finals, outputs = lax.scan(one_block, initial, jnp.arange(OWNERS, dtype=jnp.int32))
    weight_sum, feature_sum = finals
    return (outputs.reshape(NODES, D), weight_sum, feature_sum.reshape(NODES // BLK, BLK, D))
```

```python
import functools

import jax
import jax.numpy as jnp
from jax import lax
from jax.experimental import pallas as pl
from jax.experimental.pallas import tpu as pltpu
from jax.sharding import PartitionSpec as P

MESH = pl.DeviceIdType.MESH
F32 = jnp.float32
BF16 = jnp.bfloat16


def aligned(start, size, multiple):
    return pl.ds(pl.multiple_of(start, multiple), size)


def is_one(condition):
    return condition.astype(jnp.int32).astype(F32)


def pack(value, first, width):
    half = value.shape[0] // 2
    return jnp.concatenate(
        [value[:half, first : first + width], value[half:, first : first + width]], axis=1
    )


def drain(view, semaphore):
    pltpu.make_async_copy(view, view, semaphore).wait()


def kernel(
    n, groups,
    table, counts, slots,
    feat, cot, bias, values_hbm, weights_hbm,
    out_hbm, grad_w_hbm, grad_f_hbm,
    out, grad_w, grad_f, out_sem,
    weights, values, gathered, partner_staged, masked, masked_t, fetched, adj, scale, msg, msg_t, wg_own, adj_t, pre,
    pre_send, pre_recv, cot_own, active, bias_own, gp_all, gp, gm,
    part, part_recv, part_sum, part_back,
    wg_pair, wg_pair_recv, up_send, up_recv, down_send, down_recv,
    load_sem, pair_sem, sent_sem, spread_sem, back_sem,
    a_recv, b_recv, p_recv, g_recv, d_recv, w_recv, u_recv, v_recv,
):
    me = lax.axis_index("tgt")
    grp = lax.axis_index("rel")
    sections, _, quarter, width = feat.shape
    blk = quarter * groups
    rows = sections * blk
    relations = weights.shape[0]
    slot_total = slots.shape[2]
    share = width // groups
    chips = n // 2
    chip, core = me // 2, lax.rem(me, 2)

    def tgt(j):
        return lax.rem(chip + j // 2, chips) * 2 + lax.rem(core + lax.rem(j, 2), 2)

    below, above_me = chip, chips - 1 - chip
    both = jnp.minimum(below, above_me)

    def near(j):
        k = j // 2 - 1
        two_sided = jnp.where(lax.rem(k, 2) == 0, chip + k // 2 + 1, chip - k // 2 - 1)
        distance = k - both + 1
        one_sided = jnp.where(above_me > below, chip + distance, chip - distance)
        return jnp.where(k < 2 * both, two_sided, one_sided) * 2 + lax.rem(core + lax.rem(j, 2), 2)

    partner = chip * 2 + 1 - core
    row, column = grp // 2, lax.rem(grp, 2)
    beside = row * 2 + 1 - column
    above = (1 - row) * 2 + column

    square = groups == 4

    def rel(i):
        if square:
            return (grp, beside, above, (1 - row) * 2 + 1 - column)[i]
        return lax.rem(grp + i, groups)

    load_w = pltpu.make_async_copy(weights_hbm, weights, load_sem.at[0])
    load_v = pltpu.make_async_copy(values_hbm, values, load_sem.at[1])
    load_v.start()
    load_w.start()

    barrier = pltpu.get_barrier_semaphore()

    @pl.loop(1, n)
    def _(j):
        pl.semaphore_signal(barrier, inc=1, device_id=(grp, tgt(j)), device_id_type=MESH)

    for i in range(1, groups):
        pl.semaphore_signal(barrier, inc=1, device_id=(rel(i), me), device_id_type=MESH)

    def whole_block(t):
        total = jnp.zeros((blk, width), F32)
        for k in range(sections):
            total = total + feat[k].reshape(blk, width).astype(F32) * is_one(table[t, me] == k)
        return total.astype(BF16)

    fetched[aligned(me * blk, blk, blk), :] = whole_block(me)
    partner_staged[...] = whole_block(partner)
    pl.semaphore_wait(barrier, n - 1 + groups - 1)

    cut = width // 2

    def columns(h):
        return aligned(h * cut, cut, 128)

    def climb_rows(o, h, source):
        return pltpu.make_async_remote_copy(
            src_ref=source, dst_ref=gathered.at[o, :, :, columns(h)],
            send_sem=sent_sem.at[0], recv_sem=a_recv.at[o, h],
            device_id=(grp, jnp.minimum(chip + 1, chips - 1) * 2 + core), device_id_type=MESH,
        )

    def descend_rows(o, h, source):
        return pltpu.make_async_remote_copy(
            src_ref=source, dst_ref=gathered.at[o, :, :, columns(h)],
            send_sem=sent_sem.at[0], recv_sem=a_recv.at[o, h],
            device_id=(grp, jnp.maximum(chip - 1, 0) * 2 + core), device_id_type=MESH,
        )

    def across_rows(o, h):
        return pltpu.make_async_remote_copy(
            src_ref=gathered.at[o, :, :, columns(h)], dst_ref=gathered.at[o, :, :, columns(h)],
            send_sem=sent_sem.at[0], recv_sem=a_recv.at[o, h],
            device_id=(grp, partner), device_id_type=MESH,
        )

    fetch_pair = pltpu.make_async_remote_copy(
        src_ref=partner_staged, dst_ref=fetched.at[aligned(me * blk, blk, blk), :],
        send_sem=pair_sem.at[0], recv_sem=pair_sem.at[1],
        device_id=(grp, partner), device_id_type=MESH,
    )

    for h in range(2):
        @pl.when(chip < chips - 1)
        def _():
            climb_rows(me, h, feat.at[:, grp, :, columns(h)]).start()

        @pl.when(chip > 0)
        def _():
            descend_rows(me, h, feat.at[:, grp, :, columns(h)]).start()

    fetch_pair.start()

    sent = range(4) if square else range(groups - 1)

    def spread(j, h, way):
        if square:
            size = quarter if way < 2 else quarter // 2
            source = (grp, grp, beside, above)[way]
            extra = quarter // 2 if way == 3 else 0
            peer = (beside, above, above, beside)[way]
        else:
            size, source, extra, peer = quarter, grp, 0, rel(way + 1)
        rows_at = aligned(near(j) * blk + source * quarter + extra, size, size)
        return pltpu.make_async_remote_copy(
            src_ref=fetched.at[rows_at, columns(h)], dst_ref=fetched.at[rows_at, columns(h)],
            send_sem=sent_sem.at[1],
            recv_sem=b_recv.at[j, h, way] if square and way < 2 else spread_sem,
            device_id=(peer, me), device_id_type=MESH,
        )

    first_hop = sent[:2] if square else sent

    def event(e):
        inner = lax.rem(e, 4)
        paired = e < 4 * both
        k = jnp.where(paired, e // 4 * 2 + 1 + lax.rem(inner, 2), e // 2 + 1)
        return k, jnp.where(paired, inner // 2, lax.rem(e, 2))

    def pass_on(e, side):
        k, h = event(e)
        j = 2 * k + side
        if not square:
            return
        spread(j, h, 0).wait_recv()
        spread(j, h, 2).start()
        spread(j, h, 1).wait_recv()
        spread(j, h, 3).start()

    def placed(j, h):
        o = near(j)
        total = jnp.zeros((quarter, cut), F32)
        for k in range(sections):
            total = total + gathered[o, k, :, columns(h)].astype(F32) * is_one(table[me, o] == k)
        fetched[aligned(o * blk + grp * quarter, quarter, quarter), columns(h)] = total.astype(BF16)
        for way in first_hop:
            spread(j, h, way).start()

    def arrive(e):
        k, h = event(e)
        o = near(2 * k)
        across_rows(o, h).wait_recv()

        @pl.when((o < me) & (chip < chips - 1))
        def _():
            climb_rows(o, h, gathered.at[o, :, :, columns(h)]).start()

        @pl.when((o > me) & (chip > 0))
        def _():
            descend_rows(o, h, gathered.at[o, :, :, columns(h)]).start()

        across_rows(o, h).start()
        placed(2 * k, h)

    def arrive_across(e):
        k, h = event(e)
        across_rows(near(2 * k + 1), h).wait_recv()
        placed(2 * k + 1, h)

    load_v.wait()

    def adjacency(b):
        r, q = b // sections, lax.rem(b, sections)
        count = counts[r, q]
        total = jnp.zeros((blk, blk), F32)
        for s in range(slot_total):
            start = (q * blk * slot_total) + s
            tile = values[r, pl.ds(start, blk, stride=slot_total), :].astype(F32) * is_one(s < count)
            masked[s] = tile.astype(BF16)
            masked_t[s] = tile.T.astype(BF16)
            total = total + tile
        degree = jnp.sum(total, axis=1, keepdims=True)
        root = 1.0 / jnp.sqrt(jnp.maximum(degree, 1.0))
        scale[aligned(b * blk, blk, blk), :] = jnp.broadcast_to(root, (blk, 128))

        @pl.loop(0, n)
        def _(o):
            entry = jnp.zeros((blk, blk), BF16)
            entry_t = jnp.zeros((blk, blk), BF16)
            for s in range(slot_total):
                here = jnp.full((blk, blk), is_one(slots[r, q, s] == o), F32).astype(BF16)
                entry = entry + masked[s] * here
                entry_t = entry_t + masked_t[s] * here
            adj[aligned(b * blk, blk, blk), aligned(o * blk, blk, blk)] = entry
            adj_t[aligned(o * blk, blk, blk), aligned(b * blk, blk, blk)] = entry_t

    blocks = relations * sections

    @pl.loop(0, blocks // 2)
    def _(b):
        adjacency(b)

    events = 2 * (chips - 1)
    arrive(0)
    arrive(1)

    @pl.loop(0, blocks // 2)
    def _(b):
        adjacency(blocks // 2 + b)
        arrive_across(b)
        arrive(2 + b)

    @pl.loop(blocks // 2 + 2, events)
    def _(e):
        arrive(e)
        arrive_across(e - 2)

    pass_on(0, 0)
    arrive_across(events - 2)
    pass_on(0, 1)
    arrive_across(events - 1)

    @pl.loop(1, events)
    def _(e):
        pass_on(e, 0)
        pass_on(e, 1)

    load_w.wait()
    fetch_pair.wait_recv()

    late = n - 2 if square else (n - 2) * (groups - 1)
    drain(fetched.at[: late * quarter, :], spread_sem)

    tile_width = 256

    @pl.loop(0, width // tile_width)
    def _(c):
        at = aligned(c * tile_width, tile_width, tile_width)
        acc = jnp.dot(adj[...], fetched[:, at], preferred_element_type=F32)
        msg[:, at] = (acc * scale[:, 0:1]).astype(BF16)

    @pl.loop(0, width // tile_width)
    def _(c):
        at = aligned(c * tile_width, tile_width, tile_width)
        total = None
        for r in range(relations):
            part_r = jnp.dot(
                msg[r * rows : (r + 1) * rows, :], weights[r, :, at], preferred_element_type=F32
            )
            total = part_r if total is None else total + part_r
        pre[:, at] = total

    whole = pre[...]
    for k in range(groups):
        pre_send[k] = pack(whole, k * share, share).astype(BF16)

    piece_rows = rows // 4

    def reduce_pre(i, p):
        at = slice(p * piece_rows, (p + 1) * piece_rows)
        return pltpu.make_async_remote_copy(
            src_ref=pre_send.at[rel(i), at, :], dst_ref=pre_recv.at[i, at, :],
            send_sem=sent_sem.at[2], recv_sem=p_recv.at[p],
            device_id=(rel(i), me), device_id_type=MESH,
        )

    for p in range(2):
        for i in range(1, groups):
            reduce_pre(i, p).start()

    for r in range(relations):
        turned = msg[r * rows : (r + 1) * rows, :].astype(F32).T
        sliced = turned.reshape(n, width // n, rows)
        for c in range(2):
            msg_t[r, c] = jnp.concatenate([sliced[z * 2 + c] for z in range(chips)], axis=0).astype(BF16)

    for k in range(groups):
        @pl.when(grp == k)
        def _():
            cot_own[...] = pack(cot[...].astype(F32), k * share, share)
            piece = bias[...].reshape(1, width)[:, k * share : (k + 1) * share]
            bias_own[...] = jnp.concatenate([piece, piece], axis=1)

    def gather_gp(i, p):
        at = slice(p * piece_rows, (p + 1) * piece_rows)
        return pltpu.make_async_remote_copy(
            src_ref=gp_all.at[grp, at, :], dst_ref=gp_all.at[grp, at, :],
            send_sem=sent_sem.at[3], recv_sem=g_recv.at[p],
            device_id=(rel(i), me), device_id_type=MESH,
        )

    for p in range(2):
        at = slice(p * piece_rows, (p + 1) * piece_rows)
        total = pre_send[grp, at, :].astype(F32)
        drain(pre_recv.at[1:groups, at, :], p_recv.at[p])
        for i in range(1, groups):
            total = total + pre_recv[i, at, :].astype(F32)
        pre_act = total + bias_own[...]
        sigmoid = jax.nn.sigmoid(pre_act)
        derivative = sigmoid * (1.0 + pre_act * (1.0 - sigmoid))
        gp_all[grp, at, :] = (cot_own[at, :] * derivative).astype(BF16)
        for i in range(1, groups):
            gather_gp(i, p).start()
        active[at, :] = pre_act * sigmoid

    upright = active[...].T
    for h in range(2):
        out[:, h * (rows // 2) : (h + 1) * (rows // 2)] = upright[h * share : (h + 1) * share].astype(BF16)

    save_out = pltpu.make_async_copy(out, out_hbm, out_sem.at[0])
    save_w = pltpu.make_async_copy(grad_w, grad_w_hbm, out_sem.at[1])
    save_f = pltpu.make_async_copy(grad_f, grad_f_hbm, out_sem.at[2])
    save_out.start()

    for p in range(2):
        drain(pre_recv.at[1:groups, p * piece_rows : (p + 1) * piece_rows, :], g_recv.at[p])
    half = rows // 2
    for h in range(2):
        gp[h * half : (h + 1) * half, :] = jnp.concatenate(
            [gp_all[k][:, h * share : (h + 1) * share].astype(F32) for k in range(groups)], axis=1
        ).astype(BF16)

    def weight_chunks(r, c):
        product = jnp.dot(msg_t[r, c], gp[...], preferred_element_type=F32)
        return product.reshape(chips, width // n, width)

    def pair(z):
        return pltpu.make_async_remote_copy(
            src_ref=wg_pair.at[z], dst_ref=wg_pair_recv.at[z],
            send_sem=sent_sem.at[4], recv_sem=w_recv.at[z],
            device_id=(grp, partner), device_id_type=MESH,
        )

    for r in range(relations):
        wg_pair[:, r] = weight_chunks(r, 1 - core).astype(BF16)

    upper = chip >= chips // 2

    def order(i):
        return jnp.where(upper, i, chips - 1 - i)

    @pl.loop(0, chips)
    def _(i):
        pair(order(i)).start()

    for r in range(relations):
        wg_own[:, r] = weight_chunks(r, core)

    @pl.loop(0, width // tile_width)
    def _(c):
        at = aligned(c * tile_width, tile_width, tile_width)
        for r in range(relations):
            rows_r = slice(r * rows, (r + 1) * rows)
            grads = lax.dot_general(
                gp[...], weights[r, at, :],
                (((1,), (1,)), ((), ())), preferred_element_type=F32,
            )
            gm[rows_r, at] = (grads * scale[rows_r, 0:1]).astype(BF16)

    def climb(d, r):
        return pltpu.make_async_remote_copy(
            src_ref=up_send.at[d, r], dst_ref=up_recv.at[d, r],
            send_sem=sent_sem.at[5], recv_sem=u_recv.at[d, r],
            device_id=(grp, jnp.minimum(chip + 1, chips - 1) * 2 + core), device_id_type=MESH,
        )

    def descend(d, r):
        return pltpu.make_async_remote_copy(
            src_ref=down_send.at[d, r], dst_ref=down_recv.at[d, r],
            send_sem=sent_sem.at[5], recv_sem=v_recv.at[d, r],
            device_id=(grp, jnp.maximum(chip - 1, 0) * 2 + core), device_id_type=MESH,
        )

    def chip_sum(r, z):
        return wg_own[z, r] + wg_pair_recv[z, r].astype(F32)

    @pl.loop(0, chips)
    def _(i):
        z = order(i)
        pair(z).wait_recv()

        @pl.when((chip == 0) & (z > 0))
        def _():
            for r in range(relations):
                up_send[z, r] = chip_sum(r, z).astype(BF16)
                climb(z, r).start()

        @pl.when((chip == chips - 1) & (z < chips - 1))
        def _():
            for r in range(relations):
                down_send[z, r] = chip_sum(r, z).astype(BF16)
                descend(z, r).start()

    pieces = (chips - 1) * relations

    def line_piece(step):
        up = step - (chip - 1)
        d = chips - 1 - up // relations
        r = lax.rem(up, relations)

        @pl.when((chip > 0) & (up >= 0) & (up < pieces) & (d > chip))
        def _():
            climb(d, r).wait_recv()
            up_send[d, r] = (chip_sum(r, d) + up_recv[d, r].astype(F32)).astype(BF16)
            climb(d, r).start()

        down = step - (chips - 2 - chip)
        f = down // relations
        g = lax.rem(down, relations)

        @pl.when((chip < chips - 1) & (down >= 0) & (down < pieces) & (f < chip))
        def _():
            descend(f, g).wait_recv()
            down_send[f, g] = (chip_sum(g, f) + down_recv[f, g].astype(F32)).astype(BF16)
            descend(f, g).start()

    def reduce_part(o, i):
        return pltpu.make_async_remote_copy(
            src_ref=part.at[o, aligned(rel(i) * quarter, quarter, quarter), :],
            dst_ref=part_recv.at[i, o],
            send_sem=sent_sem.at[6], recv_sem=d_recv.at[o],
            device_id=(rel(i), me), device_id_type=MESH,
        )

    @pl.loop(1, chips + 1)
    def _(e):
        z = lax.rem(chip + e, chips)
        product = jnp.dot(
            adj_t[aligned(z * 2 * blk, 2 * blk, blk), :], gm[...], preferred_element_type=F32
        )
        for v in range(2):
            o = z * 2 + v
            part[o] = product[v * blk : (v + 1) * blk].astype(BF16)
            for i in range(1, groups):
                reduce_part(o, i).start()

    def give_back(j):
        return pltpu.make_async_remote_copy(
            src_ref=part_sum.at[tgt(j)], dst_ref=part_back.at[me],
            send_sem=sent_sem.at[7], recv_sem=back_sem,
            device_id=(grp, tgt(j)), device_id_type=MESH,
        )

    def reduced(o):
        total = part[o, aligned(grp * quarter, quarter, quarter), :].astype(F32)
        drain(part_recv.at[1:groups, o], d_recv.at[o])
        for i in range(1, groups):
            total = total + part_recv[i, o].astype(F32)
        return total.astype(BF16)

    def send_reduced(j):
        part_sum[tgt(j)] = reduced(tgt(j))
        give_back(j).start()

    @pl.loop(0, pieces + chips - 2)
    def _(step):
        line_piece(step)

        @pl.when(step + 2 < n)
        def _():
            send_reduced(step + 2)

    send_reduced(1)
    part_back[me] = reduced(me)

    for r in range(relations):
        grad_w[r] = chip_sum(r, chip)

    @pl.when(chip > 0)
    def _():
        for r in range(relations):
            climb(chip, r).wait_recv()
            grad_w[r] = grad_w[r] + up_recv[chip, r].astype(F32)

    @pl.when(chip < chips - 1)
    def _():
        for r in range(relations):
            descend(chip, r).wait_recv()
            grad_w[r] = grad_w[r] + down_recv[chip, r].astype(F32)

    save_w.start()

    drain(part_sum.at[: n - 1], back_sem)

    for k in range(sections):
        grad_f[k] = jnp.zeros((quarter, width), F32)

    @pl.loop(0, n)
    def _(t):
        wanted = table[t, me]
        addend = part_back[t].astype(F32)
        for k in range(sections):
            grad_f[k] = grad_f[k] + addend * is_one(wanted == k)

    save_f.start()

    fetch_pair.wait_send()
    at_end = (chip == 0) | (chip == chips - 1)

    @pl.when(at_end)
    def _():
        drain(gathered.at[:chips], sent_sem.at[0])

    @pl.when(jnp.logical_not(at_end))
    def _():
        drain(gathered, sent_sem.at[0])

    drain(fetched.at[: (n - 2) * (groups - 1) * quarter, :], sent_sem.at[1])
    drain(pre_recv.at[1:groups], sent_sem.at[2])
    drain(pre_recv.at[1:groups], sent_sem.at[3])
    drain(wg_pair, sent_sem.at[4])
    drain(up_send.at[: chips - 1], sent_sem.at[5])
    drain(part_recv.at[1:groups], sent_sem.at[6])
    drain(part_sum.at[: n - 1], sent_sem.at[7])
    save_out.wait()
    save_w.wait()
    save_f.wait()


def hand_over(out_in, grad_w_in, grad_f_in, out, grad_w, grad_f):
    out[...] = out_in[...]
    grad_w[...] = grad_w_in[...]
    grad_f[...] = grad_f_in[...]


def per_device(
    n, groups,
    features, weights, bias, cotangent, tile_values, tile_count, tile_slot, source_blocks,
):
    rows, width = features.shape
    relations, _, slot_total, blk = tile_values.shape
    sections = rows // blk
    quarter, share, chunk, chips = blk // groups, width // groups, width // n, n // 2
    half = rows // 2
    vmem = pl.BlockSpec(memory_space=pltpu.VMEM)
    smem = pl.BlockSpec(memory_space=pltpu.SMEM)
    anywhere = pl.BlockSpec(memory_space=pl.ANY)
    dma = pltpu.SemaphoreType.DMA
    out, grad_w, grad_f = pl.pallas_call(
        functools.partial(kernel, n, groups),
        out_shape=(
            jax.ShapeDtypeStruct((share, rows), BF16),
            jax.ShapeDtypeStruct((relations, chunk, width), F32),
            jax.ShapeDtypeStruct((sections, quarter, width), F32),
        ),
        in_specs=[smem, smem, smem, vmem, vmem, vmem, anywhere, anywhere],
        out_specs=(anywhere, anywhere, anywhere),
        scratch_shapes=[
            pltpu.VMEM((share, rows), BF16),
            pltpu.VMEM((relations, chunk, width), F32),
            pltpu.VMEM((sections, quarter, width), F32),
            dma((3,)),
            pltpu.VMEM((relations, width, width), BF16),
            pltpu.VMEM((relations, rows * slot_total, blk), jnp.int32),
            pltpu.VMEM((n, sections, quarter, width), BF16),
            pltpu.VMEM((blk, width), BF16),
            pltpu.VMEM((slot_total, blk, blk), BF16),
            pltpu.VMEM((slot_total, blk, blk), BF16),
            pltpu.VMEM((n * blk, width), BF16),
            pltpu.VMEM((relations * rows, n * blk), BF16),
            pltpu.VMEM((relations * rows, 128), F32),
            pltpu.VMEM((relations * rows, width), BF16),
            pltpu.VMEM((relations, 2, chips * chunk, rows), BF16),
            pltpu.VMEM((chips, relations, chunk, width), F32),
            pltpu.VMEM((n * blk, relations * rows), BF16),
            pltpu.VMEM((rows, width), F32),
            pltpu.VMEM((groups, half, 2 * share), BF16),
            pltpu.VMEM((groups, half, 2 * share), BF16),
            pltpu.VMEM((half, 2 * share), F32),
            pltpu.VMEM((half, 2 * share), F32),
            pltpu.VMEM((1, 2 * share), F32),
            pltpu.VMEM((groups, half, 2 * share), BF16),
            pltpu.VMEM((rows, width), BF16),
            pltpu.VMEM((relations * rows, width), BF16),
            pltpu.VMEM((n, blk, width), BF16),
            pltpu.VMEM((groups, n, quarter, width), BF16),
            pltpu.VMEM((n, quarter, width), BF16),
            pltpu.VMEM((n, quarter, width), BF16),
            pltpu.VMEM((chips, relations, chunk, width), BF16),
            pltpu.VMEM((chips, relations, chunk, width), BF16),
            pltpu.VMEM((chips, relations, chunk, width), BF16),
            pltpu.VMEM((chips, relations, chunk, width), BF16),
            pltpu.VMEM((chips, relations, chunk, width), BF16),
            pltpu.VMEM((chips, relations, chunk, width), BF16),
            dma((2,)), dma((2,)), dma((8,)), dma, dma,
            dma((n, 2)), dma((n, 2, 2)),
            dma((2,)), dma((2,)), dma((n,)), dma((chips,)),
            dma((chips, relations)), dma((chips, relations)),
        ],
        compiler_params=pltpu.CompilerParams(
            collective_id=0, has_side_effects=True, vmem_limit_bytes=60 << 20
        ),
        name="layer",
    )(
        source_blocks, tile_count, tile_slot,
        features.reshape(sections, groups, quarter, width), cotangent, bias,
        tile_values.reshape(relations, rows * slot_total, blk), weights,
    )
    results = (out, grad_w, grad_f)
    out, grad_w, grad_f = pl.pallas_call(
        hand_over,
        out_shape=tuple(jax.ShapeDtypeStruct(x.shape, x.dtype) for x in results),
        in_specs=[vmem] * 3,
        out_specs=(vmem,) * 3,
        name="hand_over",
    )(*results)
    return (out.T, grad_w, grad_f)


def solution(mesh):
    placed = (
        P("tgt", None),
        P("rel", None, None),
        P(),
        P("tgt", None),
        P("rel", "tgt", None, None),
        P("rel", "tgt"),
        P("rel", "tgt", None),
        P(),
    )
    return jax.shard_map(
        functools.partial(per_device, mesh.shape["tgt"], mesh.shape["rel"]),
        mesh=mesh,
        in_specs=placed,
        out_specs=(P("tgt", "rel"), P("rel", "tgt", None), P("tgt", "rel", None)),
        check_vma=False,
    )
```

```python
import functools

import jax
import jax.numpy as jnp
from jax import lax
from jax.experimental import pallas as pl
from jax.experimental.pallas import tpu as pltpu
from jax.sharding import PartitionSpec as P

MESH = pl.DeviceIdType.MESH
F32 = jnp.float32
BF16 = jnp.bfloat16


def aligned(start, size, multiple):
    return pl.ds(pl.multiple_of(start, multiple), size)


def is_one(condition):
    return condition.astype(jnp.int32).astype(F32)


def pack(value, first, width):
    half = value.shape[0] // 2
    return jnp.concatenate(
        [value[:half, first : first + width], value[half:, first : first + width]], axis=1
    )


def drain(view, semaphore):
    pltpu.make_async_copy(view, view, semaphore).wait()


def kernel(
    n, groups,
    table, counts, slots,
    feat_hbm, cot_hbm, bias, values_hbm, weights_hbm,
    out, grad_w, grad_f,
    weights, values, feat, cot, gathered, partner_staged, masked, masked_t, fetched, adj, scale, msg, msg_t, wg_own, adj_t, pre,
    pre_send, pre_recv, cot_own, active, bias_own, gp_all, gp, gm,
    part, part_recv, part_sum, part_back,
    wg_pair, wg_pair_recv, up_send, up_recv, down_send, down_recv,
    load_sem, pair_sem, sent_sem, spread_sem, back_sem,
    a_recv, b_recv, p_recv, g_recv, d_recv, w_recv, u_recv, v_recv,
):
    me = lax.axis_index("tgt")
    grp = lax.axis_index("rel")
    sections, _, quarter, width = feat.shape
    blk = quarter * groups
    rows = sections * blk
    relations = weights.shape[0]
    slot_total = slots.shape[2]
    share = width // groups
    chips = n // 2
    chip, core = me // 2, lax.rem(me, 2)

    def tgt(j):
        return lax.rem(chip + j // 2, chips) * 2 + lax.rem(core + lax.rem(j, 2), 2)

    below, above_me = chip, chips - 1 - chip
    both = jnp.minimum(below, above_me)

    def near(j):
        k = j // 2 - 1
        two_sided = jnp.where(lax.rem(k, 2) == 0, chip + k // 2 + 1, chip - k // 2 - 1)
        distance = k - both + 1
        one_sided = jnp.where(above_me > below, chip + distance, chip - distance)
        return jnp.where(k < 2 * both, two_sided, one_sided) * 2 + lax.rem(core + lax.rem(j, 2), 2)

    partner = chip * 2 + 1 - core
    row, column = grp // 2, lax.rem(grp, 2)
    beside = row * 2 + 1 - column
    above = (1 - row) * 2 + column

    square = groups == 4

    def rel(i):
        if square:
            return (grp, beside, above, (1 - row) * 2 + 1 - column)[i]
        return lax.rem(grp + i, groups)

    load_w = pltpu.make_async_copy(weights_hbm, weights, load_sem.at[0])
    load_v = pltpu.make_async_copy(values_hbm, values, load_sem.at[1])
    load_f = pltpu.make_async_copy(feat_hbm, feat, load_sem.at[2])
    load_c = pltpu.make_async_copy(cot_hbm, cot, load_sem.at[3])
    load_f.start()
    load_v.start()
    load_w.start()
    load_c.start()

    barrier = pltpu.get_barrier_semaphore()

    @pl.loop(1, n)
    def _(j):
        pl.semaphore_signal(barrier, inc=1, device_id=(grp, tgt(j)), device_id_type=MESH)

    for i in range(1, groups):
        pl.semaphore_signal(barrier, inc=1, device_id=(rel(i), me), device_id_type=MESH)

    def whole_block(t):
        total = jnp.zeros((blk, width), F32)
        for k in range(sections):
            total = total + feat[k].reshape(blk, width).astype(F32) * is_one(table[t, me] == k)
        return total.astype(BF16)

    pl.semaphore_wait(barrier, n - 1 + groups - 1)

    cut = width // 2

    def columns(h):
        return aligned(h * cut, cut, 128)

    def climb_rows(o, h, source):
        return pltpu.make_async_remote_copy(
            src_ref=source, dst_ref=gathered.at[o, :, :, columns(h)],
            send_sem=sent_sem.at[0], recv_sem=a_recv.at[o, h],
            device_id=(grp, jnp.minimum(chip + 1, chips - 1) * 2 + core), device_id_type=MESH,
        )

    def descend_rows(o, h, source):
        return pltpu.make_async_remote_copy(
            src_ref=source, dst_ref=gathered.at[o, :, :, columns(h)],
            send_sem=sent_sem.at[0], recv_sem=a_recv.at[o, h],
            device_id=(grp, jnp.maximum(chip - 1, 0) * 2 + core), device_id_type=MESH,
        )

    def across_rows(o, h):
        return pltpu.make_async_remote_copy(
            src_ref=gathered.at[o, :, :, columns(h)], dst_ref=gathered.at[o, :, :, columns(h)],
            send_sem=sent_sem.at[0], recv_sem=a_recv.at[o, h],
            device_id=(grp, partner), device_id_type=MESH,
        )

    fetch_pair = pltpu.make_async_remote_copy(
        src_ref=partner_staged, dst_ref=fetched.at[aligned(me * blk, blk, blk), :],
        send_sem=pair_sem.at[0], recv_sem=pair_sem.at[1],
        device_id=(grp, partner), device_id_type=MESH,
    )

    def leap_rows(z, h):
        return pltpu.make_async_remote_copy(
            src_ref=feat_hbm.at[:, grp, :, columns(h)], dst_ref=gathered.at[me, :, :, columns(h)],
            send_sem=sent_sem.at[0], recv_sem=a_recv.at[me, h],
            device_id=(grp, z * 2 + core), device_id_type=MESH,
        )

    for h in range(2):
        @pl.when(chip < chips - 1)
        def _():
            climb_rows(me, h, feat_hbm.at[:, grp, :, columns(h)]).start()

        @pl.when(chip > 0)
        def _():
            descend_rows(me, h, feat_hbm.at[:, grp, :, columns(h)]).start()

    @pl.loop(0, chips)
    def _(z):
        @pl.when((z > chip + 2) | (z < chip - 2))
        def _():
            for h in range(2):
                leap_rows(z, h).start()

    load_f.wait()
    partner_staged[...] = whole_block(partner)
    fetch_pair.start()
    fetched[aligned(me * blk, blk, blk), :] = whole_block(me)

    sent = range(4) if square else range(groups - 1)

    def spread(j, h, way):
        if square:
            size = quarter if way < 2 else quarter // 2
            source = (grp, grp, beside, above)[way]
            extra = quarter // 2 if way == 3 else 0
            peer = (beside, above, above, beside)[way]
        else:
            size, source, extra, peer = quarter, grp, 0, rel(way + 1)
        rows_at = aligned(near(j) * blk + source * quarter + extra, size, size)
        return pltpu.make_async_remote_copy(
            src_ref=fetched.at[rows_at, columns(h)], dst_ref=fetched.at[rows_at, columns(h)],
            send_sem=sent_sem.at[1],
            recv_sem=b_recv.at[j, h, way] if square and way < 2 else spread_sem,
            device_id=(peer, me), device_id_type=MESH,
        )

    first_hop = sent[:2] if square else sent

    def event(e):
        inner = lax.rem(e, 4)
        paired = e < 4 * both
        k = jnp.where(paired, e // 4 * 2 + 1 + lax.rem(inner, 2), e // 2 + 1)
        return k, jnp.where(paired, inner // 2, lax.rem(e, 2))

    def pass_on(e, side):
        k, h = event(e)
        j = 2 * k + side
        if not square:
            return
        spread(j, h, 0).wait_recv()
        spread(j, h, 2).start()
        spread(j, h, 1).wait_recv()
        spread(j, h, 3).start()

    def placed(j, h):
        o = near(j)
        total = jnp.zeros((quarter, cut), F32)
        for k in range(sections):
            total = total + gathered[o, k, :, columns(h)].astype(F32) * is_one(table[me, o] == k)
        fetched[aligned(o * blk + grp * quarter, quarter, quarter), columns(h)] = total.astype(BF16)
        for way in first_hop:
            spread(j, h, way).start()

    def arrive(e):
        k, h = event(e)
        o = near(2 * k)
        across_rows(o, h).wait_recv()

        @pl.when((o // 2 == chip - 1) & (chip < chips - 1))
        def _():
            climb_rows(o, h, gathered.at[o, :, :, columns(h)]).start()

        @pl.when((o // 2 == chip + 1) & (chip > 0))
        def _():
            descend_rows(o, h, gathered.at[o, :, :, columns(h)]).start()

        across_rows(o, h).start()
        placed(2 * k, h)

    def arrive_across(e):
        k, h = event(e)
        across_rows(near(2 * k + 1), h).wait_recv()
        placed(2 * k + 1, h)

    load_v.wait()

    def adjacency(b):
        r, q = b // sections, lax.rem(b, sections)
        count = counts[r, q]
        total = jnp.zeros((blk, blk), F32)
        for s in range(slot_total):
            start = (q * blk * slot_total) + s
            tile = values[r, pl.ds(start, blk, stride=slot_total), :].astype(F32) * is_one(s < count)
            masked[s] = tile.astype(BF16)
            masked_t[s] = tile.T.astype(BF16)
            total = total + tile
        degree = jnp.sum(total, axis=1, keepdims=True)
        root = 1.0 / jnp.sqrt(jnp.maximum(degree, 1.0))
        scale[aligned(b * blk, blk, blk), :] = jnp.broadcast_to(root, (blk, 128))

        @pl.loop(0, n)
        def _(o):
            entry = jnp.zeros((blk, blk), BF16)
            entry_t = jnp.zeros((blk, blk), BF16)
            for s in range(slot_total):
                here = jnp.full((blk, blk), is_one(slots[r, q, s] == o), F32).astype(BF16)
                entry = entry + masked[s] * here
                entry_t = entry_t + masked_t[s] * here
            adj[aligned(b * blk, blk, blk), aligned(o * blk, blk, blk)] = entry
            adj_t[aligned(o * blk, blk, blk), aligned(b * blk, blk, blk)] = entry_t

    blocks = relations * sections

    @pl.loop(0, blocks // 2)
    def _(b):
        adjacency(b)

    events = 2 * (chips - 1)
    arrive(0)
    arrive(1)

    @pl.loop(0, blocks // 2)
    def _(b):
        adjacency(blocks // 2 + b)
        arrive_across(b)
        arrive(2 + b)

    @pl.loop(blocks // 2 + 2, events)
    def _(e):
        arrive(e)
        arrive_across(e - 2)

    pass_on(0, 0)
    arrive_across(events - 2)
    pass_on(0, 1)
    arrive_across(events - 1)

    @pl.loop(1, events)
    def _(e):
        pass_on(e, 0)
        pass_on(e, 1)

    load_w.wait()
    fetch_pair.wait_recv()

    late = n - 2 if square else (n - 2) * (groups - 1)
    drain(fetched.at[: late * quarter, :], spread_sem)

    tile_width = 256

    @pl.loop(0, width // tile_width)
    def _(c):
        at = aligned(c * tile_width, tile_width, tile_width)
        acc = jnp.dot(adj[...], fetched[:, at], preferred_element_type=F32)
        msg[:, at] = (acc * scale[:, 0:1]).astype(BF16)

    @pl.loop(0, width // tile_width)
    def _(c):
        at = aligned(c * tile_width, tile_width, tile_width)
        total = None
        for r in range(relations):
            part_r = jnp.dot(
                msg[r * rows : (r + 1) * rows, :], weights[r, :, at], preferred_element_type=F32
            )
            total = part_r if total is None else total + part_r
        pre[:, at] = total

    whole = pre[...]
    for k in range(groups):
        pre_send[k] = pack(whole, k * share, share).astype(BF16)

    piece_rows = rows // 4

    def reduce_pre(i, p):
        at = slice(p * piece_rows, (p + 1) * piece_rows)
        return pltpu.make_async_remote_copy(
            src_ref=pre_send.at[rel(i), at, :], dst_ref=pre_recv.at[i, at, :],
            send_sem=sent_sem.at[2], recv_sem=p_recv.at[p],
            device_id=(rel(i), me), device_id_type=MESH,
        )

    for p in range(2):
        for i in range(1, groups):
            reduce_pre(i, p).start()

    for r in range(relations):
        turned = msg[r * rows : (r + 1) * rows, :].astype(F32).T
        sliced = turned.reshape(n, width // n, rows)
        for c in range(2):
            msg_t[r, c] = jnp.concatenate([sliced[z * 2 + c] for z in range(chips)], axis=0).astype(BF16)

    load_c.wait()
    for k in range(groups):
        @pl.when(grp == k)
        def _():
            cot_own[...] = pack(cot[...].astype(F32), k * share, share)
            piece = bias[...].reshape(1, width)[:, k * share : (k + 1) * share]
            bias_own[...] = jnp.concatenate([piece, piece], axis=1)

    def gather_gp(i, p):
        at = slice(p * piece_rows, (p + 1) * piece_rows)
        return pltpu.make_async_remote_copy(
            src_ref=gp_all.at[grp, at, :], dst_ref=gp_all.at[grp, at, :],
            send_sem=sent_sem.at[3], recv_sem=g_recv.at[p],
            device_id=(rel(i), me), device_id_type=MESH,
        )

    for p in range(2):
        at = slice(p * piece_rows, (p + 1) * piece_rows)
        total = pre_send[grp, at, :].astype(F32)
        drain(pre_recv.at[1:groups, at, :], p_recv.at[p])
        for i in range(1, groups):
            total = total + pre_recv[i, at, :].astype(F32)
        pre_act = total + bias_own[...]
        sigmoid = jax.nn.sigmoid(pre_act)
        derivative = sigmoid * (1.0 + pre_act * (1.0 - sigmoid))
        gp_all[grp, at, :] = (cot_own[at, :] * derivative).astype(BF16)
        for i in range(1, groups):
            gather_gp(i, p).start()
        active[at, :] = pre_act * sigmoid

    upright = active[...].T
    for h in range(2):
        out[:, h * (rows // 2) : (h + 1) * (rows // 2)] = upright[h * share : (h + 1) * share].astype(BF16)

    for p in range(2):
        drain(pre_recv.at[1:groups, p * piece_rows : (p + 1) * piece_rows, :], g_recv.at[p])
    half = rows // 2
    for h in range(2):
        gp[h * half : (h + 1) * half, :] = jnp.concatenate(
            [gp_all[k][:, h * share : (h + 1) * share].astype(F32) for k in range(groups)], axis=1
        ).astype(BF16)

    def weight_chunks(r, c):
        product = jnp.dot(msg_t[r, c], gp[...], preferred_element_type=F32)
        return product.reshape(chips, width // n, width)

    def pair(z):
        return pltpu.make_async_remote_copy(
            src_ref=wg_pair.at[z], dst_ref=wg_pair_recv.at[z],
            send_sem=sent_sem.at[4], recv_sem=w_recv.at[z],
            device_id=(grp, partner), device_id_type=MESH,
        )

    for r in range(relations):
        wg_pair[:, r] = weight_chunks(r, 1 - core).astype(BF16)

    upper = chip >= chips // 2

    def order(i):
        return jnp.where(upper, i, chips - 1 - i)

    @pl.loop(0, chips)
    def _(i):
        pair(order(i)).start()

    for r in range(relations):
        wg_own[:, r] = weight_chunks(r, core)

    @pl.loop(0, width // tile_width)
    def _(c):
        at = aligned(c * tile_width, tile_width, tile_width)
        for r in range(relations):
            rows_r = slice(r * rows, (r + 1) * rows)
            grads = lax.dot_general(
                gp[...], weights[r, at, :],
                (((1,), (1,)), ((), ())), preferred_element_type=F32,
            )
            gm[rows_r, at] = (grads * scale[rows_r, 0:1]).astype(BF16)

    def climb(d, r):
        return pltpu.make_async_remote_copy(
            src_ref=up_send.at[d, r], dst_ref=up_recv.at[d, r],
            send_sem=sent_sem.at[5], recv_sem=u_recv.at[d, r],
            device_id=(grp, jnp.minimum(chip + 1, chips - 1) * 2 + core), device_id_type=MESH,
        )

    def descend(d, r):
        return pltpu.make_async_remote_copy(
            src_ref=down_send.at[d, r], dst_ref=down_recv.at[d, r],
            send_sem=sent_sem.at[5], recv_sem=v_recv.at[d, r],
            device_id=(grp, jnp.maximum(chip - 1, 0) * 2 + core), device_id_type=MESH,
        )

    def chip_sum(r, z):
        return wg_own[z, r] + wg_pair_recv[z, r].astype(F32)

    @pl.loop(0, chips)
    def _(i):
        z = order(i)
        pair(z).wait_recv()

        @pl.when((chip == 0) & (z > 0))
        def _():
            for r in range(relations):
                up_send[z, r] = chip_sum(r, z).astype(BF16)
                climb(z, r).start()

        @pl.when((chip == chips - 1) & (z < chips - 1))
        def _():
            for r in range(relations):
                down_send[z, r] = chip_sum(r, z).astype(BF16)
                descend(z, r).start()

    pieces = (chips - 1) * relations

    def line_piece(step):
        up = step - (chip - 1)
        d = chips - 1 - up // relations
        r = lax.rem(up, relations)

        @pl.when((chip > 0) & (up >= 0) & (up < pieces) & (d > chip))
        def _():
            climb(d, r).wait_recv()
            up_send[d, r] = (chip_sum(r, d) + up_recv[d, r].astype(F32)).astype(BF16)
            climb(d, r).start()

        down = step - (chips - 2 - chip)
        f = down // relations
        g = lax.rem(down, relations)

        @pl.when((chip < chips - 1) & (down >= 0) & (down < pieces) & (f < chip))
        def _():
            descend(f, g).wait_recv()
            down_send[f, g] = (chip_sum(g, f) + down_recv[f, g].astype(F32)).astype(BF16)
            descend(f, g).start()

    def reduce_part(o, i):
        return pltpu.make_async_remote_copy(
            src_ref=part.at[o, aligned(rel(i) * quarter, quarter, quarter), :],
            dst_ref=part_recv.at[i, o],
            send_sem=sent_sem.at[6], recv_sem=d_recv.at[o],
            device_id=(rel(i), me), device_id_type=MESH,
        )

    @pl.loop(1, chips + 1)
    def _(e):
        z = lax.rem(chip + e, chips)
        product = jnp.dot(
            adj_t[aligned(z * 2 * blk, 2 * blk, blk), :], gm[...], preferred_element_type=F32
        )
        for v in range(2):
            o = z * 2 + v
            part[o] = product[v * blk : (v + 1) * blk].astype(BF16)
            for i in range(1, groups):
                reduce_part(o, i).start()

    def give_back(j):
        return pltpu.make_async_remote_copy(
            src_ref=part_sum.at[tgt(j)], dst_ref=part_back.at[me],
            send_sem=sent_sem.at[7], recv_sem=back_sem,
            device_id=(grp, tgt(j)), device_id_type=MESH,
        )

    def reduced(o):
        total = part[o, aligned(grp * quarter, quarter, quarter), :].astype(F32)
        drain(part_recv.at[1:groups, o], d_recv.at[o])
        for i in range(1, groups):
            total = total + part_recv[i, o].astype(F32)
        return total.astype(BF16)

    def send_reduced(j):
        part_sum[tgt(j)] = reduced(tgt(j))
        give_back(j).start()

    @pl.loop(0, pieces + chips - 2)
    def _(step):
        line_piece(step)

        @pl.when(step + 2 < n)
        def _():
            send_reduced(step + 2)

    send_reduced(1)
    part_back[me] = reduced(me)

    for r in range(relations):
        grad_w[r] = chip_sum(r, chip)

    @pl.when(chip > 0)
    def _():
        for r in range(relations):
            climb(chip, r).wait_recv()
            grad_w[r] = grad_w[r] + up_recv[chip, r].astype(F32)

    @pl.when(chip < chips - 1)
    def _():
        for r in range(relations):
            descend(chip, r).wait_recv()
            grad_w[r] = grad_w[r] + down_recv[chip, r].astype(F32)

    drain(part_sum.at[: n - 1], back_sem)

    for k in range(sections):
        grad_f[k] = jnp.zeros((quarter, width), F32)

    @pl.loop(0, n)
    def _(t):
        wanted = table[t, me]
        addend = part_back[t].astype(F32)
        for k in range(sections):
            grad_f[k] = grad_f[k] + addend * is_one(wanted == k)

    fetch_pair.wait_send()
    for z in range(chips):
        near_by = (z > 0) + (z < chips - 1)
        relayed = 2 * (0 < z < chips - 1)
        far = sum(abs(y - z) > 2 for y in range(chips))

        @pl.when(chip == z)
        def _():
            drain(gathered.at[: near_by + relayed + far + chips - 1], sent_sem.at[0])

    drain(fetched.at[: (n - 2) * (groups - 1) * quarter, :], sent_sem.at[1])
    drain(pre_recv.at[1:groups], sent_sem.at[2])
    drain(pre_recv.at[1:groups], sent_sem.at[3])
    drain(wg_pair, sent_sem.at[4])
    drain(up_send.at[: chips - 1], sent_sem.at[5])
    drain(part_recv.at[1:groups], sent_sem.at[6])
    drain(part_sum.at[: n - 1], sent_sem.at[7])


def hand_over(*refs):
    copies = [pltpu.make_async_copy(refs[k], refs[3 + k], refs[6].at[k]) for k in range(3)]
    for copy in copies:
        copy.start()
    for copy in copies:
        copy.wait()


def per_device(
    n, groups,
    features, weights, bias, cotangent, tile_values, tile_count, tile_slot, source_blocks,
):
    rows, width = features.shape
    relations, _, slot_total, blk = tile_values.shape
    sections = rows // blk
    quarter, share, chunk, chips = blk // groups, width // groups, width // n, n // 2
    half = rows // 2
    vmem = pl.BlockSpec(memory_space=pltpu.VMEM)
    smem = pl.BlockSpec(memory_space=pltpu.SMEM)
    anywhere = pl.BlockSpec(memory_space=pl.ANY)
    hbm = pl.BlockSpec(memory_space=pltpu.HBM)
    dma = pltpu.SemaphoreType.DMA
    out, grad_w, grad_f = pl.pallas_call(
        functools.partial(kernel, n, groups),
        out_shape=(
            pltpu.VMEM((share, rows), BF16),
            pltpu.VMEM((relations, chunk, width), F32),
            pltpu.VMEM((sections, quarter, width), F32),
        ),
        in_specs=[smem, smem, smem, hbm, hbm, vmem, hbm, hbm],
        out_specs=(vmem, vmem, vmem),
        scratch_shapes=[
            pltpu.VMEM((relations, width, width), BF16),
            pltpu.VMEM((relations, rows * slot_total, blk), jnp.int32),
            pltpu.VMEM((sections, groups, quarter, width), BF16),
            pltpu.VMEM((rows, width), BF16),
            pltpu.VMEM((n, sections, quarter, width), BF16),
            pltpu.VMEM((blk, width), BF16),
            pltpu.VMEM((slot_total, blk, blk), BF16),
            pltpu.VMEM((slot_total, blk, blk), BF16),
            pltpu.VMEM((n * blk, width), BF16),
            pltpu.VMEM((relations * rows, n * blk), BF16),
            pltpu.VMEM((relations * rows, 128), F32),
            pltpu.VMEM((relations * rows, width), BF16),
            pltpu.VMEM((relations, 2, chips * chunk, rows), BF16),
            pltpu.VMEM((chips, relations, chunk, width), F32),
            pltpu.VMEM((n * blk, relations * rows), BF16),
            pltpu.VMEM((rows, width), F32),
            pltpu.VMEM((groups, half, 2 * share), BF16),
            pltpu.VMEM((groups, half, 2 * share), BF16),
            pltpu.VMEM((half, 2 * share), F32),
            pltpu.VMEM((half, 2 * share), F32),
            pltpu.VMEM((1, 2 * share), F32),
            pltpu.VMEM((groups, half, 2 * share), BF16),
            pltpu.VMEM((rows, width), BF16),
            pltpu.VMEM((relations * rows, width), BF16),
            pltpu.VMEM((n, blk, width), BF16),
            pltpu.VMEM((groups, n, quarter, width), BF16),
            pltpu.VMEM((n, quarter, width), BF16),
            pltpu.VMEM((n, quarter, width), BF16),
            pltpu.VMEM((chips, relations, chunk, width), BF16),
            pltpu.VMEM((chips, relations, chunk, width), BF16),
            pltpu.VMEM((chips, relations, chunk, width), BF16),
            pltpu.VMEM((chips, relations, chunk, width), BF16),
            pltpu.VMEM((chips, relations, chunk, width), BF16),
            pltpu.VMEM((chips, relations, chunk, width), BF16),
            dma((4,)), dma((2,)), dma((8,)), dma, dma,
            dma((n, 2)), dma((n, 2, 2)),
            dma((2,)), dma((2,)), dma((n,)), dma((chips,)),
            dma((chips, relations)), dma((chips, relations)),
        ],
        compiler_params=pltpu.CompilerParams(
            collective_id=0, has_side_effects=True, vmem_limit_bytes=60 << 20
        ),
        name="layer",
    )(
        source_blocks, tile_count, tile_slot,
        features.reshape(sections, groups, quarter, width), cotangent, bias,
        tile_values.reshape(relations, rows * slot_total, blk), weights,
    )
    results = (out, grad_w, grad_f)
    out, grad_w, grad_f = pl.pallas_call(
        hand_over,
        out_shape=tuple(jax.ShapeDtypeStruct(x.shape, x.dtype) for x in results),
        in_specs=[vmem] * 3,
        out_specs=(anywhere,) * 3,
        scratch_shapes=[dma((3,))],
        compiler_params=pltpu.CompilerParams(vmem_limit_bytes=4 << 20),
        name="hand_over",
    )(*results)
    return (out.T, grad_w, grad_f)


def solution(mesh):
    placed = (
        P("tgt", None),
        P("rel", None, None),
        P(),
        P("tgt", None),
        P("rel", "tgt", None, None),
        P("rel", "tgt"),
        P("rel", "tgt", None),
        P(),
    )
    return jax.shard_map(
        functools.partial(per_device, mesh.shape["tgt"], mesh.shape["rel"]),
        mesh=mesh,
        in_specs=placed,
        out_specs=(P("tgt", "rel"), P("rel", "tgt", None), P("tgt", "rel", None)),
        check_vma=False,
    )
```

```python
import functools

import jax
import jax.numpy as jnp
from jax import lax
from jax.experimental import pallas as pl
from jax.experimental.pallas import tpu as pltpu
from jax.sharding import PartitionSpec as P

MESH = pl.DeviceIdType.MESH
F32 = jnp.float32
BF16 = jnp.bfloat16


def aligned(start, size, multiple):
    return pl.ds(pl.multiple_of(start, multiple), size)


def is_one(condition):
    return condition.astype(jnp.int32).astype(F32)


def pack(value, first, width):
    half = value.shape[0] // 2
    return jnp.concatenate(
        [value[:half, first : first + width], value[half:, first : first + width]], axis=1
    )


def drain(view, semaphore):
    pltpu.make_async_copy(view, view, semaphore).wait()


def kernel(
    n, groups,
    table, counts, slots,
    feat_hbm, cot_hbm, bias, values_hbm, weights_hbm,
    out, grad_w, grad_f,
    weights, values, feat, cot, gathered, partner_staged, masked, masked_t, fetched, adj, scale, turned_scratch, msg, msg_t, msg_all, msg_end, end_sum, end_send, end_recv, adj_t, pre,
    pre_send, pre_recv, cot_own, active, bias_own, gp_all, gp_full, gm,
    part, part_recv, relay, relay_recv, part_sum, part_back,
    load_sem, pair_sem, sent_sem, spread_sem, back_sem, end_sem, help_sem,
    a_recv, b_recv, p_recv, g_recv, d_recv, r_recv, msg_sem, line_sem, other_sem, across_sem,
):
    me = lax.axis_index("tgt")
    grp = lax.axis_index("rel")
    sections, _, quarter, width = feat.shape
    blk = quarter * groups
    rows = sections * blk
    relations = weights.shape[0]
    slot_total = slots.shape[2]
    share = width // groups
    chips = n // 2
    chip, core = me // 2, lax.rem(me, 2)

    def tgt(j):
        return lax.rem(chip + j // 2, chips) * 2 + lax.rem(core + lax.rem(j, 2), 2)

    below, above_me = chip, chips - 1 - chip
    both = jnp.minimum(below, above_me)
    assisted = chips == 4 or chips > 5
    last = chips - 1
    is_end = (chip == 0) | (chip == last)
    agent_low, agent_high = 2, last - 2
    helped = jnp.where(chip == agent_low, 0, last)
    is_agent = (chip == agent_low) | (chip == agent_high)

    def near(j):
        k = j // 2 - 1
        two_sided = jnp.where(lax.rem(k, 2) == 0, chip + k // 2 + 1, chip - k // 2 - 1)
        distance = k - both + 1
        one_sided = jnp.where(above_me > below, chip + distance, chip - distance)
        return jnp.where(k < 2 * both, two_sided, one_sided) * 2 + lax.rem(core + lax.rem(j, 2), 2)

    partner = chip * 2 + 1 - core
    row, column = grp // 2, lax.rem(grp, 2)
    beside = row * 2 + 1 - column
    above = (1 - row) * 2 + column

    square = groups == 4

    def rel(i):
        if square:
            return (grp, beside, above, (1 - row) * 2 + 1 - column)[i]
        return lax.rem(grp + i, groups)

    load_w = pltpu.make_async_copy(weights_hbm, weights, load_sem.at[0])
    load_v = pltpu.make_async_copy(values_hbm, values, load_sem.at[1])
    load_f = pltpu.make_async_copy(feat_hbm, feat, load_sem.at[2])
    load_c = pltpu.make_async_copy(cot_hbm, cot, load_sem.at[3])
    load_f.start()
    load_v.start()
    load_w.start()
    load_c.start()

    barrier = pltpu.get_barrier_semaphore()

    @pl.loop(1, n)
    def _(j):
        pl.semaphore_signal(barrier, inc=1, device_id=(grp, tgt(j)), device_id_type=MESH)

    for i in range(1, groups):
        pl.semaphore_signal(barrier, inc=1, device_id=(rel(i), me), device_id_type=MESH)

    def whole_block(t):
        total = jnp.zeros((blk, width), F32)
        for k in range(sections):
            total = total + feat[k].reshape(blk, width).astype(F32) * is_one(table[t, me] == k)
        return total.astype(BF16)

    pl.semaphore_wait(barrier, n - 1 + groups - 1)

    cut = width // 2

    def columns(h):
        return aligned(h * cut, cut, 128)

    def climb_rows(o, h, source):
        return pltpu.make_async_remote_copy(
            src_ref=source, dst_ref=gathered.at[o, :, :, columns(h)],
            send_sem=sent_sem.at[0], recv_sem=a_recv.at[o, h],
            device_id=(grp, jnp.minimum(chip + 1, chips - 1) * 2 + core), device_id_type=MESH,
        )

    def descend_rows(o, h, source):
        return pltpu.make_async_remote_copy(
            src_ref=source, dst_ref=gathered.at[o, :, :, columns(h)],
            send_sem=sent_sem.at[0], recv_sem=a_recv.at[o, h],
            device_id=(grp, jnp.maximum(chip - 1, 0) * 2 + core), device_id_type=MESH,
        )

    def across_rows(o, h):
        return pltpu.make_async_remote_copy(
            src_ref=gathered.at[o, :, :, columns(h)], dst_ref=gathered.at[o, :, :, columns(h)],
            send_sem=sent_sem.at[0], recv_sem=a_recv.at[o, h],
            device_id=(grp, partner), device_id_type=MESH,
        )

    fetch_pair = pltpu.make_async_remote_copy(
        src_ref=partner_staged, dst_ref=fetched.at[aligned(me * blk, blk, blk), :],
        send_sem=pair_sem.at[0], recv_sem=pair_sem.at[1],
        device_id=(grp, partner), device_id_type=MESH,
    )

    def leap_rows(z, h):
        return pltpu.make_async_remote_copy(
            src_ref=feat_hbm.at[:, grp, :, columns(h)], dst_ref=gathered.at[me, :, :, columns(h)],
            send_sem=sent_sem.at[0], recv_sem=a_recv.at[me, h],
            device_id=(grp, z * 2 + core), device_id_type=MESH,
        )

    for h in range(2):
        @pl.when(chip < chips - 1)
        def _():
            climb_rows(me, h, feat_hbm.at[:, grp, :, columns(h)]).start()

        @pl.when(chip > 0)
        def _():
            descend_rows(me, h, feat_hbm.at[:, grp, :, columns(h)]).start()

    @pl.loop(0, chips)
    def _(z):
        @pl.when((z > chip + 2) | (z < chip - 2))
        def _():
            for h in range(2):
                leap_rows(z, h).start()

    load_f.wait()
    partner_staged[...] = whole_block(partner)
    fetch_pair.start()
    fetched[aligned(me * blk, blk, blk), :] = whole_block(me)

    sent = range(4) if square else range(groups - 1)

    def spread(j, h, way):
        if square:
            size = quarter if way < 2 else quarter // 2
            source = (grp, grp, beside, above)[way]
            extra = quarter // 2 if way == 3 else 0
            peer = (beside, above, above, beside)[way]
        else:
            size, source, extra, peer = quarter, grp, 0, rel(way + 1)
        rows_at = aligned(near(j) * blk + source * quarter + extra, size, size)
        return pltpu.make_async_remote_copy(
            src_ref=fetched.at[rows_at, columns(h)], dst_ref=fetched.at[rows_at, columns(h)],
            send_sem=sent_sem.at[1],
            recv_sem=b_recv.at[j, h, way] if square and way < 2 else spread_sem,
            device_id=(peer, me), device_id_type=MESH,
        )

    first_hop = sent[:2] if square else sent

    def event(e):
        inner = lax.rem(e, 4)
        paired = e < 4 * both
        k = jnp.where(paired, e // 4 * 2 + 1 + lax.rem(inner, 2), e // 2 + 1)
        return k, jnp.where(paired, inner // 2, lax.rem(e, 2))

    def pass_on(e, side):
        k, h = event(e)
        j = 2 * k + side
        if not square:
            return
        spread(j, h, 0).wait_recv()
        spread(j, h, 2).start()
        spread(j, h, 1).wait_recv()
        spread(j, h, 3).start()

    def placed(j, h):
        o = near(j)
        total = jnp.zeros((quarter, cut), F32)
        for k in range(sections):
            total = total + gathered[o, k, :, columns(h)].astype(F32) * is_one(table[me, o] == k)
        fetched[aligned(o * blk + grp * quarter, quarter, quarter), columns(h)] = total.astype(BF16)
        for way in first_hop:
            spread(j, h, way).start()

    def arrive(e):
        k, h = event(e)
        o = near(2 * k)
        across_rows(o, h).wait_recv()

        @pl.when((o // 2 == chip - 1) & (chip < chips - 1))
        def _():
            climb_rows(o, h, gathered.at[o, :, :, columns(h)]).start()

        @pl.when((o // 2 == chip + 1) & (chip > 0))
        def _():
            descend_rows(o, h, gathered.at[o, :, :, columns(h)]).start()

        across_rows(o, h).start()
        placed(2 * k, h)

    def arrive_across(e):
        k, h = event(e)
        across_rows(near(2 * k + 1), h).wait_recv()
        placed(2 * k + 1, h)

    load_v.wait()

    def adjacency(b):
        r, q = b // sections, lax.rem(b, sections)
        count = counts[r, q]
        total = jnp.zeros((blk, blk), F32)
        for s in range(slot_total):
            start = (q * blk * slot_total) + s
            tile = values[r, pl.ds(start, blk, stride=slot_total), :].astype(F32) * is_one(s < count)
            masked[s] = tile.astype(BF16)
            masked_t[s] = tile.T.astype(BF16)
            total = total + tile
        degree = jnp.sum(total, axis=1, keepdims=True)
        root = 1.0 / jnp.sqrt(jnp.maximum(degree, 1.0))
        scale[aligned(b * blk, blk, blk), :] = jnp.broadcast_to(root, (blk, 128))

        @pl.loop(0, n)
        def _(o):
            entry = jnp.zeros((blk, blk), BF16)
            entry_t = jnp.zeros((blk, blk), BF16)
            for s in range(slot_total):
                here = jnp.full((blk, blk), is_one(slots[r, q, s] == o), F32).astype(BF16)
                entry = entry + masked[s] * here
                entry_t = entry_t + masked_t[s] * here
            adj[aligned(b * blk, blk, blk), aligned(o * blk, blk, blk)] = entry
            adj_t[aligned(o * blk, blk, blk), aligned(b * blk, blk, blk)] = entry_t

    blocks = relations * sections

    @pl.loop(0, blocks // 2)
    def _(b):
        adjacency(b)

    events = 2 * (chips - 1)
    arrive(0)
    arrive(1)

    @pl.loop(0, blocks // 2)
    def _(b):
        adjacency(blocks // 2 + b)
        arrive_across(b)
        arrive(2 + b)

    @pl.loop(blocks // 2 + 2, events)
    def _(e):
        arrive(e)
        arrive_across(e - 2)

    pass_on(0, 0)
    arrive_across(events - 2)
    pass_on(0, 1)
    arrive_across(events - 1)

    @pl.loop(1, events)
    def _(e):
        pass_on(e, 0)
        pass_on(e, 1)

    load_w.wait()
    fetch_pair.wait_recv()

    late = n - 2 if square else (n - 2) * (groups - 1)
    drain(fetched.at[: late * quarter, :], spread_sem)

    tile_width = 256
    chunk = width // n
    for c in range(width // tile_width):
        at = slice(c * tile_width, (c + 1) * tile_width)
        acc = jnp.dot(adj[...], fetched[:, at], preferred_element_type=F32) * scale[:, 0:1]
        msg[:, at] = acc.astype(BF16)
        for r in range(relations):
            turned_scratch[r, at, :] = acc[r * rows : (r + 1) * rows, :].T

    for r in range(relations):
        msg_t[:, r] = turned_scratch[r].reshape(n, chunk, rows).astype(BF16)

    def send_messages(target, z, landing, semaphore):
        return pltpu.make_async_remote_copy(
            src_ref=msg_t.at[target], dst_ref=landing.at[me],
            send_sem=sent_sem.at[4], recv_sem=semaphore,
            device_id=(grp, z * 2 + lax.rem(target, 2)), device_id_type=MESH,
        )

    def start_messages(j):
        target = near(j)
        z = target // 2
        if not assisted:
            send_messages(target, z, msg_all, msg_sem).start()
            return
        away = ((z == 0) & (chip >= agent_low)) | ((z == last) & (chip <= agent_high))

        @pl.when(jnp.logical_not(away))
        def _():
            send_messages(target, z, msg_all, msg_sem).start()

        agent = jnp.where(z == 0, agent_low, agent_high)

        @pl.when(away & jnp.logical_not((agent == chip) & (lax.rem(target, 2) == core)))
        def _():
            send_messages(target, agent, msg_end, end_sem).start()

    @pl.loop(2, n)
    def _(j):
        start_messages(j)

    send_messages(partner, chip, msg_all, msg_sem).start()
    msg_all[me] = msg_t[me]
    if assisted:
        msg_end[me] = msg_t[helped * 2 + core]

    @pl.loop(0, width // tile_width)
    def _(c):
        at = aligned(c * tile_width, tile_width, tile_width)
        total = None
        for r in range(relations):
            part_r = jnp.dot(
                msg[r * rows : (r + 1) * rows, :], weights[r, :, at], preferred_element_type=F32
            )
            total = part_r if total is None else total + part_r
        pre[:, at] = total

    whole = pre[...]
    for k in range(groups):
        pre_send[k] = pack(whole, k * share, share).astype(BF16)

    piece_rows = rows // 4

    def reduce_pre(i, p):
        at = slice(p * piece_rows, (p + 1) * piece_rows)
        return pltpu.make_async_remote_copy(
            src_ref=pre_send.at[rel(i), at, :], dst_ref=pre_recv.at[i, at, :],
            send_sem=sent_sem.at[2], recv_sem=p_recv.at[p],
            device_id=(rel(i), me), device_id_type=MESH,
        )

    for p in range(2):
        for i in range(1, groups):
            reduce_pre(i, p).start()

    load_c.wait()
    for k in range(groups):
        @pl.when(grp == k)
        def _():
            cot_own[...] = pack(cot[...].astype(F32), k * share, share)
            piece = bias[...].reshape(1, width)[:, k * share : (k + 1) * share]
            bias_own[...] = jnp.concatenate([piece, piece], axis=1)

    def gather_gp(i, p):
        at = slice(p * piece_rows, (p + 1) * piece_rows)
        return pltpu.make_async_remote_copy(
            src_ref=gp_all.at[grp, at, :], dst_ref=gp_all.at[grp, at, :],
            send_sem=sent_sem.at[3], recv_sem=g_recv.at[p],
            device_id=(rel(i), me), device_id_type=MESH,
        )

    for p in range(2):
        at = slice(p * piece_rows, (p + 1) * piece_rows)
        total = pre_send[grp, at, :].astype(F32)
        drain(pre_recv.at[1:groups, at, :], p_recv.at[p])
        for i in range(1, groups):
            total = total + pre_recv[i, at, :].astype(F32)
        pre_act = total + bias_own[...]
        sigmoid = jax.nn.sigmoid(pre_act)
        derivative = sigmoid * (1.0 + pre_act * (1.0 - sigmoid))
        gp_all[grp, at, :] = (cot_own[at, :] * derivative).astype(BF16)
        for i in range(1, groups):
            gather_gp(i, p).start()
        active[at, :] = pre_act * sigmoid

    upright = active[...].T
    for h in range(2):
        out[:, h * (rows // 2) : (h + 1) * (rows // 2)] = upright[h * share : (h + 1) * share].astype(BF16)

    for p in range(2):
        drain(pre_recv.at[1:groups, p * piece_rows : (p + 1) * piece_rows, :], g_recv.at[p])
    half = rows // 2
    for h in range(2):
        gp_full[me, h * half : (h + 1) * half, :] = jnp.concatenate(
            [gp_all[k][:, h * share : (h + 1) * share].astype(F32) for k in range(groups)], axis=1
        ).astype(BF16)

    if square:
        span, mine, other = half, jnp.where(core == 0, column, row), jnp.where(core == 0, beside, above)
    else:
        span, mine, other = rows, 0, grp

    def piece_of(o, part_of):
        return gp_full.at[o, aligned(part_of * span, span, span), :]

    def climb_gp(o):
        return pltpu.make_async_remote_copy(
            src_ref=piece_of(o, mine), dst_ref=piece_of(o, mine),
            send_sem=sent_sem.at[5], recv_sem=line_sem.at[o // 2],
            device_id=(grp, jnp.minimum(chip + 1, chips - 1) * 2 + core), device_id_type=MESH,
        )

    def descend_gp(o):
        return pltpu.make_async_remote_copy(
            src_ref=piece_of(o, mine), dst_ref=piece_of(o, mine),
            send_sem=sent_sem.at[5], recv_sem=line_sem.at[o // 2],
            device_id=(grp, jnp.maximum(chip - 1, 0) * 2 + core), device_id_type=MESH,
        )

    def exchange_gp(o):
        return pltpu.make_async_remote_copy(
            src_ref=piece_of(o, mine), dst_ref=piece_of(o, mine),
            send_sem=sent_sem.at[8], recv_sem=other_sem.at[o // 2],
            device_id=(other, me), device_id_type=MESH,
        )

    def across_gp(o, part_of):
        return pltpu.make_async_remote_copy(
            src_ref=piece_of(o, part_of), dst_ref=piece_of(o, part_of),
            send_sem=sent_sem.at[9], recv_sem=across_sem.at[o // 2],
            device_id=(grp, partner), device_id_type=MESH,
        )

    @pl.when(chip < chips - 1)
    def _():
        climb_gp(me).start()

    @pl.when(chip > 0)
    def _():
        descend_gp(me).start()

    for h in range(rows // span):
        across_gp(me, h).start()

    def gp_arrives(k):
        o = near(2 * k)
        climb_gp(o).wait_recv()

        @pl.when((o < me) & (chip < last - assisted))
        def _():
            climb_gp(o).start()

        @pl.when((o > me) & (chip > 0 + assisted))
        def _():
            descend_gp(o).start()

        if square:
            exchange_gp(o).start()
        across_gp(o, mine).start()

    def gp_completes(k):
        if square:
            o = near(2 * k)
            pltpu.make_async_remote_copy(
                src_ref=piece_of(o, 1 - mine), dst_ref=piece_of(o, 1 - mine),
                send_sem=sent_sem.at[8], recv_sem=other_sem.at[o // 2],
                device_id=(other, me), device_id_type=MESH,
            ).wait_recv()
            across_gp(o, 1 - mine).start()

    def gp_crossed(o):
        drain(gp_full.at[o], across_sem.at[o // 2])

    def weigh(o):
        chunk = width // n
        if chunk % 16 == 0:
            product = jnp.dot(
                msg_all[o].reshape(relations * chunk, rows), gp_full[o], preferred_element_type=F32
            )
            grad_w[...] = grad_w[...] + product.reshape(relations, chunk, width)
        else:
            for r in range(relations):
                grad_w[r] = grad_w[r] + jnp.dot(msg_all[o, r], gp_full[o], preferred_element_type=F32)

    def weigh_end(o):
        for r in range(relations):
            end_sum[r] = end_sum[r] + jnp.dot(msg_end[o, r], gp_full[o], preferred_element_type=F32)

    grad_w[...] = jnp.zeros(grad_w.shape, F32)
    end_sum[...] = jnp.zeros(end_sum.shape, F32)
    help_end = pltpu.make_async_remote_copy(
        src_ref=end_send, dst_ref=end_recv,
        send_sem=sent_sem.at[11], recv_sem=help_sem,
        device_id=(grp, helped * 2 + core), device_id_type=MESH,
    )

    @pl.loop(0, width // tile_width)
    def _(c):
        at = aligned(c * tile_width, tile_width, tile_width)
        for r in range(relations):
            rows_r = slice(r * rows, (r + 1) * rows)
            grads = lax.dot_general(
                gp_full[me], weights[r, at, :],
                (((1,), (1,)), ((), ())), preferred_element_type=F32,
            )
            gm[rows_r, at] = (grads * scale[rows_r, 0:1]).astype(BF16)

    lower, higher = slice(0, cut), slice(cut, width)

    def far(j):
        return near(n - j + 2 * lax.rem(j, 2))

    def reduce_part(o, i):
        if square:
            source = part.at[o, :, 1 - column, :, lower] if i == 1 else part.at[o, 1 - row, :, :, higher]
            target, peer = part_recv.at[o, i - 1], (beside, above)[i - 1]
        else:
            source, target, peer = part.at[o, rel(i)], part_recv.at[i, o], rel(i)
        return pltpu.make_async_remote_copy(
            src_ref=source, dst_ref=target,
            send_sem=sent_sem.at[6], recv_sem=d_recv.at[o],
            device_id=(peer, me), device_id_type=MESH,
        )

    def relay_part(o, w):
        return pltpu.make_async_remote_copy(
            src_ref=relay.at[o, w], dst_ref=relay_recv.at[o, w],
            send_sem=sent_sem.at[10], recv_sem=r_recv.at[o],
            device_id=((above, beside)[w], me), device_id_type=MESH,
        )

    @pl.loop(1, chips + 1)
    def _(e):
        z = jnp.where(e == chips, chip, near(jnp.maximum(n - 2 * e, 2)) // 2)
        product = jnp.dot(
            adj_t[aligned(z * 2 * blk, 2 * blk, blk), :], gm[...], preferred_element_type=F32
        )
        for v in range(2):
            o = z * 2 + v
            part[o] = product[v * blk : (v + 1) * blk].astype(BF16).reshape(part.shape[1:])
            for i in range(1, 3 if square else groups):
                reduce_part(o, i).start()

    def give_back(j):
        return pltpu.make_async_remote_copy(
            src_ref=part_sum.at[far(j)], dst_ref=part_back.at[me],
            send_sem=sent_sem.at[7], recv_sem=back_sem,
            device_id=(grp, far(j)), device_id_type=MESH,
        )

    def relayed(o):
        if square:
            drain(part_recv.at[o], d_recv.at[o])
            up = part[o, 1 - row, column, :, lower].astype(F32) + part_recv[o, 0, 1 - row].astype(F32)
            relay[o, 0] = up.astype(BF16)
            relay_part(o, 0).start()
            aside = part[o, row, 1 - column, :, higher].astype(F32) + part_recv[o, 1, 1 - column].astype(F32)
            relay[o, 1] = aside.astype(BF16)
            relay_part(o, 1).start()

    def reduced(o):
        if square:
            drain(relay_recv.at[o], r_recv.at[o])
            first = part[o, row, column, :, lower].astype(F32) + part_recv[o, 0, row].astype(F32)
            second = part[o, row, column, :, higher].astype(F32) + part_recv[o, 1, column].astype(F32)
            first = first + relay_recv[o, 0].astype(F32)
            second = second + relay_recv[o, 1].astype(F32)
            return jnp.concatenate([first, second], axis=1).astype(BF16)
        total = part[o, grp].astype(F32)
        drain(part_recv.at[1:groups, o], d_recv.at[o])
        for i in range(1, groups):
            total = total + part_recv[i, o].astype(F32)
        return total.astype(BF16)

    def send_reduced(j):
        part_sum[far(j)] = reduced(far(j))
        give_back(j).start()

    relays = both > 0
    weigh(me)
    gp_arrives(1)

    @pl.when(relays)
    def _():
        gp_arrives(2)

    @pl.loop(2, n - 2)
    def _(j):
        relayed(far(j))

    if not assisted:
        @pl.when(jnp.logical_not(relays))
        def _():
            gp_arrives(2)

    relayed(far(n - 2))
    relayed(far(n - 1))

    @pl.when(relays)
    def _():
        @pl.loop(3, chips)
        def _(k):
            gp_arrives(k)

    relayed(partner)
    relayed(me)
    sides = jnp.where(helped == 0, last - chip, chip)

    def beyond(i):
        return jnp.where(helped == 0, chip + 1, chip - 1 - (sides - 1)) + i

    def complete(k):
        gp_completes(k)
        gp_crossed(near(2 * k + 1))

    soon = chips == 4
    if assisted and soon:
        @pl.when(is_agent)
        def _():
            complete(1)
            complete(2)
            gp_crossed(partner)

    def help_out():
        drain(msg_end.at[: 2 * (chips - 2) - 1], end_sem)
        weigh_end(me)
        weigh_end(partner)

        @pl.loop(0, sides)
        def _(i):
            weigh_end(beyond(i) * 2)
            weigh_end(beyond(i) * 2 + 1)

        end_send[...] = end_sum[...].astype(BF16)
        help_end.start()

    if assisted and soon:
        pl.when(is_agent)(help_out)


    @pl.loop(2, n)
    def _(j):
        send_reduced(j)

    if not assisted:
        @pl.when(jnp.logical_not(relays))
        def _():
            @pl.loop(3, chips)
            def _(k):
                gp_arrives(k)

    part_sum[partner] = reduced(partner)
    give_partner = pltpu.make_async_remote_copy(
        src_ref=part_sum.at[partner], dst_ref=part_back.at[me],
        send_sem=sent_sem.at[7], recv_sem=back_sem,
        device_id=(grp, partner), device_id_type=MESH,
    )
    give_partner.start()
    part_back[me] = reduced(me)

    if assisted:
        @pl.when(is_end)
        def _():
            drain(msg_all.at[:3], msg_sem)

        @pl.when(jnp.logical_not(is_end))
        def _():
            drain(msg_all.at[: n - 1], msg_sem)
    else:
        drain(msg_all.at[: n - 1], msg_sem)

    reach = jnp.where(is_end, 2, chips) if assisted else chips
    done = jnp.where(is_end, 1, 3) if assisted and soon else 1

    @pl.loop(done, reach)
    def _(k):
        gp_completes(k)

    @pl.loop(done, reach)
    def _(k):
        gp_crossed(near(2 * k + 1))

    if assisted and soon:
        @pl.when(is_end)
        def _():
            gp_crossed(partner)
    else:
        gp_crossed(partner)

    weigh(partner)

    @pl.loop(1, reach)
    def _(k):
        weigh(near(2 * k))
        weigh(near(2 * k + 1))

    if assisted and not soon:
        pl.when(is_agent)(help_out)

    drain(part_sum.at[: n - 1], back_sem)
    if assisted:
        @pl.when(is_end)
        def _():
            help_end.wait_recv()
            grad_w[...] = grad_w[...] + end_recv[...].astype(F32)


    for k in range(sections):
        grad_f[k] = jnp.zeros((quarter, width), F32)

    @pl.loop(0, n)
    def _(t):
        wanted = table[t, me]
        addend = part_back[t].astype(F32)
        for k in range(sections):
            grad_f[k] = grad_f[k] + addend * is_one(wanted == k)

    fetch_pair.wait_send()
    for z in range(chips):
        near_by = (z > 0) + (z < chips - 1)
        relayed = 2 * (0 < z < chips - 1)
        far = sum(abs(y - z) > 2 for y in range(chips))

        @pl.when(chip == z)
        def _():
            drain(gathered.at[: near_by + relayed + far + chips - 1], sent_sem.at[0])

    drain(fetched.at[: (n - 2) * (groups - 1) * quarter, :], sent_sem.at[1])
    drain(pre_recv.at[1:groups], sent_sem.at[2])
    drain(pre_recv.at[1:groups], sent_sem.at[3])
    if assisted:
        @pl.when(is_agent)
        def _():
            drain(msg_all.at[: n - 2], sent_sem.at[4])
            help_end.wait_send()

        @pl.when(jnp.logical_not(is_agent))
        def _():
            drain(msg_all.at[: n - 1], sent_sem.at[4])
    else:
        drain(msg_all.at[: n - 1], sent_sem.at[4])

    for z in range(chips):
        at_end = z in (0, last)
        climbs = z * (z + 1 <= last - assisted) + (z < last)
        descents = (last - z) * (z - 1 >= 0 + assisted) + (z > 0)
        climbs, descents = (climbs if z < last else 0), (descents if z > 0 else 0)
        if at_end:
            climbs, descents = int(z == 0), int(z == last)
        known = 1 if at_end and assisted else last

        @pl.when(chip == z)
        def _():
            if square:
                drain(fetched.at[: (climbs + descents) * span, :], sent_sem.at[5])
                drain(fetched.at[: known * span, :], sent_sem.at[8])
            else:
                drain(gp_full.at[: climbs + descents], sent_sem.at[5])
            drain(gp_full.at[: known + 1], sent_sem.at[9])

    if square:
        drain(part_recv, sent_sem.at[6])
        drain(relay_recv, sent_sem.at[10])
    else:
        drain(part_recv.at[1:groups], sent_sem.at[6])
    drain(part_sum.at[: n - 1], sent_sem.at[7])


def hand_over(*refs):
    copies = [pltpu.make_async_copy(refs[k], refs[3 + k], refs[6].at[k]) for k in range(3)]
    for copy in copies:
        copy.start()
    for copy in copies:
        copy.wait()


def per_device(
    n, groups,
    features, weights, bias, cotangent, tile_values, tile_count, tile_slot, source_blocks,
):
    rows, width = features.shape
    relations, _, slot_total, blk = tile_values.shape
    sections = rows // blk
    quarter, share, chunk, chips = blk // groups, width // groups, width // n, n // 2
    half = rows // 2
    square = groups == 4
    grid = (2, 2) if square else (groups,)
    vmem = pl.BlockSpec(memory_space=pltpu.VMEM)
    smem = pl.BlockSpec(memory_space=pltpu.SMEM)
    anywhere = pl.BlockSpec(memory_space=pl.ANY)
    hbm = pl.BlockSpec(memory_space=pltpu.HBM)
    dma = pltpu.SemaphoreType.DMA
    out, grad_w, grad_f = pl.pallas_call(
        functools.partial(kernel, n, groups),
        out_shape=(
            pltpu.VMEM((share, rows), BF16),
            pltpu.VMEM((relations, chunk, width), F32),
            pltpu.VMEM((sections, quarter, width), F32),
        ),
        in_specs=[smem, smem, smem, hbm, hbm, vmem, hbm, hbm],
        out_specs=(vmem, vmem, vmem),
        scratch_shapes=[
            pltpu.VMEM((relations, width, width), BF16),
            pltpu.VMEM((relations, rows * slot_total, blk), jnp.int32),
            pltpu.VMEM((sections, groups, quarter, width), BF16),
            pltpu.VMEM((rows, width), BF16),
            pltpu.VMEM((n, sections, quarter, width), BF16),
            pltpu.VMEM((blk, width), BF16),
            pltpu.VMEM((slot_total, blk, blk), BF16),
            pltpu.VMEM((slot_total, blk, blk), BF16),
            pltpu.VMEM((n * blk, width), BF16),
            pltpu.VMEM((relations * rows, n * blk), BF16),
            pltpu.VMEM((relations * rows, 128), F32),
            pltpu.VMEM((relations, width, rows), F32),
            pltpu.VMEM((relations * rows, width), BF16),
            pltpu.VMEM((n, relations, chunk, rows), BF16),
            pltpu.VMEM((n, relations, chunk, rows), BF16),
            pltpu.VMEM((n, relations, chunk, rows), BF16),
            pltpu.VMEM((relations, chunk, width), F32),
            pltpu.VMEM((relations, chunk, width), BF16),
            pltpu.VMEM((relations, chunk, width), BF16),
            pltpu.VMEM((n * blk, relations * rows), BF16),
            pltpu.VMEM((rows, width), F32),
            pltpu.VMEM((groups, half, 2 * share), BF16),
            pltpu.VMEM((groups, half, 2 * share), BF16),
            pltpu.VMEM((half, 2 * share), F32),
            pltpu.VMEM((half, 2 * share), F32),
            pltpu.VMEM((1, 2 * share), F32),
            pltpu.VMEM((groups, half, 2 * share), BF16),
            pltpu.VMEM((n, rows, width), BF16),
            pltpu.VMEM((relations * rows, width), BF16),
            pltpu.VMEM((n, *grid, quarter, width), BF16),
            pltpu.VMEM((n, 2, 2, quarter, width // 2) if square else (groups, n, quarter, width), BF16),
            pltpu.VMEM((n, 2, quarter, width // 2), BF16),
            pltpu.VMEM((n, 2, quarter, width // 2), BF16),
            pltpu.VMEM((n, quarter, width), BF16),
            pltpu.VMEM((n, quarter, width), BF16),
            dma((4,)), dma((2,)), dma((12,)), dma, dma, dma, dma,
            dma((n, 2)), dma((n, 2, 2)),
            dma((2,)), dma((2,)), dma((n,)), dma((n,)), dma,
            dma((chips,)), dma((chips,)), dma((chips,)),
        ],
        compiler_params=pltpu.CompilerParams(
            collective_id=0, has_side_effects=True, vmem_limit_bytes=60 << 20
        ),
        name="layer",
    )(
        source_blocks, tile_count, tile_slot,
        features.reshape(sections, groups, quarter, width), cotangent, bias,
        tile_values.reshape(relations, rows * slot_total, blk), weights,
    )
    results = (out, grad_w, grad_f)
    out, grad_w, grad_f = pl.pallas_call(
        hand_over,
        out_shape=tuple(jax.ShapeDtypeStruct(x.shape, x.dtype) for x in results),
        in_specs=[vmem] * 3,
        out_specs=(anywhere,) * 3,
        scratch_shapes=[dma((3,))],
        compiler_params=pltpu.CompilerParams(vmem_limit_bytes=4 << 20),
        name="hand_over",
    )(*results)
    return (out.T, grad_w, grad_f)


def solution(mesh):
    placed = (
        P("tgt", None),
        P("rel", None, None),
        P(),
        P("tgt", None),
        P("rel", "tgt", None, None),
        P("rel", "tgt"),
        P("rel", "tgt", None),
        P(),
    )
    return jax.shard_map(
        functools.partial(per_device, mesh.shape["tgt"], mesh.shape["rel"]),
        mesh=mesh,
        in_specs=placed,
        out_specs=(P("tgt", "rel"), P("rel", "tgt", None), P("tgt", "rel", None)),
        check_vma=False,
    )
```

```python
import functools

import jax
import jax.numpy as jnp
from jax import lax
from jax.experimental import pallas as pl
from jax.experimental.pallas import tpu as pltpu
from jax.sharding import PartitionSpec as P

MESH = pl.DeviceIdType.MESH
F32 = jnp.float32
BF16 = jnp.bfloat16


def aligned(start, size, multiple):
    return pl.ds(pl.multiple_of(start, multiple), size)


def is_one(condition):
    return condition.astype(jnp.int32).astype(F32)


def pack(value, first, width):
    half = value.shape[0] // 2
    return jnp.concatenate(
        [value[:half, first : first + width], value[half:, first : first + width]], axis=1
    )


def drain(view, semaphore):
    pltpu.make_async_copy(view, view, semaphore).wait()


def kernel(
    n, groups,
    table, counts, slots,
    feat_hbm, cot_hbm, bias, values_hbm, weights_hbm,
    out, grad_w, grad_f,
    weights, values, feat, cot, gathered, partner_staged, masked, masked_t, fetched, adj, scale, turned_scratch, msg, msg_t, msg_all, msg_end, end_sum, end_send, end_recv, adj_t, pre,
    pre_send, pre_recv, cot_own, active, bias_own, gp_all, gp_full, gm,
    part, part_recv, relay, relay_recv, part_sum, part_back, inbox, crossed, gathered_sum, collected,
    load_sem, pair_sem, sent_sem, spread_sem, back_sem, end_sem, help_sem, inbox_sem, crossed_sem, collect_sem,
    a_recv, b_recv, p_recv, g_recv, d_recv, r_recv, msg_sem, line_sem, other_sem, across_sem,
):
    me = lax.axis_index("tgt")
    grp = lax.axis_index("rel")
    sections, _, quarter, width = feat.shape
    blk = quarter * groups
    rows = sections * blk
    relations = weights.shape[0]
    slot_total = slots.shape[2]
    share = width // groups
    chips = n // 2
    chip, core = me // 2, lax.rem(me, 2)

    def tgt(j):
        return lax.rem(chip + j // 2, chips) * 2 + lax.rem(core + lax.rem(j, 2), 2)

    below, above_me = chip, chips - 1 - chip
    both = jnp.minimum(below, above_me)
    assisted = chips == 4 or chips > 5
    last = chips - 1
    is_end = (chip == 0) | (chip == last)
    agent_low, agent_high = 2, last - 2
    helped = jnp.where(chip == agent_low, 0, last)
    is_agent = (chip == agent_low) | (chip == agent_high)

    def near(j):
        k = j // 2 - 1
        two_sided = jnp.where(lax.rem(k, 2) == 0, chip + k // 2 + 1, chip - k // 2 - 1)
        distance = k - both + 1
        one_sided = jnp.where(above_me > below, chip + distance, chip - distance)
        return jnp.where(k < 2 * both, two_sided, one_sided) * 2 + lax.rem(core + lax.rem(j, 2), 2)

    partner = chip * 2 + 1 - core
    row, column = grp // 2, lax.rem(grp, 2)
    beside = row * 2 + 1 - column
    above = (1 - row) * 2 + column

    square = groups == 4

    def rel(i):
        if square:
            return (grp, beside, above, (1 - row) * 2 + 1 - column)[i]
        return lax.rem(grp + i, groups)

    load_w = pltpu.make_async_copy(weights_hbm, weights, load_sem.at[0])
    load_v = pltpu.make_async_copy(values_hbm, values, load_sem.at[1])
    load_f = pltpu.make_async_copy(feat_hbm, feat, load_sem.at[2])
    load_c = pltpu.make_async_copy(cot_hbm, cot, load_sem.at[3])
    load_f.start()
    load_v.start()
    load_w.start()
    load_c.start()

    barrier = pltpu.get_barrier_semaphore()

    @pl.loop(1, n)
    def _(j):
        pl.semaphore_signal(barrier, inc=1, device_id=(grp, tgt(j)), device_id_type=MESH)

    for i in range(1, groups):
        pl.semaphore_signal(barrier, inc=1, device_id=(rel(i), me), device_id_type=MESH)

    def whole_block(t):
        total = jnp.zeros((blk, width), F32)
        for k in range(sections):
            total = total + feat[k].reshape(blk, width).astype(F32) * is_one(table[t, me] == k)
        return total.astype(BF16)

    pl.semaphore_wait(barrier, n - 1 + groups - 1)

    cut = width // 2

    def columns(h):
        return aligned(h * cut, cut, 128)

    def climb_rows(o, h, source):
        return pltpu.make_async_remote_copy(
            src_ref=source, dst_ref=gathered.at[o, :, :, columns(h)],
            send_sem=sent_sem.at[0], recv_sem=a_recv.at[o, h],
            device_id=(grp, jnp.minimum(chip + 1, chips - 1) * 2 + core), device_id_type=MESH,
        )

    def descend_rows(o, h, source):
        return pltpu.make_async_remote_copy(
            src_ref=source, dst_ref=gathered.at[o, :, :, columns(h)],
            send_sem=sent_sem.at[0], recv_sem=a_recv.at[o, h],
            device_id=(grp, jnp.maximum(chip - 1, 0) * 2 + core), device_id_type=MESH,
        )

    def across_rows(o, h):
        return pltpu.make_async_remote_copy(
            src_ref=gathered.at[o, :, :, columns(h)], dst_ref=gathered.at[o, :, :, columns(h)],
            send_sem=sent_sem.at[0], recv_sem=a_recv.at[o, h],
            device_id=(grp, partner), device_id_type=MESH,
        )

    fetch_pair = pltpu.make_async_remote_copy(
        src_ref=partner_staged, dst_ref=fetched.at[aligned(me * blk, blk, blk), :],
        send_sem=pair_sem.at[0], recv_sem=pair_sem.at[1],
        device_id=(grp, partner), device_id_type=MESH,
    )

    def leap_rows(z, h):
        return pltpu.make_async_remote_copy(
            src_ref=feat_hbm.at[:, grp, :, columns(h)], dst_ref=gathered.at[me, :, :, columns(h)],
            send_sem=sent_sem.at[0], recv_sem=a_recv.at[me, h],
            device_id=(grp, z * 2 + core), device_id_type=MESH,
        )

    for h in range(2):
        @pl.when(chip < chips - 1)
        def _():
            climb_rows(me, h, feat_hbm.at[:, grp, :, columns(h)]).start()

        @pl.when(chip > 0)
        def _():
            descend_rows(me, h, feat_hbm.at[:, grp, :, columns(h)]).start()

    @pl.loop(0, chips)
    def _(z):
        @pl.when((z > chip + 2) | (z < chip - 2))
        def _():
            for h in range(2):
                leap_rows(z, h).start()

    load_f.wait()
    partner_staged[...] = whole_block(partner)
    fetch_pair.start()
    fetched[aligned(me * blk, blk, blk), :] = whole_block(me)

    sent = range(4) if square else range(groups - 1)

    def spread(j, h, way):
        if square:
            size = quarter if way < 2 else quarter // 2
            source = (grp, grp, beside, above)[way]
            extra = quarter // 2 if way == 3 else 0
            peer = (beside, above, above, beside)[way]
        else:
            size, source, extra, peer = quarter, grp, 0, rel(way + 1)
        rows_at = aligned(near(j) * blk + source * quarter + extra, size, size)
        return pltpu.make_async_remote_copy(
            src_ref=fetched.at[rows_at, columns(h)], dst_ref=fetched.at[rows_at, columns(h)],
            send_sem=sent_sem.at[1],
            recv_sem=b_recv.at[j, h, way] if square and way < 2 else spread_sem,
            device_id=(peer, me), device_id_type=MESH,
        )

    first_hop = sent[:2] if square else sent

    def event(e):
        inner = lax.rem(e, 4)
        paired = e < 4 * both
        k = jnp.where(paired, e // 4 * 2 + 1 + lax.rem(inner, 2), e // 2 + 1)
        return k, jnp.where(paired, inner // 2, lax.rem(e, 2))

    def pass_on(e, side):
        k, h = event(e)
        j = 2 * k + side
        if not square:
            return
        spread(j, h, 0).wait_recv()
        spread(j, h, 2).start()
        spread(j, h, 1).wait_recv()
        spread(j, h, 3).start()

    def placed(j, h):
        o = near(j)
        total = jnp.zeros((quarter, cut), F32)
        for k in range(sections):
            total = total + gathered[o, k, :, columns(h)].astype(F32) * is_one(table[me, o] == k)
        fetched[aligned(o * blk + grp * quarter, quarter, quarter), columns(h)] = total.astype(BF16)
        for way in first_hop:
            spread(j, h, way).start()

    def arrive(e):
        k, h = event(e)
        o = near(2 * k)
        across_rows(o, h).wait_recv()

        @pl.when((o // 2 == chip - 1) & (chip < chips - 1))
        def _():
            climb_rows(o, h, gathered.at[o, :, :, columns(h)]).start()

        @pl.when((o // 2 == chip + 1) & (chip > 0))
        def _():
            descend_rows(o, h, gathered.at[o, :, :, columns(h)]).start()

        across_rows(o, h).start()
        placed(2 * k, h)

    def arrive_across(e):
        k, h = event(e)
        across_rows(near(2 * k + 1), h).wait_recv()
        placed(2 * k + 1, h)

    load_v.wait()

    def adjacency(b):
        r, q = b // sections, lax.rem(b, sections)
        count = counts[r, q]
        total = jnp.zeros((blk, blk), F32)
        for s in range(slot_total):
            start = (q * blk * slot_total) + s
            tile = values[r, pl.ds(start, blk, stride=slot_total), :].astype(F32) * is_one(s < count)
            masked[s] = tile.astype(BF16)
            masked_t[s] = tile.T.astype(BF16)
            total = total + tile
        degree = jnp.sum(total, axis=1, keepdims=True)
        root = 1.0 / jnp.sqrt(jnp.maximum(degree, 1.0))
        scale[aligned(b * blk, blk, blk), :] = jnp.broadcast_to(root, (blk, 128))

        @pl.loop(0, n)
        def _(o):
            entry = jnp.zeros((blk, blk), BF16)
            entry_t = jnp.zeros((blk, blk), BF16)
            for s in range(slot_total):
                here = jnp.full((blk, blk), is_one(slots[r, q, s] == o), F32).astype(BF16)
                entry = entry + masked[s] * here
                entry_t = entry_t + masked_t[s] * here
            adj[aligned(b * blk, blk, blk), aligned(o * blk, blk, blk)] = entry
            adj_t[aligned(o * blk, blk, blk), aligned(b * blk, blk, blk)] = entry_t

    blocks = relations * sections

    @pl.loop(0, blocks // 2)
    def _(b):
        adjacency(b)

    events = 2 * (chips - 1)
    arrive(0)
    arrive(1)

    @pl.loop(0, blocks // 2)
    def _(b):
        adjacency(blocks // 2 + b)
        arrive_across(b)
        arrive(2 + b)

    @pl.loop(blocks // 2 + 2, events)
    def _(e):
        arrive(e)
        arrive_across(e - 2)

    pass_on(0, 0)
    arrive_across(events - 2)
    pass_on(0, 1)
    arrive_across(events - 1)

    @pl.loop(1, events)
    def _(e):
        pass_on(e, 0)
        pass_on(e, 1)

    load_w.wait()
    fetch_pair.wait_recv()

    late = n - 2 if square else (n - 2) * (groups - 1)
    drain(fetched.at[: late * quarter, :], spread_sem)

    tile_width = 256
    chunk = width // n
    for c in range(width // tile_width):
        at = slice(c * tile_width, (c + 1) * tile_width)
        acc = jnp.dot(adj[...], fetched[:, at], preferred_element_type=F32) * scale[:, 0:1]
        msg[:, at] = acc.astype(BF16)
        for r in range(relations):
            turned_scratch[r, at, :] = acc[r * rows : (r + 1) * rows, :].T

    for r in range(relations):
        msg_t[:, r] = turned_scratch[r].reshape(n, chunk, rows).astype(BF16)

    def send_messages(target, z, landing, semaphore):
        return pltpu.make_async_remote_copy(
            src_ref=msg_t.at[target], dst_ref=landing.at[me],
            send_sem=sent_sem.at[4], recv_sem=semaphore,
            device_id=(grp, z * 2 + lax.rem(target, 2)), device_id_type=MESH,
        )

    def start_messages(j):
        target = near(j)
        z = target // 2
        if not assisted:
            send_messages(target, z, msg_all, msg_sem).start()
            return
        away = ((z == 0) & (chip >= agent_low)) | ((z == last) & (chip <= agent_high))

        @pl.when(jnp.logical_not(away))
        def _():
            send_messages(target, z, msg_all, msg_sem).start()

        agent = jnp.where(z == 0, agent_low, agent_high)

        @pl.when(away & jnp.logical_not((agent == chip) & (lax.rem(target, 2) == core)))
        def _():
            send_messages(target, agent, msg_end, end_sem).start()

    @pl.loop(2, n)
    def _(j):
        start_messages(j)

    send_messages(partner, chip, msg_all, msg_sem).start()
    msg_all[me] = msg_t[me]
    if assisted:
        msg_end[me] = msg_t[helped * 2 + core]

    @pl.loop(0, width // tile_width)
    def _(c):
        at = aligned(c * tile_width, tile_width, tile_width)
        total = None
        for r in range(relations):
            part_r = jnp.dot(
                msg[r * rows : (r + 1) * rows, :], weights[r, :, at], preferred_element_type=F32
            )
            total = part_r if total is None else total + part_r
        pre[:, at] = total

    whole = pre[...]
    for k in range(groups):
        pre_send[k] = pack(whole, k * share, share).astype(BF16)

    piece_rows = rows // 4

    def reduce_pre(i, p):
        at = slice(p * piece_rows, (p + 1) * piece_rows)
        return pltpu.make_async_remote_copy(
            src_ref=pre_send.at[rel(i), at, :], dst_ref=pre_recv.at[i, at, :],
            send_sem=sent_sem.at[2], recv_sem=p_recv.at[p],
            device_id=(rel(i), me), device_id_type=MESH,
        )

    for p in range(2):
        for i in range(1, groups):
            reduce_pre(i, p).start()

    load_c.wait()
    for k in range(groups):
        @pl.when(grp == k)
        def _():
            cot_own[...] = pack(cot[...].astype(F32), k * share, share)
            piece = bias[...].reshape(1, width)[:, k * share : (k + 1) * share]
            bias_own[...] = jnp.concatenate([piece, piece], axis=1)

    def gather_gp(i, p):
        at = slice(p * piece_rows, (p + 1) * piece_rows)
        return pltpu.make_async_remote_copy(
            src_ref=gp_all.at[grp, at, :], dst_ref=gp_all.at[grp, at, :],
            send_sem=sent_sem.at[3], recv_sem=g_recv.at[p],
            device_id=(rel(i), me), device_id_type=MESH,
        )

    for p in range(2):
        at = slice(p * piece_rows, (p + 1) * piece_rows)
        total = pre_send[grp, at, :].astype(F32)
        drain(pre_recv.at[1:groups, at, :], p_recv.at[p])
        for i in range(1, groups):
            total = total + pre_recv[i, at, :].astype(F32)
        pre_act = total + bias_own[...]
        sigmoid = jax.nn.sigmoid(pre_act)
        derivative = sigmoid * (1.0 + pre_act * (1.0 - sigmoid))
        gp_all[grp, at, :] = (cot_own[at, :] * derivative).astype(BF16)
        for i in range(1, groups):
            gather_gp(i, p).start()
        active[at, :] = pre_act * sigmoid

    upright = active[...].T
    for h in range(2):
        out[:, h * (rows // 2) : (h + 1) * (rows // 2)] = upright[h * share : (h + 1) * share].astype(BF16)

    for p in range(2):
        drain(pre_recv.at[1:groups, p * piece_rows : (p + 1) * piece_rows, :], g_recv.at[p])
    half = rows // 2
    for h in range(2):
        gp_full[me, h * half : (h + 1) * half, :] = jnp.concatenate(
            [gp_all[k][:, h * share : (h + 1) * share].astype(F32) for k in range(groups)], axis=1
        ).astype(BF16)

    if square:
        span, mine, other = half, jnp.where(core == 0, column, row), jnp.where(core == 0, beside, above)
    else:
        span, mine, other = rows, 0, grp

    def piece_of(o, part_of):
        return gp_full.at[o, aligned(part_of * span, span, span), :]

    def climb_gp(o):
        return pltpu.make_async_remote_copy(
            src_ref=piece_of(o, mine), dst_ref=piece_of(o, mine),
            send_sem=sent_sem.at[5], recv_sem=line_sem.at[o // 2],
            device_id=(grp, jnp.minimum(chip + 1, chips - 1) * 2 + core), device_id_type=MESH,
        )

    def descend_gp(o):
        return pltpu.make_async_remote_copy(
            src_ref=piece_of(o, mine), dst_ref=piece_of(o, mine),
            send_sem=sent_sem.at[5], recv_sem=line_sem.at[o // 2],
            device_id=(grp, jnp.maximum(chip - 1, 0) * 2 + core), device_id_type=MESH,
        )

    def exchange_gp(o):
        return pltpu.make_async_remote_copy(
            src_ref=piece_of(o, mine), dst_ref=piece_of(o, mine),
            send_sem=sent_sem.at[8], recv_sem=other_sem.at[o // 2],
            device_id=(other, me), device_id_type=MESH,
        )

    def across_gp(o, part_of):
        return pltpu.make_async_remote_copy(
            src_ref=piece_of(o, part_of), dst_ref=piece_of(o, part_of),
            send_sem=sent_sem.at[9], recv_sem=across_sem.at[o // 2],
            device_id=(grp, partner), device_id_type=MESH,
        )

    @pl.when(chip < chips - 1)
    def _():
        climb_gp(me).start()

    @pl.when(chip > 0)
    def _():
        descend_gp(me).start()

    whole_end = assisted and square
    next_in = jnp.where(chip == 0, 1, last - 1)

    def beside_end(o):
        return ((o // 2 == 0) & (chip == 1)) | ((o // 2 == last) & (chip == last - 1))

    if whole_end:
        @pl.when(is_end)
        def _():
            pltpu.make_async_remote_copy(
                src_ref=piece_of(me, 1 - mine), dst_ref=piece_of(me, 1 - mine),
                send_sem=sent_sem.at[5], recv_sem=other_sem.at[chip],
                device_id=(grp, next_in * 2 + core), device_id_type=MESH,
            ).start()

    for h in range(rows // span):
        across_gp(me, h).start()

    def gp_arrives(k):
        o = near(2 * k)
        climb_gp(o).wait_recv()

        @pl.when((o < me) & (chip < last - assisted))
        def _():
            climb_gp(o).start()

        @pl.when((o > me) & (chip > 0 + assisted))
        def _():
            descend_gp(o).start()

        if whole_end:
            @pl.when(jnp.logical_not(beside_end(o)))
            def _():
                exchange_gp(o).start()
        elif square:
            exchange_gp(o).start()
        across_gp(o, mine).start()

    def gp_completes(k):
        if square:
            o = near(2 * k)
            pltpu.make_async_remote_copy(
                src_ref=piece_of(o, 1 - mine), dst_ref=piece_of(o, 1 - mine),
                send_sem=sent_sem.at[8], recv_sem=other_sem.at[o // 2],
                device_id=(other, me), device_id_type=MESH,
            ).wait_recv()
            across_gp(o, 1 - mine).start()

    def gp_crossed(o):
        drain(gp_full.at[o], across_sem.at[o // 2])

    def weigh(o):
        chunk = width // n
        if chunk % 16 == 0:
            product = jnp.dot(
                msg_all[o].reshape(relations * chunk, rows), gp_full[o], preferred_element_type=F32
            )
            grad_w[...] = grad_w[...] + product.reshape(relations, chunk, width)
        else:
            for r in range(relations):
                grad_w[r] = grad_w[r] + jnp.dot(msg_all[o, r], gp_full[o], preferred_element_type=F32)

    def weigh_end(o):
        for r in range(relations):
            end_sum[r] = end_sum[r] + jnp.dot(msg_end[o, r], gp_full[o], preferred_element_type=F32)

    grad_w[...] = jnp.zeros(grad_w.shape, F32)
    end_sum[...] = jnp.zeros(end_sum.shape, F32)
    help_end = pltpu.make_async_remote_copy(
        src_ref=end_send, dst_ref=end_recv,
        send_sem=sent_sem.at[11], recv_sem=help_sem,
        device_id=(grp, helped * 2 + core), device_id_type=MESH,
    )

    @pl.loop(0, width // tile_width)
    def _(c):
        at = aligned(c * tile_width, tile_width, tile_width)
        for r in range(relations):
            rows_r = slice(r * rows, (r + 1) * rows)
            grads = lax.dot_general(
                gp_full[me], weights[r, at, :],
                (((1,), (1,)), ((), ())), preferred_element_type=F32,
            )
            gm[rows_r, at] = (grads * scale[rows_r, 0:1]).astype(BF16)

    lower, higher = slice(0, cut), slice(cut, width)

    def far(j):
        return near(n - j + 2 * lax.rem(j, 2))

    def reduce_part(o, i):
        if square:
            source = part.at[o, :, 1 - column, :, lower] if i == 1 else part.at[o, 1 - row, :, :, higher]
            target, peer = part_recv.at[o, i - 1], (beside, above)[i - 1]
        else:
            source, target, peer = part.at[o, rel(i)], part_recv.at[i, o], rel(i)
        return pltpu.make_async_remote_copy(
            src_ref=source, dst_ref=target,
            send_sem=sent_sem.at[6], recv_sem=d_recv.at[o],
            device_id=(peer, me), device_id_type=MESH,
        )

    def relay_part(o, w):
        return pltpu.make_async_remote_copy(
            src_ref=relay.at[o, w], dst_ref=relay_recv.at[o, w],
            send_sem=sent_sem.at[10], recv_sem=r_recv.at[o],
            device_id=((above, beside)[w], me), device_id_type=MESH,
        )

    @pl.loop(1, chips + 1)
    def _(e):
        z = jnp.where(e == chips, chip, near(jnp.maximum(n - 2 * e, 2)) // 2)
        product = jnp.dot(
            adj_t[aligned(z * 2 * blk, 2 * blk, blk), :], gm[...], preferred_element_type=F32
        )
        for v in range(2):
            o = z * 2 + v
            part[o] = product[v * blk : (v + 1) * blk].astype(BF16).reshape(part.shape[1:])
            for i in range(1, 3 if square else groups):
                reduce_part(o, i).start()

    far_chips = chips - 2
    is_inner = (chip == 1) | (chip == last - 1)
    low_side = chip <= 1

    def crosses(o, source):
        return ((source <= 1) & (o // 2 >= 2)) | ((source >= last - 1) & (o // 2 <= last - 2))

    def hand(o, device, landing, semaphore):
        return pltpu.make_async_remote_copy(
            src_ref=part_sum.at[o], dst_ref=landing,
            send_sem=sent_sem.at[7], recv_sem=semaphore,
            device_id=(grp, device), device_id_type=MESH,
        )

    def give_back(j):
        o = far(j)
        if not assisted:
            hand(o, o, part_back.at[me], back_sem).start()
            return
        slot = jnp.where(low_side, jnp.maximum(o // 2 - 2, 0), jnp.minimum(o // 2, far_chips - 1))
        odd = lax.rem(o, 2)
        over = crosses(o, chip)

        @pl.when(over & is_end)
        def _():
            hand(o, next_in * 2 + odd, inbox.at[core, slot], inbox_sem).start()

        @pl.when(over & is_inner & (odd != core))
        def _():
            hand(o, partner, crossed.at[slot], crossed_sem).start()

        @pl.when(jnp.logical_not(over & (is_end | is_inner)))
        def _():
            hand(o, o, part_back.at[me], back_sem).start()

    def collect(slot):
        z = jnp.where(low_side, slot + 2, slot)
        side = jnp.where(low_side, 0, 1)
        return pltpu.make_async_remote_copy(
            src_ref=gathered_sum.at[slot], dst_ref=collected.at[side],
            send_sem=sent_sem.at[12], recv_sem=collect_sem.at[side],
            device_id=(grp, z * 2 + core), device_id_type=MESH,
        )

    def sum_for_far_side():
        drain(crossed, crossed_sem)
        drain(inbox, inbox_sem)
        outer = jnp.where(low_side, 0, last)

        @pl.loop(0, far_chips)
        def _(slot):
            o = jnp.where(low_side, slot + 2, slot) * 2 + core
            terms = (
                (me, part_sum[o].astype(F32)),
                (partner, crossed[slot].astype(F32)),
                (outer * 2, inbox[0, slot].astype(F32)),
                (outer * 2 + 1, inbox[1, slot].astype(F32)),
            )
            for k in range(sections):
                total = None
                for t, term in terms:
                    kept = term * is_one(table[t, o] == k)
                    total = kept if total is None else total + kept
                gathered_sum[slot, k] = total.astype(BF16)
            collect(slot).start()

    def relayed(o):
        if square:
            drain(part_recv.at[o], d_recv.at[o])
            up = part[o, 1 - row, column, :, lower].astype(F32) + part_recv[o, 0, 1 - row].astype(F32)
            relay[o, 0] = up.astype(BF16)
            relay_part(o, 0).start()
            aside = part[o, row, 1 - column, :, higher].astype(F32) + part_recv[o, 1, 1 - column].astype(F32)
            relay[o, 1] = aside.astype(BF16)
            relay_part(o, 1).start()

    def reduced(o):
        if square:
            drain(relay_recv.at[o], r_recv.at[o])
            first = part[o, row, column, :, lower].astype(F32) + part_recv[o, 0, row].astype(F32)
            second = part[o, row, column, :, higher].astype(F32) + part_recv[o, 1, column].astype(F32)
            first = first + relay_recv[o, 0].astype(F32)
            second = second + relay_recv[o, 1].astype(F32)
            return jnp.concatenate([first, second], axis=1).astype(BF16)
        total = part[o, grp].astype(F32)
        drain(part_recv.at[1:groups, o], d_recv.at[o])
        for i in range(1, groups):
            total = total + part_recv[i, o].astype(F32)
        return total.astype(BF16)

    def send_reduced(j):
        part_sum[far(j)] = reduced(far(j))
        give_back(j)

    relays = both > 0
    weigh(me)
    gp_arrives(1)

    @pl.when(relays)
    def _():
        gp_arrives(2)

    @pl.loop(2, n - 2)
    def _(j):
        relayed(far(j))

    sides = jnp.where(helped == 0, last - chip, chip)

    def beyond(i):
        return jnp.where(helped == 0, chip + 1, chip - 1 - (sides - 1)) + i

    def complete(k):
        gp_completes(k)
        gp_crossed(near(2 * k + 1))

    soon = chips == 4
    outward = jnp.where(chip == 1, 2, 1)
    if assisted and soon:
        @pl.when(is_agent)
        def _():
            complete(outward)
            gp_crossed(partner)

    def help_out():
        drain(msg_end.at[: 2 * (chips - 2) - 1], end_sem)
        weigh_end(me)
        weigh_end(partner)

        @pl.loop(0, sides)
        def _(i):
            weigh_end(beyond(i) * 2)
            weigh_end(beyond(i) * 2 + 1)

        end_send[...] = end_sum[...].astype(BF16)
        help_end.start()

    if assisted and soon:
        pl.when(is_agent)(help_out)

    if not assisted:
        @pl.when(jnp.logical_not(relays))
        def _():
            gp_arrives(2)

    relayed(far(n - 2))
    relayed(far(n - 1))

    @pl.when(relays)
    def _():
        @pl.loop(3, chips)
        def _(k):
            gp_arrives(k)

    relayed(partner)
    relayed(me)

    @pl.loop(2, n)
    def _(j):
        send_reduced(j)

    if not assisted:
        @pl.when(jnp.logical_not(relays))
        def _():
            @pl.loop(3, chips)
            def _(k):
                gp_arrives(k)

    part_sum[partner] = reduced(partner)
    give_partner = pltpu.make_async_remote_copy(
        src_ref=part_sum.at[partner], dst_ref=part_back.at[me],
        send_sem=sent_sem.at[7], recv_sem=back_sem,
        device_id=(grp, partner), device_id_type=MESH,
    )
    give_partner.start()
    part_back[me] = reduced(me)
    if assisted:
        pl.when(is_inner)(sum_for_far_side)

    if assisted:
        @pl.when(is_end)
        def _():
            drain(msg_all.at[:3], msg_sem)

        @pl.when(jnp.logical_not(is_end))
        def _():
            drain(msg_all.at[: n - 1], msg_sem)
    else:
        drain(msg_all.at[: n - 1], msg_sem)

    reach = jnp.where(is_end, 2, chips) if assisted else chips
    waited = jnp.where(is_agent, outward, 0) if assisted and soon else 0

    @pl.loop(1, reach)
    def _(k):
        @pl.when(k != waited)
        def _():
            gp_completes(k)

    @pl.loop(1, reach)
    def _(k):
        @pl.when(k != waited)
        def _():
            gp_crossed(near(2 * k + 1))

    if assisted and soon:
        @pl.when(is_end)
        def _():
            gp_crossed(partner)
    else:
        gp_crossed(partner)

    weigh(partner)

    @pl.loop(1, reach)
    def _(k):
        weigh(near(2 * k))
        weigh(near(2 * k + 1))

    if assisted and not soon:
        pl.when(is_agent)(help_out)

    for k in range(sections):
        grad_f[k] = jnp.zeros((quarter, width), F32)

    if assisted:
        for z in range(chips):
            direct = n - 1 - 4 * (z >= 2) - 4 * (z <= last - 2)

            @pl.when(chip == z)
            def _():
                drain(part_sum.at[:direct], back_sem)
    else:
        drain(part_sum.at[: n - 1], back_sem)

    @pl.loop(0, n)
    def _(t):
        def add():
            wanted = table[t, me]
            addend = part_back[t].astype(F32)
            for k in range(sections):
                grad_f[k] = grad_f[k] + addend * is_one(wanted == k)

        if assisted:
            pl.when(jnp.logical_not(crosses(me, t // 2)))(add)
        else:
            add()

    if assisted:
        for side, has in ((0, chip >= 2), (1, chip <= last - 2)):
            @pl.when(has)
            def _():
                drain(collected.at[side], collect_sem.at[side])
                grad_f[...] = grad_f[...] + collected[side].astype(F32)

        @pl.when(is_end)
        def _():
            help_end.wait_recv()
            grad_w[...] = grad_w[...] + end_recv[...].astype(F32)

    fetch_pair.wait_send()
    for z in range(chips):
        near_by = (z > 0) + (z < chips - 1)
        relayed = 2 * (0 < z < chips - 1)
        far = sum(abs(y - z) > 2 for y in range(chips))

        @pl.when(chip == z)
        def _():
            drain(gathered.at[: near_by + relayed + far + chips - 1], sent_sem.at[0])

    drain(fetched.at[: (n - 2) * (groups - 1) * quarter, :], sent_sem.at[1])
    drain(pre_recv.at[1:groups], sent_sem.at[2])
    drain(pre_recv.at[1:groups], sent_sem.at[3])
    if assisted:
        @pl.when(is_agent)
        def _():
            drain(msg_all.at[: n - 2], sent_sem.at[4])
            help_end.wait_send()

        @pl.when(jnp.logical_not(is_agent))
        def _():
            drain(msg_all.at[: n - 1], sent_sem.at[4])
    else:
        drain(msg_all.at[: n - 1], sent_sem.at[4])

    for z in range(chips):
        at_end = z in (0, last)
        climbs = z * (z + 1 <= last - assisted) + (z < last)
        descents = (last - z) * (z - 1 >= 0 + assisted) + (z > 0)
        climbs, descents = (climbs if z < last else 0), (descents if z > 0 else 0)
        if at_end:
            climbs, descents = int(z == 0), int(z == last)
        known = 1 if at_end and assisted else last
        doubled = int(at_end and assisted and square)
        swapped = known - (assisted and z in (1, last - 1))

        @pl.when(chip == z)
        def _():
            if square:
                drain(fetched.at[: (climbs + descents + doubled) * span, :], sent_sem.at[5])
                drain(fetched.at[: swapped * span, :], sent_sem.at[8])
            else:
                drain(gp_full.at[: climbs + descents], sent_sem.at[5])
            drain(gp_full.at[: known + 1], sent_sem.at[9])

    if square:
        drain(part_recv, sent_sem.at[6])
        drain(relay_recv, sent_sem.at[10])
    else:
        drain(part_recv.at[1:groups], sent_sem.at[6])
    if assisted:
        @pl.when(is_inner)
        def _():
            drain(part_sum.at[: n - 1 - far_chips], sent_sem.at[7])
            drain(gathered_sum, sent_sem.at[12])

        @pl.when(jnp.logical_not(is_inner))
        def _():
            drain(part_sum.at[: n - 1], sent_sem.at[7])
    else:
        drain(part_sum.at[: n - 1], sent_sem.at[7])


def hand_over(*refs):
    copies = [pltpu.make_async_copy(refs[k], refs[3 + k], refs[6].at[k]) for k in range(3)]
    for copy in copies:
        copy.start()
    for copy in copies:
        copy.wait()


def per_device(
    n, groups,
    features, weights, bias, cotangent, tile_values, tile_count, tile_slot, source_blocks,
):
    rows, width = features.shape
    relations, _, slot_total, blk = tile_values.shape
    sections = rows // blk
    quarter, share, chunk, chips = blk // groups, width // groups, width // n, n // 2
    half = rows // 2
    square = groups == 4
    grid = (2, 2) if square else (groups,)
    vmem = pl.BlockSpec(memory_space=pltpu.VMEM)
    smem = pl.BlockSpec(memory_space=pltpu.SMEM)
    anywhere = pl.BlockSpec(memory_space=pl.ANY)
    hbm = pl.BlockSpec(memory_space=pltpu.HBM)
    dma = pltpu.SemaphoreType.DMA
    out, grad_w, grad_f = pl.pallas_call(
        functools.partial(kernel, n, groups),
        out_shape=(
            pltpu.VMEM((share, rows), BF16),
            pltpu.VMEM((relations, chunk, width), F32),
            pltpu.VMEM((sections, quarter, width), F32),
        ),
        in_specs=[smem, smem, smem, hbm, hbm, vmem, hbm, hbm],
        out_specs=(vmem, vmem, vmem),
        scratch_shapes=[
            pltpu.VMEM((relations, width, width), BF16),
            pltpu.VMEM((relations, rows * slot_total, blk), jnp.int32),
            pltpu.VMEM((sections, groups, quarter, width), BF16),
            pltpu.VMEM((rows, width), BF16),
            pltpu.VMEM((n, sections, quarter, width), BF16),
            pltpu.VMEM((blk, width), BF16),
            pltpu.VMEM((slot_total, blk, blk), BF16),
            pltpu.VMEM((slot_total, blk, blk), BF16),
            pltpu.VMEM((n * blk, width), BF16),
            pltpu.VMEM((relations * rows, n * blk), BF16),
            pltpu.VMEM((relations * rows, 128), F32),
            pltpu.VMEM((relations, width, rows), F32),
            pltpu.VMEM((relations * rows, width), BF16),
            pltpu.VMEM((n, relations, chunk, rows), BF16),
            pltpu.VMEM((n, relations, chunk, rows), BF16),
            pltpu.VMEM((n, relations, chunk, rows), BF16),
            pltpu.VMEM((relations, chunk, width), F32),
            pltpu.VMEM((relations, chunk, width), BF16),
            pltpu.VMEM((relations, chunk, width), BF16),
            pltpu.VMEM((n * blk, relations * rows), BF16),
            pltpu.VMEM((rows, width), F32),
            pltpu.VMEM((groups, half, 2 * share), BF16),
            pltpu.VMEM((groups, half, 2 * share), BF16),
            pltpu.VMEM((half, 2 * share), F32),
            pltpu.VMEM((half, 2 * share), F32),
            pltpu.VMEM((1, 2 * share), F32),
            pltpu.VMEM((groups, half, 2 * share), BF16),
            pltpu.VMEM((n, rows, width), BF16),
            pltpu.VMEM((relations * rows, width), BF16),
            pltpu.VMEM((n, *grid, quarter, width), BF16),
            pltpu.VMEM((n, 2, 2, quarter, width // 2) if square else (groups, n, quarter, width), BF16),
            pltpu.VMEM((n, 2, quarter, width // 2), BF16),
            pltpu.VMEM((n, 2, quarter, width // 2), BF16),
            pltpu.VMEM((n, quarter, width), BF16),
            pltpu.VMEM((n, quarter, width), BF16),
            pltpu.VMEM((2, chips - 2, quarter, width), BF16),
            pltpu.VMEM((chips - 2, quarter, width), BF16),
            pltpu.VMEM((chips - 2, sections, quarter, width), BF16),
            pltpu.VMEM((2, sections, quarter, width), BF16),
            dma((4,)), dma((2,)), dma((13,)), dma, dma, dma, dma, dma, dma, dma((2,)),
            dma((n, 2)), dma((n, 2, 2)),
            dma((2,)), dma((2,)), dma((n,)), dma((n,)), dma,
            dma((chips,)), dma((chips,)), dma((chips,)),
        ],
        compiler_params=pltpu.CompilerParams(
            collective_id=0, has_side_effects=True, vmem_limit_bytes=60 << 20
        ),
        name="layer",
    )(
        source_blocks, tile_count, tile_slot,
        features.reshape(sections, groups, quarter, width), cotangent, bias,
        tile_values.reshape(relations, rows * slot_total, blk), weights,
    )
    results = (out, grad_w, grad_f)
    out, grad_w, grad_f = pl.pallas_call(
        hand_over,
        out_shape=tuple(jax.ShapeDtypeStruct(x.shape, x.dtype) for x in results),
        in_specs=[vmem] * 3,
        out_specs=(anywhere,) * 3,
        scratch_shapes=[dma((3,))],
        compiler_params=pltpu.CompilerParams(vmem_limit_bytes=4 << 20),
        name="hand_over",
    )(*results)
    return (out.T, grad_w, grad_f)


def solution(mesh):
    placed = (
        P("tgt", None),
        P("rel", None, None),
        P(),
        P("tgt", None),
        P("rel", "tgt", None, None),
        P("rel", "tgt"),
        P("rel", "tgt", None),
        P(),
    )
    return jax.shard_map(
        functools.partial(per_device, mesh.shape["tgt"], mesh.shape["rel"]),
        mesh=mesh,
        in_specs=placed,
        out_specs=(P("tgt", "rel"), P("rel", "tgt", None), P("tgt", "rel", None)),
        check_vma=False,
    )
```

```python
import functools

import jax
import jax.numpy as jnp
from jax import lax
from jax.experimental import pallas as pl
from jax.experimental.pallas import tpu as pltpu
from jax.sharding import PartitionSpec as P

MESH = pl.DeviceIdType.MESH
F32 = jnp.float32
BF16 = jnp.bfloat16


def aligned(start, size, multiple):
    return pl.ds(pl.multiple_of(start, multiple), size)


def is_one(condition):
    return condition.astype(jnp.int32).astype(F32)


def pack(value, first, width):
    half = value.shape[0] // 2
    return jnp.concatenate(
        [value[:half, first : first + width], value[half:, first : first + width]], axis=1
    )


def drain(view, semaphore):
    pltpu.make_async_copy(view, view, semaphore).wait()


def kernel(
    n, groups,
    table, counts, slots,
    feat_hbm, cot_hbm, bias, values_hbm, weights_hbm,
    out, grad_w, grad_f,
    weights, values, feat, cot, gathered, partner_staged, masked, masked_t, fetched, adj, scale, turned_scratch, msg, msg_t, msg_all, msg_end, end_sum, end_send, end_recv, adj_t, pre,
    pre_send, pre_recv, cot_own, active, bias_own, gp_all, gp_full, gm,
    part, part_recv, relay, relay_recv, part_sum, part_back, inbox, crossed, gathered_sum, collected,
    load_sem, pair_sem, sent_sem, spread_sem, back_sem, end_sem, help_sem, inbox_sem, crossed_sem, collect_sem, slab_sem, cross_slab_sem,
    a_recv, b_recv, p_recv, g_recv, d_recv, r_recv, msg_sem, line_sem, other_sem, across_sem,
):
    me = lax.axis_index("tgt")
    grp = lax.axis_index("rel")
    sections, _, quarter, width = feat.shape
    blk = quarter * groups
    rows = sections * blk
    relations = weights.shape[0]
    slot_total = slots.shape[2]
    share = width // groups
    chips = n // 2
    chip, core = me // 2, lax.rem(me, 2)

    def tgt(j):
        return lax.rem(chip + j // 2, chips) * 2 + lax.rem(core + lax.rem(j, 2), 2)

    below, above_me = chip, chips - 1 - chip
    both = jnp.minimum(below, above_me)
    assisted = chips == 4 or chips > 5
    last = chips - 1
    is_end = (chip == 0) | (chip == last)
    agent_low, agent_high = 2, last - 2
    soon = chips == 4
    sliced = soon and groups == 4
    outward = jnp.where(chip == 1, 2, 1)
    outer_chip = jnp.where(chip == 1, 0, last)
    helped = jnp.where(chip == agent_low, 0, last)
    is_agent = (chip == agent_low) | (chip == agent_high)

    def near(j):
        k = j // 2 - 1
        two_sided = jnp.where(lax.rem(k, 2) == 0, chip + k // 2 + 1, chip - k // 2 - 1)
        distance = k - both + 1
        one_sided = jnp.where(above_me > below, chip + distance, chip - distance)
        return jnp.where(k < 2 * both, two_sided, one_sided) * 2 + lax.rem(core + lax.rem(j, 2), 2)

    partner = chip * 2 + 1 - core
    row, column = grp // 2, lax.rem(grp, 2)
    beside = row * 2 + 1 - column
    above = (1 - row) * 2 + column

    square = groups == 4

    def rel(i):
        if square:
            return (grp, beside, above, (1 - row) * 2 + 1 - column)[i]
        return lax.rem(grp + i, groups)

    load_w = pltpu.make_async_copy(weights_hbm, weights, load_sem.at[0])
    load_v = pltpu.make_async_copy(values_hbm, values, load_sem.at[1])
    load_f = pltpu.make_async_copy(feat_hbm, feat, load_sem.at[2])
    load_c = pltpu.make_async_copy(cot_hbm, cot, load_sem.at[3])
    load_f.start()
    load_v.start()
    load_w.start()
    load_c.start()

    barrier = pltpu.get_barrier_semaphore()

    @pl.loop(1, n)
    def _(j):
        pl.semaphore_signal(barrier, inc=1, device_id=(grp, tgt(j)), device_id_type=MESH)

    for i in range(1, groups):
        pl.semaphore_signal(barrier, inc=1, device_id=(rel(i), me), device_id_type=MESH)

    def whole_block(t):
        total = jnp.zeros((blk, width), F32)
        for k in range(sections):
            total = total + feat[k].reshape(blk, width).astype(F32) * is_one(table[t, me] == k)
        return total.astype(BF16)

    pl.semaphore_wait(barrier, n - 1 + groups - 1)

    cut = width // 2

    def columns(h):
        return aligned(h * cut, cut, 128)

    def climb_rows(o, h, source):
        return pltpu.make_async_remote_copy(
            src_ref=source, dst_ref=gathered.at[o, :, :, columns(h)],
            send_sem=sent_sem.at[0], recv_sem=a_recv.at[o, h],
            device_id=(grp, jnp.minimum(chip + 1, chips - 1) * 2 + core), device_id_type=MESH,
        )

    def descend_rows(o, h, source):
        return pltpu.make_async_remote_copy(
            src_ref=source, dst_ref=gathered.at[o, :, :, columns(h)],
            send_sem=sent_sem.at[0], recv_sem=a_recv.at[o, h],
            device_id=(grp, jnp.maximum(chip - 1, 0) * 2 + core), device_id_type=MESH,
        )

    def across_rows(o, h):
        return pltpu.make_async_remote_copy(
            src_ref=gathered.at[o, :, :, columns(h)], dst_ref=gathered.at[o, :, :, columns(h)],
            send_sem=sent_sem.at[0], recv_sem=a_recv.at[o, h],
            device_id=(grp, partner), device_id_type=MESH,
        )

    fetch_pair = pltpu.make_async_remote_copy(
        src_ref=partner_staged, dst_ref=fetched.at[aligned(me * blk, blk, blk), :],
        send_sem=pair_sem.at[0], recv_sem=pair_sem.at[1],
        device_id=(grp, partner), device_id_type=MESH,
    )

    def leap_rows(z, h):
        return pltpu.make_async_remote_copy(
            src_ref=feat_hbm.at[:, grp, :, columns(h)], dst_ref=gathered.at[me, :, :, columns(h)],
            send_sem=sent_sem.at[0], recv_sem=a_recv.at[me, h],
            device_id=(grp, z * 2 + core), device_id_type=MESH,
        )

    for h in range(2):
        @pl.when(chip < chips - 1)
        def _():
            climb_rows(me, h, feat_hbm.at[:, grp, :, columns(h)]).start()

        @pl.when(chip > 0)
        def _():
            descend_rows(me, h, feat_hbm.at[:, grp, :, columns(h)]).start()

    @pl.loop(0, chips)
    def _(z):
        @pl.when((z > chip + 2) | (z < chip - 2))
        def _():
            for h in range(2):
                leap_rows(z, h).start()

    load_f.wait()
    partner_staged[...] = whole_block(partner)
    fetch_pair.start()
    fetched[aligned(me * blk, blk, blk), :] = whole_block(me)

    sent = range(4) if square else range(groups - 1)

    def spread(j, h, way):
        if square:
            size = quarter if way < 2 else quarter // 2
            source = (grp, grp, beside, above)[way]
            extra = quarter // 2 if way == 3 else 0
            peer = (beside, above, above, beside)[way]
        else:
            size, source, extra, peer = quarter, grp, 0, rel(way + 1)
        rows_at = aligned(near(j) * blk + source * quarter + extra, size, size)
        return pltpu.make_async_remote_copy(
            src_ref=fetched.at[rows_at, columns(h)], dst_ref=fetched.at[rows_at, columns(h)],
            send_sem=sent_sem.at[1],
            recv_sem=b_recv.at[j, h, way] if square and way < 2 else spread_sem,
            device_id=(peer, me), device_id_type=MESH,
        )

    first_hop = sent[:2] if square else sent

    def event(e):
        inner = lax.rem(e, 4)
        paired = e < 4 * both
        k = jnp.where(paired, e // 4 * 2 + 1 + lax.rem(inner, 2), e // 2 + 1)
        return k, jnp.where(paired, inner // 2, lax.rem(e, 2))

    def pass_on(e, side):
        k, h = event(e)
        j = 2 * k + side
        if not square:
            return
        spread(j, h, 0).wait_recv()
        spread(j, h, 2).start()
        spread(j, h, 1).wait_recv()
        spread(j, h, 3).start()

    def placed(j, h):
        o = near(j)
        total = jnp.zeros((quarter, cut), F32)
        for k in range(sections):
            total = total + gathered[o, k, :, columns(h)].astype(F32) * is_one(table[me, o] == k)
        fetched[aligned(o * blk + grp * quarter, quarter, quarter), columns(h)] = total.astype(BF16)
        for way in first_hop:
            spread(j, h, way).start()

    def arrive(e):
        k, h = event(e)
        o = near(2 * k)
        across_rows(o, h).wait_recv()

        @pl.when((o // 2 == chip - 1) & (chip < chips - 1))
        def _():
            climb_rows(o, h, gathered.at[o, :, :, columns(h)]).start()

        @pl.when((o // 2 == chip + 1) & (chip > 0))
        def _():
            descend_rows(o, h, gathered.at[o, :, :, columns(h)]).start()

        across_rows(o, h).start()
        placed(2 * k, h)

    def arrive_across(e):
        k, h = event(e)
        across_rows(near(2 * k + 1), h).wait_recv()
        placed(2 * k + 1, h)

    load_v.wait()

    def adjacency(b):
        r, q = b // sections, lax.rem(b, sections)
        count = counts[r, q]
        total = jnp.zeros((blk, blk), F32)
        for s in range(slot_total):
            start = (q * blk * slot_total) + s
            tile = values[r, pl.ds(start, blk, stride=slot_total), :].astype(F32) * is_one(s < count)
            masked[s] = tile.astype(BF16)
            masked_t[s] = tile.T.astype(BF16)
            total = total + tile
        degree = jnp.sum(total, axis=1, keepdims=True)
        root = 1.0 / jnp.sqrt(jnp.maximum(degree, 1.0))
        scale[aligned(b * blk, blk, blk), :] = jnp.broadcast_to(root, (blk, 128))

        @pl.loop(0, n)
        def _(o):
            entry = jnp.zeros((blk, blk), BF16)
            entry_t = jnp.zeros((blk, blk), BF16)
            for s in range(slot_total):
                here = jnp.full((blk, blk), is_one(slots[r, q, s] == o), F32).astype(BF16)
                entry = entry + masked[s] * here
                entry_t = entry_t + masked_t[s] * here
            adj[aligned(b * blk, blk, blk), aligned(o * blk, blk, blk)] = entry
            adj_t[aligned(o * blk, blk, blk), aligned(b * blk, blk, blk)] = entry_t

    blocks = relations * sections

    @pl.loop(0, blocks // 2)
    def _(b):
        adjacency(b)

    events = 2 * (chips - 1)
    arrive(0)
    arrive(1)

    @pl.loop(0, blocks // 2)
    def _(b):
        adjacency(blocks // 2 + b)
        arrive_across(b)
        arrive(2 + b)

    @pl.loop(blocks // 2 + 2, events)
    def _(e):
        arrive(e)
        arrive_across(e - 2)

    pass_on(0, 0)
    arrive_across(events - 2)
    pass_on(0, 1)
    arrive_across(events - 1)

    @pl.loop(1, events)
    def _(e):
        pass_on(e, 0)
        pass_on(e, 1)

    load_w.wait()
    fetch_pair.wait_recv()

    late = n - 2 if square else (n - 2) * (groups - 1)
    drain(fetched.at[: late * quarter, :], spread_sem)

    tile_width = 256
    chunk = width // n
    for c in range(width // tile_width):
        at = slice(c * tile_width, (c + 1) * tile_width)
        acc = jnp.dot(adj[...], fetched[:, at], preferred_element_type=F32) * scale[:, 0:1]
        msg[:, at] = acc.astype(BF16)
        for r in range(relations):
            turned_scratch[r, at, :] = acc[r * rows : (r + 1) * rows, :].T

    for r in range(relations):
        msg_t[:, r] = turned_scratch[r].reshape(n, chunk, rows).astype(BF16)

    def send_messages(target, z, landing, semaphore):
        return pltpu.make_async_remote_copy(
            src_ref=msg_t.at[target], dst_ref=landing.at[me],
            send_sem=sent_sem.at[4], recv_sem=semaphore,
            device_id=(grp, z * 2 + lax.rem(target, 2)), device_id_type=MESH,
        )

    def start_messages(j):
        target = near(j)
        z = target // 2
        if not assisted:
            send_messages(target, z, msg_all, msg_sem).start()
            return
        away = ((z == 0) & (chip >= agent_low)) | ((z == last) & (chip <= agent_high))

        @pl.when(jnp.logical_not(away))
        def _():
            send_messages(target, z, msg_all, msg_sem).start()

        agent = jnp.where(z == 0, agent_low, agent_high)

        @pl.when(away & jnp.logical_not((agent == chip) & (lax.rem(target, 2) == core)))
        def _():
            send_messages(target, agent, msg_end, end_sem).start()

    @pl.loop(4, n)
    def _(j):
        start_messages(n + 3 - j)

    def start_next_messages():
        start_messages(2)
        start_messages(3)

    pl.when(jnp.logical_not(is_end))(start_next_messages)

    send_messages(partner, chip, msg_all, msg_sem).start()
    msg_all[me] = msg_t[me]
    if assisted:
        msg_end[me] = msg_t[helped * 2 + core]

    @pl.loop(0, width // tile_width)
    def _(c):
        at = aligned(c * tile_width, tile_width, tile_width)
        total = None
        for r in range(relations):
            part_r = jnp.dot(
                msg[r * rows : (r + 1) * rows, :], weights[r, :, at], preferred_element_type=F32
            )
            total = part_r if total is None else total + part_r
        pre[:, at] = total

    whole = pre[...]
    for k in range(groups):
        pre_send[k] = pack(whole, k * share, share).astype(BF16)

    pieces = 4
    piece_rows = rows // 2 // pieces

    def reduce_pre(i, p):
        at = slice(p * piece_rows, (p + 1) * piece_rows)
        return pltpu.make_async_remote_copy(
            src_ref=pre_send.at[rel(i), at, :], dst_ref=pre_recv.at[i, at, :],
            send_sem=sent_sem.at[2], recv_sem=p_recv.at[p],
            device_id=(rel(i), me), device_id_type=MESH,
        )

    for p in range(pieces):
        for i in range(1, groups):
            reduce_pre(i, p).start()

    load_c.wait()
    for k in range(groups):
        @pl.when(grp == k)
        def _():
            cot_own[...] = pack(cot[...].astype(F32), k * share, share)
            piece = bias[...].reshape(1, width)[:, k * share : (k + 1) * share]
            bias_own[...] = jnp.concatenate([piece, piece], axis=1)

    def gather_gp(i, p):
        at = slice(p * piece_rows, (p + 1) * piece_rows)
        return pltpu.make_async_remote_copy(
            src_ref=gp_all.at[grp, at, :], dst_ref=gp_all.at[grp, at, :],
            send_sem=sent_sem.at[3], recv_sem=g_recv.at[p],
            device_id=(rel(i), me), device_id_type=MESH,
        )

    for p in range(pieces):
        at = slice(p * piece_rows, (p + 1) * piece_rows)
        total = pre_send[grp, at, :].astype(F32)
        drain(pre_recv.at[1:groups, at, :], p_recv.at[p])
        for i in range(1, groups):
            total = total + pre_recv[i, at, :].astype(F32)
        pre_act = total + bias_own[...]
        sigmoid = jax.nn.sigmoid(pre_act)
        derivative = sigmoid * (1.0 + pre_act * (1.0 - sigmoid))
        gp_all[grp, at, :] = (cot_own[at, :] * derivative).astype(BF16)
        for i in range(1, groups):
            gather_gp(i, p).start()
        active[at, :] = pre_act * sigmoid

    upright = active[...].T
    for h in range(2):
        out[:, h * (rows // 2) : (h + 1) * (rows // 2)] = upright[h * share : (h + 1) * share].astype(BF16)

    half = rows // 2
    for p in range(pieces):
        at = slice(p * piece_rows, (p + 1) * piece_rows)
        drain(pre_recv.at[1:groups, at, :], g_recv.at[p])
        for h in range(2):
            gp_full[me, h * half + p * piece_rows : h * half + (p + 1) * piece_rows, :] = jnp.concatenate(
                [gp_all[k, at, h * share : (h + 1) * share].astype(F32) for k in range(groups)], axis=1
            ).astype(BF16)

    if square:
        span, mine, other = half, jnp.where(core == 0, column, row), jnp.where(core == 0, beside, above)
    else:
        span, mine, other = rows, 0, grp

    def piece_of(o, part_of):
        return gp_full.at[o, aligned(part_of * span, span, span), :]

    def climb_gp(o):
        return pltpu.make_async_remote_copy(
            src_ref=piece_of(o, mine), dst_ref=piece_of(o, mine),
            send_sem=sent_sem.at[5], recv_sem=line_sem.at[o // 2],
            device_id=(grp, jnp.minimum(chip + 1, chips - 1) * 2 + core), device_id_type=MESH,
        )

    def descend_gp(o):
        return pltpu.make_async_remote_copy(
            src_ref=piece_of(o, mine), dst_ref=piece_of(o, mine),
            send_sem=sent_sem.at[5], recv_sem=line_sem.at[o // 2],
            device_id=(grp, jnp.maximum(chip - 1, 0) * 2 + core), device_id_type=MESH,
        )

    def exchange_gp(o):
        return pltpu.make_async_remote_copy(
            src_ref=piece_of(o, mine), dst_ref=piece_of(o, mine),
            send_sem=sent_sem.at[8], recv_sem=other_sem.at[o // 2],
            device_id=(other, me), device_id_type=MESH,
        )

    def across_gp(o, part_of):
        return pltpu.make_async_remote_copy(
            src_ref=piece_of(o, part_of), dst_ref=piece_of(o, part_of),
            send_sem=sent_sem.at[9], recv_sem=across_sem.at[o // 2],
            device_id=(grp, partner), device_id_type=MESH,
        )

    whole_end = assisted and square
    next_in = jnp.where(chip == 0, 1, last - 1)

    def slab(o, c):
        return gp_full.at[o, :, columns(c)]

    def across_slab(o, c):
        return pltpu.make_async_remote_copy(
            src_ref=slab(o, c), dst_ref=slab(o, c),
            send_sem=sent_sem.at[9], recv_sem=cross_slab_sem.at[c],
            device_id=(grp, partner), device_id_type=MESH,
        )

    def beside_end(o):
        return ((o // 2 == 0) & (chip == 1)) | ((o // 2 == last) & (chip == last - 1))

    along = jnp.logical_not(is_end) if sliced else chip >= 0

    @pl.when(along & (chip < chips - 1))
    def _():
        climb_gp(me).start()

    @pl.when(along & (chip > 0))
    def _():
        descend_gp(me).start()

    if sliced:
        @pl.when(is_end)
        def _():
            for c in range(2):
                pltpu.make_async_remote_copy(
                    src_ref=slab(me, c), dst_ref=slab(me, c),
                    send_sem=sent_sem.at[5], recv_sem=slab_sem.at[c],
                    device_id=(grp, next_in * 2 + core), device_id_type=MESH,
                ).start()
    elif whole_end:
        @pl.when(is_end)
        def _():
            pltpu.make_async_remote_copy(
                src_ref=piece_of(me, 1 - mine), dst_ref=piece_of(me, 1 - mine),
                send_sem=sent_sem.at[5], recv_sem=other_sem.at[chip],
                device_id=(grp, next_in * 2 + core), device_id_type=MESH,
            ).start()

    for h in range(rows // span):
        across_gp(me, h).start()


    def gp_arrives(k):
        o = near(2 * k)
        climb_gp(o).wait_recv()

        @pl.when((o < me) & (chip < last - assisted))
        def _():
            climb_gp(o).start()

        @pl.when((o > me) & (chip > 0 + assisted))
        def _():
            descend_gp(o).start()

        if whole_end:
            @pl.when(jnp.logical_not(beside_end(o)))
            def _():
                exchange_gp(o).start()
        elif square:
            exchange_gp(o).start()
        across_gp(o, mine).start()

    def gp_completes(k):
        if square:
            o = near(2 * k)
            pltpu.make_async_remote_copy(
                src_ref=piece_of(o, 1 - mine), dst_ref=piece_of(o, 1 - mine),
                send_sem=sent_sem.at[8], recv_sem=other_sem.at[o // 2],
                device_id=(other, me), device_id_type=MESH,
            ).wait_recv()
            across_gp(o, 1 - mine).start()

    def gp_crossed(o):
        drain(gp_full.at[o], across_sem.at[o // 2])

    def weigh(o):
        chunk = width // n
        if chunk % 16 == 0:
            product = jnp.dot(
                msg_all[o].reshape(relations * chunk, rows), gp_full[o], preferred_element_type=F32
            )
            grad_w[...] = grad_w[...] + product.reshape(relations, chunk, width)
        else:
            for r in range(relations):
                grad_w[r] = grad_w[r] + jnp.dot(msg_all[o, r], gp_full[o], preferred_element_type=F32)

    def weigh_end(o):
        for r in range(relations):
            end_sum[r] = end_sum[r] + jnp.dot(msg_end[o, r], gp_full[o], preferred_element_type=F32)

    grad_w[...] = jnp.zeros(grad_w.shape, F32)
    end_sum[...] = jnp.zeros(end_sum.shape, F32)
    help_end = pltpu.make_async_remote_copy(
        src_ref=end_send, dst_ref=end_recv,
        send_sem=sent_sem.at[11], recv_sem=help_sem,
        device_id=(grp, helped * 2 + core), device_id_type=MESH,
    )

    @pl.loop(0, width // tile_width)
    def _(c):
        at = aligned(c * tile_width, tile_width, tile_width)
        for r in range(relations):
            rows_r = slice(r * rows, (r + 1) * rows)
            grads = lax.dot_general(
                gp_full[me], weights[r, at, :],
                (((1,), (1,)), ((), ())), preferred_element_type=F32,
            )
            gm[rows_r, at] = (grads * scale[rows_r, 0:1]).astype(BF16)

    lower, higher = slice(0, cut), slice(cut, width)

    def far(j):
        return near(n - j + 2 * lax.rem(j, 2))

    def reduce_part(o, i):
        if square:
            source = part.at[o, :, 1 - column, :, lower] if i == 1 else part.at[o, 1 - row, :, :, higher]
            target, peer = part_recv.at[o, i - 1], (beside, above)[i - 1]
        else:
            source, target, peer = part.at[o, rel(i)], part_recv.at[i, o], rel(i)
        return pltpu.make_async_remote_copy(
            src_ref=source, dst_ref=target,
            send_sem=sent_sem.at[6], recv_sem=d_recv.at[o],
            device_id=(peer, me), device_id_type=MESH,
        )

    def relay_part(o, w):
        return pltpu.make_async_remote_copy(
            src_ref=relay.at[o, w], dst_ref=relay_recv.at[o, w],
            send_sem=sent_sem.at[10], recv_sem=r_recv.at[o],
            device_id=((above, beside)[w], me), device_id_type=MESH,
        )

    def start_parts(z):
        product = jnp.dot(
            adj_t[aligned(z * 2 * blk, 2 * blk, blk), :], gm[...], preferred_element_type=F32
        )
        for v in range(2):
            o = z * 2 + v
            part[o] = product[v * blk : (v + 1) * blk].astype(BF16).reshape(part.shape[1:])
            for i in range(1, 3 if square else groups):
                reduce_part(o, i).start()

    @pl.loop(1, chips)
    def _(e):
        start_parts(near(n - 2 * e) // 2)

    far_chips = chips - 2
    is_inner = (chip == 1) | (chip == last - 1)
    low_side = chip <= 1

    def crosses(o, source):
        return ((source <= 1) & (o // 2 >= 2)) | ((source >= last - 1) & (o // 2 <= last - 2))

    def hand(o, device, landing, semaphore):
        return pltpu.make_async_remote_copy(
            src_ref=part_sum.at[o], dst_ref=landing,
            send_sem=sent_sem.at[7], recv_sem=semaphore,
            device_id=(grp, device), device_id_type=MESH,
        )

    def give_back(j):
        o = far(j)
        if not assisted:
            hand(o, o, part_back.at[me], back_sem).start()
            return
        slot = jnp.where(low_side, jnp.maximum(o // 2 - 2, 0), jnp.minimum(o // 2, far_chips - 1))
        odd = lax.rem(o, 2)
        over = crosses(o, chip)

        @pl.when(over & is_end)
        def _():
            hand(o, next_in * 2 + odd, inbox.at[slot, core], inbox_sem.at[slot]).start()

        @pl.when(over & is_inner & (odd != core))
        def _():
            hand(o, partner, crossed.at[slot], crossed_sem.at[slot]).start()

        @pl.when(jnp.logical_not(over & (is_end | is_inner)))
        def _():
            hand(o, o, part_back.at[me], back_sem).start()

    def collect(slot):
        z = jnp.where(low_side, slot + 2, slot)
        side = jnp.where(low_side, 0, 1)
        return pltpu.make_async_remote_copy(
            src_ref=gathered_sum.at[slot], dst_ref=collected.at[side],
            send_sem=sent_sem.at[12], recv_sem=collect_sem.at[side],
            device_id=(grp, z * 2 + core), device_id_type=MESH,
        )

    def sum_for_far_side():
        outer = jnp.where(low_side, 0, last)

        @pl.loop(0, far_chips)
        def _(i):
            slot = jnp.where(low_side, far_chips - 1 - i, i)
            drain(crossed.at[slot], crossed_sem.at[slot])
            drain(inbox.at[slot], inbox_sem.at[slot])
            o = jnp.where(low_side, slot + 2, slot) * 2 + core
            terms = (
                (me, part_sum[o].astype(F32)),
                (partner, crossed[slot].astype(F32)),
                (outer * 2, inbox[slot, 0].astype(F32)),
                (outer * 2 + 1, inbox[slot, 1].astype(F32)),
            )
            for k in range(sections):
                total = None
                for t, term in terms:
                    kept = term * is_one(table[t, o] == k)
                    total = kept if total is None else total + kept
                gathered_sum[slot, k] = total.astype(BF16)
            collect(slot).start()

    def relayed(o):
        if square:
            drain(part_recv.at[o], d_recv.at[o])
            up = part[o, 1 - row, column, :, lower].astype(F32) + part_recv[o, 0, 1 - row].astype(F32)
            relay[o, 0] = up.astype(BF16)
            relay_part(o, 0).start()
            aside = part[o, row, 1 - column, :, higher].astype(F32) + part_recv[o, 1, 1 - column].astype(F32)
            relay[o, 1] = aside.astype(BF16)
            relay_part(o, 1).start()

    def reduced(o):
        if square:
            drain(relay_recv.at[o], r_recv.at[o])
            first = part[o, row, column, :, lower].astype(F32) + part_recv[o, 0, row].astype(F32)
            second = part[o, row, column, :, higher].astype(F32) + part_recv[o, 1, column].astype(F32)
            first = first + relay_recv[o, 0].astype(F32)
            second = second + relay_recv[o, 1].astype(F32)
            return jnp.concatenate([first, second], axis=1).astype(BF16)
        total = part[o, grp].astype(F32)
        drain(part_recv.at[1:groups, o], d_recv.at[o])
        for i in range(1, groups):
            total = total + part_recv[i, o].astype(F32)
        return total.astype(BF16)

    def send_reduced(j):
        part_sum[far(j)] = reduced(far(j))
        give_back(j)

    relays = both > 0
    weigh(me)

    def slab_arrives(c):
        drain(slab(outer_chip * 2 + core, c), slab_sem.at[c])
        outer = outer_chip * 2 + core
        across_slab(outer, c).start()
        ahead = gp_full.at[outer, aligned(mine * span, span, span), columns(c)]
        pltpu.make_async_remote_copy(
            src_ref=ahead, dst_ref=ahead,
            send_sem=sent_sem.at[5], recv_sem=line_sem.at[outer_chip],
            device_id=(grp, jnp.where(chip == 1, 2, last - 2) * 2 + core), device_id_type=MESH,
        ).start()

    def help_slab(c):
        other = outer_chip * 2 + 1 - core
        drain(slab(other, c), cross_slab_sem.at[c])
        for r in range(relations):
            total = None
            for o in (me, partner, outer_chip * 2 + core, other):
                product = jnp.dot(msg_end[o, r], gp_full[o, :, c * cut : (c + 1) * cut], preferred_element_type=F32)
                total = product if total is None else total + product
            end_send[r, :, c * cut : (c + 1) * cut] = total.astype(BF16)
        pltpu.make_async_remote_copy(
            src_ref=end_send.at[:, :, columns(c)], dst_ref=end_recv.at[:, :, columns(c)],
            send_sem=sent_sem.at[11], recv_sem=help_sem,
            device_id=(grp, helped * 2 + core), device_id_type=MESH,
        ).start()

    if sliced:
        @pl.when(is_end)
        def _():
            gp_arrives(1)

            @pl.loop(2, n - 2)
            def _(j):
                relayed(far(j))

        @pl.when(jnp.logical_not(is_end))
        def _():
            gp_arrives(3 - outward)
            slab_arrives(0)
            relayed(far(2))
            relayed(far(3))
            gp_crossed(partner)
            drain(msg_end.at[: 2 * (chips - 2) - 1], end_sem)
            help_slab(0)
            slab_arrives(1)
            relayed(far(4))
            relayed(far(5))
            help_slab(1)
    else:
        gp_arrives(1)

        @pl.when(relays)
        def _():
            gp_arrives(2)

        @pl.loop(2, n - 2)
        def _(j):
            relayed(far(j))

    start_parts(chip)

    sides = jnp.where(helped == 0, last - chip, chip)

    def beyond(i):
        return jnp.where(helped == 0, chip + 1, chip - 1 - (sides - 1)) + i

    def complete(k):
        gp_completes(k)
        gp_crossed(near(2 * k + 1))

    if assisted and soon and not sliced:
        @pl.when(is_agent)
        def _():
            complete(outward)
            gp_crossed(partner)

    def help_out():
        drain(msg_end.at[: 2 * (chips - 2) - 1], end_sem)
        weigh_end(me)
        weigh_end(partner)

        @pl.loop(0, sides)
        def _(i):
            weigh_end(beyond(i) * 2)
            weigh_end(beyond(i) * 2 + 1)

        end_send[...] = end_sum[...].astype(BF16)
        help_end.start()

    if assisted and soon and not sliced:
        pl.when(is_agent)(help_out)

    pl.when(is_end)(start_next_messages)
    if not assisted:
        @pl.when(jnp.logical_not(relays))
        def _():
            gp_arrives(2)

    relayed(far(n - 2))
    relayed(far(n - 1))

    if not sliced:
        @pl.when(relays)
        def _():
            @pl.loop(3, chips)
            def _(k):
                gp_arrives(k)


    @pl.loop(2, n - 2)
    def _(j):
        send_reduced(j)

    if sliced:
        pl.when(relays)(lambda: gp_arrives(3))

    relayed(partner)
    relayed(me)
    send_reduced(n - 2)
    send_reduced(n - 1)

    if not assisted:
        @pl.when(jnp.logical_not(relays))
        def _():
            @pl.loop(3, chips)
            def _(k):
                gp_arrives(k)

    if assisted:
        pl.when(is_inner)(sum_for_far_side)

    part_sum[partner] = reduced(partner)
    give_partner = pltpu.make_async_remote_copy(
        src_ref=part_sum.at[partner], dst_ref=part_back.at[me],
        send_sem=sent_sem.at[7], recv_sem=back_sem,
        device_id=(grp, partner), device_id_type=MESH,
    )
    give_partner.start()
    part_back[me] = reduced(me)

    if assisted:
        @pl.when(is_end)
        def _():
            drain(msg_all.at[:3], msg_sem)

        @pl.when(jnp.logical_not(is_end))
        def _():
            drain(msg_all.at[: n - 1], msg_sem)
    else:
        drain(msg_all.at[: n - 1], msg_sem)

    reach = jnp.where(is_end, 2, chips) if assisted else chips
    waited = jnp.where(is_agent, outward, 0) if assisted and soon else 0

    @pl.loop(1, reach)
    def _(k):
        @pl.when(k != waited)
        def _():
            gp_completes(k)

    @pl.loop(1, reach)
    def _(k):
        @pl.when(k != waited)
        def _():
            gp_crossed(near(2 * k + 1))

    if assisted and soon:
        @pl.when(is_end)
        def _():
            gp_crossed(partner)
    else:
        gp_crossed(partner)

    weigh(partner)

    @pl.loop(1, reach)
    def _(k):
        weigh(near(2 * k))
        weigh(near(2 * k + 1))

    if assisted and not soon:
        pl.when(is_agent)(help_out)

    for k in range(sections):
        grad_f[k] = jnp.zeros((quarter, width), F32)

    if assisted:
        for z in range(chips):
            direct = n - 1 - 4 * (z >= 2) - 4 * (z <= last - 2)

            @pl.when(chip == z)
            def _():
                drain(part_sum.at[:direct], back_sem)
    else:
        drain(part_sum.at[: n - 1], back_sem)

    @pl.loop(0, n)
    def _(t):
        def add():
            wanted = table[t, me]
            addend = part_back[t].astype(F32)
            for k in range(sections):
                grad_f[k] = grad_f[k] + addend * is_one(wanted == k)

        if assisted:
            pl.when(jnp.logical_not(crosses(me, t // 2)))(add)
        else:
            add()

    if assisted:
        for side, has in ((0, chip >= 2), (1, chip <= last - 2)):
            @pl.when(has)
            def _():
                drain(collected.at[side], collect_sem.at[side])
                grad_f[...] = grad_f[...] + collected[side].astype(F32)

        @pl.when(is_end)
        def _():
            drain(end_recv, help_sem)
            grad_w[...] = grad_w[...] + end_recv[...].astype(F32)

    fetch_pair.wait_send()
    for z in range(chips):
        near_by = (z > 0) + (z < chips - 1)
        relayed = 2 * (0 < z < chips - 1)
        far = sum(abs(y - z) > 2 for y in range(chips))

        @pl.when(chip == z)
        def _():
            drain(gathered.at[: near_by + relayed + far + chips - 1], sent_sem.at[0])

    drain(fetched.at[: (n - 2) * (groups - 1) * quarter, :], sent_sem.at[1])
    drain(pre_recv.at[1:groups], sent_sem.at[2])
    drain(pre_recv.at[1:groups], sent_sem.at[3])
    if assisted:
        @pl.when(is_agent)
        def _():
            drain(msg_all.at[: n - 2], sent_sem.at[4])
            drain(end_send, sent_sem.at[11])

        @pl.when(jnp.logical_not(is_agent))
        def _():
            drain(msg_all.at[: n - 1], sent_sem.at[4])
    else:
        drain(msg_all.at[: n - 1], sent_sem.at[4])

    for z in range(chips):
        at_end = z in (0, last)
        climbs = z * (z + 1 <= last - assisted) + (z < last)
        descents = (last - z) * (z - 1 >= 0 + assisted) + (z > 0)
        climbs, descents = (climbs if z < last else 0), (descents if z > 0 else 0)
        if at_end:
            climbs, descents = int(z == 0), int(z == last)
        known = 1 if at_end and assisted else last
        doubled = int(at_end and assisted and square)
        swapped = known - (assisted and z in (1, last - 1))

        @pl.when(chip == z)
        def _():
            if square:
                drain(fetched.at[: (climbs + descents + doubled) * span, :], sent_sem.at[5])
                drain(fetched.at[: swapped * span, :], sent_sem.at[8])
            else:
                drain(gp_full.at[: climbs + descents], sent_sem.at[5])
            drain(gp_full.at[: known + 1], sent_sem.at[9])

    if square:
        drain(part_recv, sent_sem.at[6])
        drain(relay_recv, sent_sem.at[10])
    else:
        drain(part_recv.at[1:groups], sent_sem.at[6])
    if assisted:
        @pl.when(is_inner)
        def _():
            drain(part_sum.at[: n - 1 - far_chips], sent_sem.at[7])
            drain(gathered_sum, sent_sem.at[12])

        @pl.when(jnp.logical_not(is_inner))
        def _():
            drain(part_sum.at[: n - 1], sent_sem.at[7])
    else:
        drain(part_sum.at[: n - 1], sent_sem.at[7])


def hand_over(*refs):
    copies = [pltpu.make_async_copy(refs[k], refs[3 + k], refs[6].at[k]) for k in range(3)]
    for copy in copies:
        copy.start()
    for copy in copies:
        copy.wait()


def per_device(
    n, groups,
    features, weights, bias, cotangent, tile_values, tile_count, tile_slot, source_blocks,
):
    rows, width = features.shape
    relations, _, slot_total, blk = tile_values.shape
    sections = rows // blk
    quarter, share, chunk, chips = blk // groups, width // groups, width // n, n // 2
    half = rows // 2
    square = groups == 4
    grid = (2, 2) if square else (groups,)
    vmem = pl.BlockSpec(memory_space=pltpu.VMEM)
    smem = pl.BlockSpec(memory_space=pltpu.SMEM)
    anywhere = pl.BlockSpec(memory_space=pl.ANY)
    hbm = pl.BlockSpec(memory_space=pltpu.HBM)
    dma = pltpu.SemaphoreType.DMA
    out, grad_w, grad_f = pl.pallas_call(
        functools.partial(kernel, n, groups),
        out_shape=(
            pltpu.VMEM((share, rows), BF16),
            pltpu.VMEM((relations, chunk, width), F32),
            pltpu.VMEM((sections, quarter, width), F32),
        ),
        in_specs=[smem, smem, smem, hbm, hbm, vmem, hbm, hbm],
        out_specs=(vmem, vmem, vmem),
        scratch_shapes=[
            pltpu.VMEM((relations, width, width), BF16),
            pltpu.VMEM((relations, rows * slot_total, blk), jnp.int32),
            pltpu.VMEM((sections, groups, quarter, width), BF16),
            pltpu.VMEM((rows, width), BF16),
            pltpu.VMEM((n, sections, quarter, width), BF16),
            pltpu.VMEM((blk, width), BF16),
            pltpu.VMEM((slot_total, blk, blk), BF16),
            pltpu.VMEM((slot_total, blk, blk), BF16),
            pltpu.VMEM((n * blk, width), BF16),
            pltpu.VMEM((relations * rows, n * blk), BF16),
            pltpu.VMEM((relations * rows, 128), F32),
            pltpu.VMEM((relations, width, rows), F32),
            pltpu.VMEM((relations * rows, width), BF16),
            pltpu.VMEM((n, relations, chunk, rows), BF16),
            pltpu.VMEM((n, relations, chunk, rows), BF16),
            pltpu.VMEM((n, relations, chunk, rows), BF16),
            pltpu.VMEM((relations, chunk, width), F32),
            pltpu.VMEM((relations, chunk, width), BF16),
            pltpu.VMEM((relations, chunk, width), BF16),
            pltpu.VMEM((n * blk, relations * rows), BF16),
            pltpu.VMEM((rows, width), F32),
            pltpu.VMEM((groups, half, 2 * share), BF16),
            pltpu.VMEM((groups, half, 2 * share), BF16),
            pltpu.VMEM((half, 2 * share), F32),
            pltpu.VMEM((half, 2 * share), F32),
            pltpu.VMEM((1, 2 * share), F32),
            pltpu.VMEM((groups, half, 2 * share), BF16),
            pltpu.VMEM((n, rows, width), BF16),
            pltpu.VMEM((relations * rows, width), BF16),
            pltpu.VMEM((n, *grid, quarter, width), BF16),
            pltpu.VMEM((n, 2, 2, quarter, width // 2) if square else (groups, n, quarter, width), BF16),
            pltpu.VMEM((n, 2, quarter, width // 2), BF16),
            pltpu.VMEM((n, 2, quarter, width // 2), BF16),
            pltpu.VMEM((n, quarter, width), BF16),
            pltpu.VMEM((n, quarter, width), BF16),
            pltpu.VMEM((chips - 2, 2, quarter, width), BF16),
            pltpu.VMEM((chips - 2, quarter, width), BF16),
            pltpu.VMEM((chips - 2, sections, quarter, width), BF16),
            pltpu.VMEM((2, sections, quarter, width), BF16),
            dma((4,)), dma((2,)), dma((13,)), dma, dma, dma, dma, dma((chips - 2,)), dma((chips - 2,)), dma((2,)), dma((2,)), dma((2,)),
            dma((n, 2)), dma((n, 2, 2)),
            dma((4,)), dma((4,)), dma((n,)), dma((n,)), dma,
            dma((chips,)), dma((chips,)), dma((chips,)),
        ],
        compiler_params=pltpu.CompilerParams(
            collective_id=0, has_side_effects=True, vmem_limit_bytes=60 << 20
        ),
        name="layer",
    )(
        source_blocks, tile_count, tile_slot,
        features.reshape(sections, groups, quarter, width), cotangent, bias,
        tile_values.reshape(relations, rows * slot_total, blk), weights,
    )
    results = (out, grad_w, grad_f)
    out, grad_w, grad_f = pl.pallas_call(
        hand_over,
        out_shape=tuple(jax.ShapeDtypeStruct(x.shape, x.dtype) for x in results),
        in_specs=[vmem] * 3,
        out_specs=(anywhere,) * 3,
        scratch_shapes=[dma((3,))],
        compiler_params=pltpu.CompilerParams(vmem_limit_bytes=4 << 20),
        name="hand_over",
    )(*results)
    return (out.T, grad_w, grad_f)


def solution(mesh):
    placed = (
        P("tgt", None),
        P("rel", None, None),
        P(),
        P("tgt", None),
        P("rel", "tgt", None, None),
        P("rel", "tgt"),
        P("rel", "tgt", None),
        P(),
    )
    return jax.shard_map(
        functools.partial(per_device, mesh.shape["tgt"], mesh.shape["rel"]),
        mesh=mesh,
        in_specs=placed,
        out_specs=(P("tgt", "rel"), P("rel", "tgt", None), P("tgt", "rel", None)),
        check_vma=False,
    )
```

```python
import functools

import jax
import jax.numpy as jnp
from jax import lax
from jax.experimental import pallas as pl
from jax.experimental.pallas import tpu as pltpu
from jax.sharding import PartitionSpec as P

MESH = pl.DeviceIdType.MESH
F32 = jnp.float32
BF16 = jnp.bfloat16


def aligned(start, size, multiple):
    return pl.ds(pl.multiple_of(start, multiple), size)


def is_one(condition):
    return condition.astype(jnp.int32).astype(F32)


def pack(value, first, width):
    half = value.shape[0] // 2
    return jnp.concatenate(
        [value[:half, first : first + width], value[half:, first : first + width]], axis=1
    )


def drain(view, semaphore):
    pltpu.make_async_copy(view, view, semaphore).wait()


def kernel(
    n, groups,
    table, counts, slots,
    feat_hbm, cot_hbm, bias, values_hbm, weights_hbm,
    out, grad_w, grad_f,
    weights, values, feat, cot, gathered, partner_staged, masked, masked_t, fetched, adj, scale, turned_scratch, msg, msg_t, msg_all, msg_end, end_sum, end_send, end_recv, adj_t, pre,
    pre_send, pre_recv, cot_own, active, bias_own, gp_all, gp_full, gm,
    part, part_recv, relay, relay_recv, part_sum, part_back, inbox, crossed, gathered_sum, collected,
    load_sem, pair_sem, sent_sem, spread_sem, back_sem, end_sem, help_sem, inbox_sem, crossed_sem, collect_sem, slab_sem, cross_slab_sem,
    a_recv, b_recv, p_recv, g_recv, d_recv, r_recv, msg_sem, line_sem, other_sem, across_sem,
):
    me = lax.axis_index("tgt")
    grp = lax.axis_index("rel")
    sections, _, quarter, width = feat.shape
    blk = quarter * groups
    rows = sections * blk
    relations = weights.shape[0]
    slot_total = slots.shape[2]
    share = width // groups
    chips = n // 2
    chip, core = me // 2, lax.rem(me, 2)

    def tgt(j):
        return lax.rem(chip + j // 2, chips) * 2 + lax.rem(core + lax.rem(j, 2), 2)

    below, above_me = chip, chips - 1 - chip
    both = jnp.minimum(below, above_me)
    assisted = chips == 4 or chips > 5
    last = chips - 1
    is_end = (chip == 0) | (chip == last)
    agent_low, agent_high = 2, last - 2
    soon = chips == 4
    sliced = soon and groups == 4
    outward = jnp.where(chip == 1, 2, 1)
    outer_chip = jnp.where(chip == 1, 0, last)
    helped = jnp.where(chip == agent_low, 0, last)
    is_agent = (chip == agent_low) | (chip == agent_high)

    def near(j):
        k = j // 2 - 1
        two_sided = jnp.where(lax.rem(k, 2) == 0, chip + k // 2 + 1, chip - k // 2 - 1)
        distance = k - both + 1
        one_sided = jnp.where(above_me > below, chip + distance, chip - distance)
        return jnp.where(k < 2 * both, two_sided, one_sided) * 2 + lax.rem(core + lax.rem(j, 2), 2)

    partner = chip * 2 + 1 - core
    row, column = grp // 2, lax.rem(grp, 2)
    beside = row * 2 + 1 - column
    above = (1 - row) * 2 + column

    square = groups == 4

    def rel(i):
        if square:
            return (grp, beside, above, (1 - row) * 2 + 1 - column)[i]
        return lax.rem(grp + i, groups)

    load_w = pltpu.make_async_copy(weights_hbm, weights, load_sem.at[0])
    load_v = pltpu.make_async_copy(values_hbm, values, load_sem.at[1])
    load_f = pltpu.make_async_copy(feat_hbm, feat, load_sem.at[2])
    load_c = pltpu.make_async_copy(cot_hbm, cot, load_sem.at[3])
    load_f.start()
    load_v.start()
    load_w.start()
    load_c.start()

    barrier = pltpu.get_barrier_semaphore()

    @pl.loop(1, n)
    def _(j):
        pl.semaphore_signal(barrier, inc=1, device_id=(grp, tgt(j)), device_id_type=MESH)

    for i in range(1, groups):
        pl.semaphore_signal(barrier, inc=1, device_id=(rel(i), me), device_id_type=MESH)

    def whole_block(t):
        total = jnp.zeros((blk, width), F32)
        for k in range(sections):
            total = total + feat[k].reshape(blk, width).astype(F32) * is_one(table[t, me] == k)
        return total.astype(BF16)

    pl.semaphore_wait(barrier, n - 1 + groups - 1)

    cut = width // 2

    def columns(h):
        return aligned(h * cut, cut, 128)

    def climb_rows(o, h, source):
        return pltpu.make_async_remote_copy(
            src_ref=source, dst_ref=gathered.at[o, :, :, columns(h)],
            send_sem=sent_sem.at[0], recv_sem=a_recv.at[o, h],
            device_id=(grp, jnp.minimum(chip + 1, chips - 1) * 2 + core), device_id_type=MESH,
        )

    def descend_rows(o, h, source):
        return pltpu.make_async_remote_copy(
            src_ref=source, dst_ref=gathered.at[o, :, :, columns(h)],
            send_sem=sent_sem.at[0], recv_sem=a_recv.at[o, h],
            device_id=(grp, jnp.maximum(chip - 1, 0) * 2 + core), device_id_type=MESH,
        )

    def across_rows(o, h):
        return pltpu.make_async_remote_copy(
            src_ref=gathered.at[o, :, :, columns(h)], dst_ref=gathered.at[o, :, :, columns(h)],
            send_sem=sent_sem.at[0], recv_sem=a_recv.at[o, h],
            device_id=(grp, partner), device_id_type=MESH,
        )

    fetch_pair = pltpu.make_async_remote_copy(
        src_ref=partner_staged, dst_ref=fetched.at[aligned(me * blk, blk, blk), :],
        send_sem=pair_sem.at[0], recv_sem=pair_sem.at[1],
        device_id=(grp, partner), device_id_type=MESH,
    )

    def leap_rows(z, h):
        return pltpu.make_async_remote_copy(
            src_ref=feat_hbm.at[:, grp, :, columns(h)], dst_ref=gathered.at[me, :, :, columns(h)],
            send_sem=sent_sem.at[0], recv_sem=a_recv.at[me, h],
            device_id=(grp, z * 2 + core), device_id_type=MESH,
        )

    for h in range(2):
        @pl.when(chip < chips - 1)
        def _():
            climb_rows(me, h, feat_hbm.at[:, grp, :, columns(h)]).start()

        @pl.when(chip > 0)
        def _():
            descend_rows(me, h, feat_hbm.at[:, grp, :, columns(h)]).start()

    @pl.loop(0, chips)
    def _(z):
        @pl.when((z > chip + 2) | (z < chip - 2))
        def _():
            for h in range(2):
                leap_rows(z, h).start()

    load_f.wait()
    partner_staged[...] = whole_block(partner)
    fetch_pair.start()
    fetched[aligned(me * blk, blk, blk), :] = whole_block(me)

    sent = range(4) if square else range(groups - 1)

    def spread(j, h, way):
        if square:
            size = quarter if way < 2 else quarter // 2
            source = (grp, grp, beside, above)[way]
            extra = quarter // 2 if way == 3 else 0
            peer = (beside, above, above, beside)[way]
        else:
            size, source, extra, peer = quarter, grp, 0, rel(way + 1)
        rows_at = aligned(near(j) * blk + source * quarter + extra, size, size)
        return pltpu.make_async_remote_copy(
            src_ref=fetched.at[rows_at, columns(h)], dst_ref=fetched.at[rows_at, columns(h)],
            send_sem=sent_sem.at[1],
            recv_sem=b_recv.at[j, h, way] if square and way < 2 else spread_sem,
            device_id=(peer, me), device_id_type=MESH,
        )

    first_hop = sent[:2] if square else sent

    def event(e):
        inner = lax.rem(e, 4)
        paired = e < 4 * both
        k = jnp.where(paired, e // 4 * 2 + 1 + lax.rem(inner, 2), e // 2 + 1)
        return k, jnp.where(paired, inner // 2, lax.rem(e, 2))

    def pass_on(e, side):
        k, h = event(e)
        j = 2 * k + side
        if not square:
            return
        spread(j, h, 0).wait_recv()
        spread(j, h, 2).start()
        spread(j, h, 1).wait_recv()
        spread(j, h, 3).start()

    def placed(j, h):
        o = near(j)
        total = jnp.zeros((quarter, cut), F32)
        for k in range(sections):
            total = total + gathered[o, k, :, columns(h)].astype(F32) * is_one(table[me, o] == k)
        fetched[aligned(o * blk + grp * quarter, quarter, quarter), columns(h)] = total.astype(BF16)
        for way in first_hop:
            spread(j, h, way).start()

    def arrive(e):
        k, h = event(e)
        o = near(2 * k)
        across_rows(o, h).wait_recv()

        @pl.when((o // 2 == chip - 1) & (chip < chips - 1))
        def _():
            climb_rows(o, h, gathered.at[o, :, :, columns(h)]).start()

        @pl.when((o // 2 == chip + 1) & (chip > 0))
        def _():
            descend_rows(o, h, gathered.at[o, :, :, columns(h)]).start()

        across_rows(o, h).start()
        placed(2 * k, h)

    def arrive_across(e):
        k, h = event(e)
        across_rows(near(2 * k + 1), h).wait_recv()
        placed(2 * k + 1, h)

    load_v.wait()

    def adjacency(b):
        r, q = b // sections, lax.rem(b, sections)
        count = counts[r, q]
        total = jnp.zeros((blk, blk), F32)
        for s in range(slot_total):
            start = (q * blk * slot_total) + s
            tile = values[r, pl.ds(start, blk, stride=slot_total), :].astype(F32) * is_one(s < count)
            masked[s] = tile.astype(BF16)
            masked_t[s] = tile.T.astype(BF16)
            total = total + tile
        degree = jnp.sum(total, axis=1, keepdims=True)
        root = 1.0 / jnp.sqrt(jnp.maximum(degree, 1.0))
        scale[aligned(b * blk, blk, blk), :] = jnp.broadcast_to(root, (blk, 128))

        @pl.loop(0, n)
        def _(o):
            entry = jnp.zeros((blk, blk), BF16)
            entry_t = jnp.zeros((blk, blk), BF16)
            for s in range(slot_total):
                here = jnp.full((blk, blk), is_one(slots[r, q, s] == o), F32).astype(BF16)
                entry = entry + masked[s] * here
                entry_t = entry_t + masked_t[s] * here
            adj[aligned(b * blk, blk, blk), aligned(o * blk, blk, blk)] = entry
            adj_t[aligned(o * blk, blk, blk), aligned(b * blk, blk, blk)] = entry_t

    blocks = relations * sections

    @pl.loop(0, blocks // 2)
    def _(b):
        adjacency(b)

    events = 2 * (chips - 1)
    arrive(0)
    arrive(1)

    @pl.loop(0, blocks // 2)
    def _(b):
        adjacency(blocks // 2 + b)
        arrive_across(b)
        arrive(2 + b)

    @pl.loop(blocks // 2 + 2, events)
    def _(e):
        arrive(e)
        arrive_across(e - 2)

    pass_on(0, 0)
    arrive_across(events - 2)
    pass_on(0, 1)
    arrive_across(events - 1)

    @pl.loop(1, events)
    def _(e):
        pass_on(e, 0)
        pass_on(e, 1)

    load_w.wait()
    fetch_pair.wait_recv()

    late = n - 2 if square else (n - 2) * (groups - 1)
    drain(fetched.at[: late * quarter, :], spread_sem)

    tile_width = 256
    chunk = width // n
    for c in range(width // tile_width):
        at = slice(c * tile_width, (c + 1) * tile_width)
        acc = jnp.dot(adj[...], fetched[:, at], preferred_element_type=F32) * scale[:, 0:1]
        msg[:, at] = acc.astype(BF16)
        for r in range(relations):
            turned_scratch[r, at, :] = acc[r * rows : (r + 1) * rows, :].T

    for r in range(relations):
        msg_t[:, r] = turned_scratch[r].reshape(n, chunk, rows).astype(BF16)

    def send_messages(target, z, landing, semaphore):
        return pltpu.make_async_remote_copy(
            src_ref=msg_t.at[target], dst_ref=landing.at[me],
            send_sem=sent_sem.at[4], recv_sem=semaphore,
            device_id=(grp, z * 2 + lax.rem(target, 2)), device_id_type=MESH,
        )

    def start_messages(j):
        target = near(j)
        z = target // 2
        if not assisted:
            send_messages(target, z, msg_all, msg_sem).start()
            return
        away = ((z == 0) & (chip >= agent_low)) | ((z == last) & (chip <= agent_high))

        @pl.when(jnp.logical_not(away))
        def _():
            send_messages(target, z, msg_all, msg_sem).start()

        agent = jnp.where(z == 0, agent_low, agent_high)

        @pl.when(away & jnp.logical_not((agent == chip) & (lax.rem(target, 2) == core)))
        def _():
            send_messages(target, agent, msg_end, end_sem).start()

    @pl.loop(4, n)
    def _(j):
        start_messages(n + 3 - j)

    def start_next_messages():
        start_messages(2)
        start_messages(3)

    pl.when(jnp.logical_not(is_end))(start_next_messages)

    send_messages(partner, chip, msg_all, msg_sem).start()
    msg_all[me] = msg_t[me]
    if assisted:
        msg_end[me] = msg_t[helped * 2 + core]

    @pl.loop(0, width // tile_width)
    def _(c):
        at = aligned(c * tile_width, tile_width, tile_width)
        total = None
        for r in range(relations):
            part_r = jnp.dot(
                msg[r * rows : (r + 1) * rows, :], weights[r, :, at], preferred_element_type=F32
            )
            total = part_r if total is None else total + part_r
        pre[:, at] = total

    whole = pre[...]
    for k in range(groups):
        pre_send[k] = pack(whole, k * share, share).astype(BF16)

    pieces = 4
    piece_rows = rows // 2 // pieces

    def reduce_pre(i, p):
        at = slice(p * piece_rows, (p + 1) * piece_rows)
        return pltpu.make_async_remote_copy(
            src_ref=pre_send.at[rel(i), at, :], dst_ref=pre_recv.at[i, at, :],
            send_sem=sent_sem.at[2], recv_sem=p_recv.at[p],
            device_id=(rel(i), me), device_id_type=MESH,
        )

    for p in range(pieces):
        for i in range(1, groups):
            reduce_pre(i, p).start()

    load_c.wait()
    for k in range(groups):
        @pl.when(grp == k)
        def _():
            cot_own[...] = pack(cot[...].astype(F32), k * share, share)
            piece = bias[...].reshape(1, width)[:, k * share : (k + 1) * share]
            bias_own[...] = jnp.concatenate([piece, piece], axis=1)

    def gather_gp(i, p):
        at = slice(p * piece_rows, (p + 1) * piece_rows)
        return pltpu.make_async_remote_copy(
            src_ref=gp_all.at[grp, at, :], dst_ref=gp_all.at[grp, at, :],
            send_sem=sent_sem.at[3], recv_sem=g_recv.at[p],
            device_id=(rel(i), me), device_id_type=MESH,
        )

    for p in range(pieces):
        at = slice(p * piece_rows, (p + 1) * piece_rows)
        total = pre_send[grp, at, :].astype(F32)
        drain(pre_recv.at[1:groups, at, :], p_recv.at[p])
        for i in range(1, groups):
            total = total + pre_recv[i, at, :].astype(F32)
        pre_act = total + bias_own[...]
        sigmoid = jax.nn.sigmoid(pre_act)
        derivative = sigmoid * (1.0 + pre_act * (1.0 - sigmoid))
        gp_all[grp, at, :] = (cot_own[at, :] * derivative).astype(BF16)
        for i in range(1, groups):
            gather_gp(i, p).start()
        active[at, :] = pre_act * sigmoid

    upright = active[...].T
    for h in range(2):
        out[:, h * (rows // 2) : (h + 1) * (rows // 2)] = upright[h * share : (h + 1) * share].astype(BF16)

    half = rows // 2
    for p in range(pieces):
        at = slice(p * piece_rows, (p + 1) * piece_rows)
        drain(pre_recv.at[1:groups, at, :], g_recv.at[p])
        for h in range(2):
            gp_full[me, h * half + p * piece_rows : h * half + (p + 1) * piece_rows, :] = jnp.concatenate(
                [gp_all[k, at, h * share : (h + 1) * share].astype(F32) for k in range(groups)], axis=1
            ).astype(BF16)

    if square:
        span, mine, other = half, jnp.where(core == 0, column, row), jnp.where(core == 0, beside, above)
    else:
        span, mine, other = rows, 0, grp

    def piece_of(o, part_of):
        return gp_full.at[o, aligned(part_of * span, span, span), :]

    def climb_gp(o):
        return pltpu.make_async_remote_copy(
            src_ref=piece_of(o, mine), dst_ref=piece_of(o, mine),
            send_sem=sent_sem.at[5], recv_sem=line_sem.at[o // 2],
            device_id=(grp, jnp.minimum(chip + 1, chips - 1) * 2 + core), device_id_type=MESH,
        )

    def descend_gp(o):
        return pltpu.make_async_remote_copy(
            src_ref=piece_of(o, mine), dst_ref=piece_of(o, mine),
            send_sem=sent_sem.at[5], recv_sem=line_sem.at[o // 2],
            device_id=(grp, jnp.maximum(chip - 1, 0) * 2 + core), device_id_type=MESH,
        )

    def exchange_gp(o):
        return pltpu.make_async_remote_copy(
            src_ref=piece_of(o, mine), dst_ref=piece_of(o, mine),
            send_sem=sent_sem.at[8], recv_sem=other_sem.at[o // 2],
            device_id=(other, me), device_id_type=MESH,
        )

    def across_gp(o, part_of):
        return pltpu.make_async_remote_copy(
            src_ref=piece_of(o, part_of), dst_ref=piece_of(o, part_of),
            send_sem=sent_sem.at[9], recv_sem=across_sem.at[o // 2],
            device_id=(grp, partner), device_id_type=MESH,
        )

    whole_end = assisted and square
    next_in = jnp.where(chip == 0, 1, last - 1)

    def slab(o, c):
        return gp_full.at[o, :, columns(c)]

    def across_slab(o, c):
        return pltpu.make_async_remote_copy(
            src_ref=slab(o, c), dst_ref=slab(o, c),
            send_sem=sent_sem.at[9], recv_sem=cross_slab_sem.at[c],
            device_id=(grp, partner), device_id_type=MESH,
        )

    def beside_end(o):
        return ((o // 2 == 0) & (chip == 1)) | ((o // 2 == last) & (chip == last - 1))

    along = jnp.logical_not(is_end) if sliced else chip >= 0

    @pl.when(along & (chip < chips - 1))
    def _():
        climb_gp(me).start()

    @pl.when(along & (chip > 0))
    def _():
        descend_gp(me).start()

    if sliced:
        @pl.when(is_end)
        def _():
            for c in range(2):
                pltpu.make_async_remote_copy(
                    src_ref=slab(me, c), dst_ref=slab(me, c),
                    send_sem=sent_sem.at[5], recv_sem=slab_sem.at[c],
                    device_id=(grp, next_in * 2 + core), device_id_type=MESH,
                ).start()
    elif whole_end:
        @pl.when(is_end)
        def _():
            pltpu.make_async_remote_copy(
                src_ref=piece_of(me, 1 - mine), dst_ref=piece_of(me, 1 - mine),
                send_sem=sent_sem.at[5], recv_sem=other_sem.at[chip],
                device_id=(grp, next_in * 2 + core), device_id_type=MESH,
            ).start()

    for h in range(rows // span):
        across_gp(me, h).start()


    def gp_arrives(k):
        o = near(2 * k)
        climb_gp(o).wait_recv()

        @pl.when((o < me) & (chip < last - assisted))
        def _():
            climb_gp(o).start()

        @pl.when((o > me) & (chip > 0 + assisted))
        def _():
            descend_gp(o).start()

        if whole_end:
            @pl.when(jnp.logical_not(beside_end(o)))
            def _():
                exchange_gp(o).start()
        elif square:
            exchange_gp(o).start()
        across_gp(o, mine).start()

    def gp_completes(k):
        if square:
            o = near(2 * k)
            pltpu.make_async_remote_copy(
                src_ref=piece_of(o, 1 - mine), dst_ref=piece_of(o, 1 - mine),
                send_sem=sent_sem.at[8], recv_sem=other_sem.at[o // 2],
                device_id=(other, me), device_id_type=MESH,
            ).wait_recv()
            across_gp(o, 1 - mine).start()

    def gp_crossed(o):
        drain(gp_full.at[o], across_sem.at[o // 2])

    def weigh(o):
        chunk = width // n
        if chunk % 16 == 0:
            product = jnp.dot(
                msg_all[o].reshape(relations * chunk, rows), gp_full[o], preferred_element_type=F32
            )
            grad_w[...] = grad_w[...] + product.reshape(relations, chunk, width)
        else:
            for r in range(relations):
                grad_w[r] = grad_w[r] + jnp.dot(msg_all[o, r], gp_full[o], preferred_element_type=F32)

    def weigh_end(o):
        for r in range(relations):
            end_sum[r] = end_sum[r] + jnp.dot(msg_end[o, r], gp_full[o], preferred_element_type=F32)

    grad_w[...] = jnp.zeros(grad_w.shape, F32)
    end_sum[...] = jnp.zeros(end_sum.shape, F32)
    help_end = pltpu.make_async_remote_copy(
        src_ref=end_send, dst_ref=end_recv,
        send_sem=sent_sem.at[11], recv_sem=help_sem,
        device_id=(grp, helped * 2 + core), device_id_type=MESH,
    )

    @pl.loop(0, width // tile_width)
    def _(c):
        at = aligned(c * tile_width, tile_width, tile_width)
        for r in range(relations):
            rows_r = slice(r * rows, (r + 1) * rows)
            grads = lax.dot_general(
                gp_full[me], weights[r, at, :],
                (((1,), (1,)), ((), ())), preferred_element_type=F32,
            )
            gm[rows_r, at] = (grads * scale[rows_r, 0:1]).astype(BF16)

    lower, higher = slice(0, cut), slice(cut, width)

    def far(j):
        return near(n - j + 2 * lax.rem(j, 2))

    def reduce_part(o, i):
        if square:
            source = part.at[o, :, 1 - column, :, lower] if i == 1 else part.at[o, 1 - row, :, :, higher]
            target, peer = part_recv.at[o, i - 1], (beside, above)[i - 1]
        else:
            source, target, peer = part.at[o, rel(i)], part_recv.at[i, o], rel(i)
        return pltpu.make_async_remote_copy(
            src_ref=source, dst_ref=target,
            send_sem=sent_sem.at[6], recv_sem=d_recv.at[o],
            device_id=(peer, me), device_id_type=MESH,
        )

    def relay_part(o, w):
        return pltpu.make_async_remote_copy(
            src_ref=relay.at[o, w], dst_ref=relay_recv.at[o, w],
            send_sem=sent_sem.at[10], recv_sem=r_recv.at[o],
            device_id=((above, beside)[w], me), device_id_type=MESH,
        )

    def start_parts(z):
        product = jnp.dot(
            adj_t[aligned(z * 2 * blk, 2 * blk, blk), :], gm[...], preferred_element_type=F32
        )
        for v in range(2):
            o = z * 2 + v
            part[o] = product[v * blk : (v + 1) * blk].astype(BF16).reshape(part.shape[1:])
            for i in range(1, 3 if square else groups):
                reduce_part(o, i).start()

    @pl.loop(1, chips)
    def _(e):
        start_parts(near(n - 2 * e) // 2)

    far_chips = chips - 2
    is_inner = (chip == 1) | (chip == last - 1)
    low_side = chip <= 1

    def crosses(o, source):
        return ((source <= 1) & (o // 2 >= 2)) | ((source >= last - 1) & (o // 2 <= last - 2))

    def hand(o, device, landing, semaphore):
        return pltpu.make_async_remote_copy(
            src_ref=part_sum.at[o], dst_ref=landing,
            send_sem=sent_sem.at[7], recv_sem=semaphore,
            device_id=(grp, device), device_id_type=MESH,
        )

    def give_back(j):
        o = far(j)
        if not assisted:
            hand(o, o, part_back.at[me], back_sem).start()
            return
        slot = jnp.where(low_side, jnp.maximum(o // 2 - 2, 0), jnp.minimum(o // 2, far_chips - 1))
        odd = lax.rem(o, 2)
        over = crosses(o, chip)

        @pl.when(over & is_end)
        def _():
            hand(o, next_in * 2 + odd, inbox.at[slot, core], inbox_sem.at[slot]).start()

        @pl.when(over & is_inner & (odd != core))
        def _():
            hand(o, partner, crossed.at[slot], crossed_sem.at[slot]).start()

        @pl.when(jnp.logical_not(over & (is_end | is_inner)))
        def _():
            hand(o, o, part_back.at[me], back_sem).start()

    def collect(slot):
        z = jnp.where(low_side, slot + 2, slot)
        side = jnp.where(low_side, 0, 1)
        return pltpu.make_async_remote_copy(
            src_ref=gathered_sum.at[slot], dst_ref=collected.at[side],
            send_sem=sent_sem.at[12], recv_sem=collect_sem.at[side],
            device_id=(grp, z * 2 + core), device_id_type=MESH,
        )

    def sum_for_far_side(first=0, past=far_chips):
        outer = jnp.where(low_side, 0, last)

        @pl.loop(first, past)
        def _(i):
            slot = jnp.where(low_side, far_chips - 1 - i, i)
            drain(crossed.at[slot], crossed_sem.at[slot])
            drain(inbox.at[slot], inbox_sem.at[slot])
            o = jnp.where(low_side, slot + 2, slot) * 2 + core
            terms = (
                (me, part_sum[o].astype(F32)),
                (partner, crossed[slot].astype(F32)),
                (outer * 2, inbox[slot, 0].astype(F32)),
                (outer * 2 + 1, inbox[slot, 1].astype(F32)),
            )
            for k in range(sections):
                total = None
                for t, term in terms:
                    kept = term * is_one(table[t, o] == k)
                    total = kept if total is None else total + kept
                gathered_sum[slot, k] = total.astype(BF16)
            collect(slot).start()

    def relayed(o):
        if square:
            drain(part_recv.at[o], d_recv.at[o])
            up = part[o, 1 - row, column, :, lower].astype(F32) + part_recv[o, 0, 1 - row].astype(F32)
            relay[o, 0] = up.astype(BF16)
            relay_part(o, 0).start()
            aside = part[o, row, 1 - column, :, higher].astype(F32) + part_recv[o, 1, 1 - column].astype(F32)
            relay[o, 1] = aside.astype(BF16)
            relay_part(o, 1).start()

    def reduced(o):
        if square:
            drain(relay_recv.at[o], r_recv.at[o])
            first = part[o, row, column, :, lower].astype(F32) + part_recv[o, 0, row].astype(F32)
            second = part[o, row, column, :, higher].astype(F32) + part_recv[o, 1, column].astype(F32)
            first = first + relay_recv[o, 0].astype(F32)
            second = second + relay_recv[o, 1].astype(F32)
            return jnp.concatenate([first, second], axis=1).astype(BF16)
        total = part[o, grp].astype(F32)
        drain(part_recv.at[1:groups, o], d_recv.at[o])
        for i in range(1, groups):
            total = total + part_recv[i, o].astype(F32)
        return total.astype(BF16)

    def send_reduced(j):
        part_sum[far(j)] = reduced(far(j))
        give_back(j)

    relays = both > 0
    weigh(me)

    def slab_arrives(c):
        drain(slab(outer_chip * 2 + core, c), slab_sem.at[c])
        outer = outer_chip * 2 + core
        across_slab(outer, c).start()
        ahead = gp_full.at[outer, aligned(mine * span, span, span), columns(c)]
        pltpu.make_async_remote_copy(
            src_ref=ahead, dst_ref=ahead,
            send_sem=sent_sem.at[5], recv_sem=line_sem.at[outer_chip],
            device_id=(grp, jnp.where(chip == 1, 2, last - 2) * 2 + core), device_id_type=MESH,
        ).start()

    def help_slab(c):
        other = outer_chip * 2 + 1 - core
        drain(slab(other, c), cross_slab_sem.at[c])
        for r in range(relations):
            total = None
            for o in (me, partner, outer_chip * 2 + core, other):
                product = jnp.dot(msg_end[o, r], gp_full[o, :, c * cut : (c + 1) * cut], preferred_element_type=F32)
                total = product if total is None else total + product
            end_send[r, :, c * cut : (c + 1) * cut] = total.astype(BF16)
        pltpu.make_async_remote_copy(
            src_ref=end_send.at[:, :, columns(c)], dst_ref=end_recv.at[:, :, columns(c)],
            send_sem=sent_sem.at[11], recv_sem=help_sem,
            device_id=(grp, helped * 2 + core), device_id_type=MESH,
        ).start()

    if sliced:
        @pl.when(is_end)
        def _():
            gp_arrives(1)
            relayed(far(2))
            relayed(far(3))
            start_next_messages()
            relayed(far(4))
            relayed(far(5))

        @pl.when(jnp.logical_not(is_end))
        def _():
            gp_arrives(3 - outward)
            slab_arrives(0)
            relayed(far(2))
            relayed(far(3))
            gp_crossed(partner)
            drain(msg_end.at[: 2 * (chips - 2) - 1], end_sem)
            help_slab(0)
            slab_arrives(1)
            relayed(far(4))
            relayed(far(5))
            help_slab(1)
    else:
        gp_arrives(1)

        @pl.when(relays)
        def _():
            gp_arrives(2)

        @pl.loop(2, n - 2)
        def _(j):
            relayed(far(j))

    start_parts(chip)

    sides = jnp.where(helped == 0, last - chip, chip)

    def beyond(i):
        return jnp.where(helped == 0, chip + 1, chip - 1 - (sides - 1)) + i

    def complete(k):
        gp_completes(k)
        gp_crossed(near(2 * k + 1))

    if assisted and soon and not sliced:
        @pl.when(is_agent)
        def _():
            complete(outward)
            gp_crossed(partner)

    def help_out():
        drain(msg_end.at[: 2 * (chips - 2) - 1], end_sem)
        weigh_end(me)
        weigh_end(partner)

        @pl.loop(0, sides)
        def _(i):
            weigh_end(beyond(i) * 2)
            weigh_end(beyond(i) * 2 + 1)

        end_send[...] = end_sum[...].astype(BF16)
        help_end.start()

    if assisted and soon and not sliced:
        pl.when(is_agent)(help_out)

    if not sliced:
        pl.when(is_end)(start_next_messages)
    if not assisted:
        @pl.when(jnp.logical_not(relays))
        def _():
            gp_arrives(2)

    relayed(far(n - 2))
    relayed(far(n - 1))

    if not sliced:
        @pl.when(relays)
        def _():
            @pl.loop(3, chips)
            def _(k):
                gp_arrives(k)


    @pl.loop(2, n - 2)
    def _(j):
        send_reduced(j)

    relayed(partner)
    relayed(me)
    send_reduced(n - 2)
    send_reduced(n - 1)

    if sliced:
        @pl.when(relays)
        def _():
            sum_for_far_side(0, 1)
            gp_arrives(3)

    if not assisted:
        @pl.when(jnp.logical_not(relays))
        def _():
            @pl.loop(3, chips)
            def _(k):
                gp_arrives(k)

    if assisted:
        pl.when(is_inner)(functools.partial(sum_for_far_side, 1 if sliced else 0))

    if assisted:
        @pl.when(is_end)
        def _():
            drain(msg_all.at[:3], msg_sem)

        @pl.when(jnp.logical_not(is_end))
        def _():
            drain(msg_all.at[: n - 1], msg_sem)
    else:
        drain(msg_all.at[: n - 1], msg_sem)

    if sliced:
        @pl.when(is_end)
        def _():
            gp_completes(1)
            gp_crossed(partner)
            weigh(partner)
            weigh(near(2))

        @pl.when(jnp.logical_not(is_end))
        def _():
            inward = 3 - outward

            @pl.loop(0, 3)
            def _(i):
                weigh(jnp.where(i == 0, partner, near(2 * outward + jnp.maximum(i - 1, 0))))

            gp_completes(inward)
            weigh(near(2 * inward))
            gp_crossed(near(2 * inward + 1))
            weigh(near(2 * inward + 1))
            gp_completes(3)

    part_sum[partner] = reduced(partner)
    give_partner = pltpu.make_async_remote_copy(
        src_ref=part_sum.at[partner], dst_ref=part_back.at[me],
        send_sem=sent_sem.at[7], recv_sem=back_sem,
        device_id=(grp, partner), device_id_type=MESH,
    )
    give_partner.start()
    part_back[me] = reduced(me)

    if sliced:
        @pl.when(is_end)
        def _():
            gp_crossed(near(3))
            weigh(near(3))

        @pl.when(jnp.logical_not(is_end))
        def _():
            weigh(near(6))
            gp_crossed(near(7))
            weigh(near(7))
    else:
        reach = jnp.where(is_end, 2, chips) if assisted else chips
        waited = jnp.where(is_agent, outward, 0) if assisted and soon else 0

        @pl.loop(1, reach)
        def _(k):
            @pl.when(k != waited)
            def _():
                gp_completes(k)

        @pl.loop(1, reach)
        def _(k):
            @pl.when(k != waited)
            def _():
                gp_crossed(near(2 * k + 1))

        if assisted and soon:
            @pl.when(is_end)
            def _():
                gp_crossed(partner)
        else:
            gp_crossed(partner)

        weigh(partner)

        @pl.loop(1, reach)
        def _(k):
            weigh(near(2 * k))
            weigh(near(2 * k + 1))

        if assisted and not soon:
            pl.when(is_agent)(help_out)

    for k in range(sections):
        grad_f[k] = jnp.zeros((quarter, width), F32)

    if assisted:
        for z in range(chips):
            direct = n - 1 - 4 * (z >= 2) - 4 * (z <= last - 2)

            @pl.when(chip == z)
            def _():
                drain(part_sum.at[:direct], back_sem)
    else:
        drain(part_sum.at[: n - 1], back_sem)

    @pl.loop(0, n)
    def _(t):
        def add():
            wanted = table[t, me]
            addend = part_back[t].astype(F32)
            for k in range(sections):
                grad_f[k] = grad_f[k] + addend * is_one(wanted == k)

        if assisted:
            pl.when(jnp.logical_not(crosses(me, t // 2)))(add)
        else:
            add()

    if assisted:
        for side, has in ((0, chip >= 2), (1, chip <= last - 2)):
            @pl.when(has)
            def _():
                drain(collected.at[side], collect_sem.at[side])
                grad_f[...] = grad_f[...] + collected[side].astype(F32)

        @pl.when(is_end)
        def _():
            drain(end_recv, help_sem)
            grad_w[...] = grad_w[...] + end_recv[...].astype(F32)

    fetch_pair.wait_send()
    for z in range(chips):
        near_by = (z > 0) + (z < chips - 1)
        relayed = 2 * (0 < z < chips - 1)
        far = sum(abs(y - z) > 2 for y in range(chips))

        @pl.when(chip == z)
        def _():
            drain(gathered.at[: near_by + relayed + far + chips - 1], sent_sem.at[0])

    drain(fetched.at[: (n - 2) * (groups - 1) * quarter, :], sent_sem.at[1])
    drain(pre_recv.at[1:groups], sent_sem.at[2])
    drain(pre_recv.at[1:groups], sent_sem.at[3])
    if assisted:
        @pl.when(is_agent)
        def _():
            drain(msg_all.at[: n - 2], sent_sem.at[4])
            drain(end_send, sent_sem.at[11])

        @pl.when(jnp.logical_not(is_agent))
        def _():
            drain(msg_all.at[: n - 1], sent_sem.at[4])
    else:
        drain(msg_all.at[: n - 1], sent_sem.at[4])

    for z in range(chips):
        at_end = z in (0, last)
        climbs = z * (z + 1 <= last - assisted) + (z < last)
        descents = (last - z) * (z - 1 >= 0 + assisted) + (z > 0)
        climbs, descents = (climbs if z < last else 0), (descents if z > 0 else 0)
        if at_end:
            climbs, descents = int(z == 0), int(z == last)
        known = 1 if at_end and assisted else last
        doubled = int(at_end and assisted and square)
        swapped = known - (assisted and z in (1, last - 1))

        @pl.when(chip == z)
        def _():
            if square:
                drain(fetched.at[: (climbs + descents + doubled) * span, :], sent_sem.at[5])
                drain(fetched.at[: swapped * span, :], sent_sem.at[8])
            else:
                drain(gp_full.at[: climbs + descents], sent_sem.at[5])
            drain(gp_full.at[: known + 1], sent_sem.at[9])

    if square:
        drain(part_recv, sent_sem.at[6])
        drain(relay_recv, sent_sem.at[10])
    else:
        drain(part_recv.at[1:groups], sent_sem.at[6])
    if assisted:
        @pl.when(is_inner)
        def _():
            drain(part_sum.at[: n - 1 - far_chips], sent_sem.at[7])
            drain(gathered_sum, sent_sem.at[12])

        @pl.when(jnp.logical_not(is_inner))
        def _():
            drain(part_sum.at[: n - 1], sent_sem.at[7])
    else:
        drain(part_sum.at[: n - 1], sent_sem.at[7])


def hand_over(*refs):
    copies = [pltpu.make_async_copy(refs[k], refs[3 + k], refs[6].at[k]) for k in range(3)]
    for copy in copies:
        copy.start()
    for copy in copies:
        copy.wait()


def per_device(
    n, groups,
    features, weights, bias, cotangent, tile_values, tile_count, tile_slot, source_blocks,
):
    rows, width = features.shape
    relations, _, slot_total, blk = tile_values.shape
    sections = rows // blk
    quarter, share, chunk, chips = blk // groups, width // groups, width // n, n // 2
    half = rows // 2
    square = groups == 4
    grid = (2, 2) if square else (groups,)
    vmem = pl.BlockSpec(memory_space=pltpu.VMEM)
    smem = pl.BlockSpec(memory_space=pltpu.SMEM)
    anywhere = pl.BlockSpec(memory_space=pl.ANY)
    hbm = pl.BlockSpec(memory_space=pltpu.HBM)
    dma = pltpu.SemaphoreType.DMA
    out, grad_w, grad_f = pl.pallas_call(
        functools.partial(kernel, n, groups),
        out_shape=(
            pltpu.VMEM((share, rows), BF16),
            pltpu.VMEM((relations, chunk, width), F32),
            pltpu.VMEM((sections, quarter, width), F32),
        ),
        in_specs=[smem, smem, smem, hbm, hbm, vmem, hbm, hbm],
        out_specs=(vmem, vmem, vmem),
        scratch_shapes=[
            pltpu.VMEM((relations, width, width), BF16),
            pltpu.VMEM((relations, rows * slot_total, blk), jnp.int32),
            pltpu.VMEM((sections, groups, quarter, width), BF16),
            pltpu.VMEM((rows, width), BF16),
            pltpu.VMEM((n, sections, quarter, width), BF16),
            pltpu.VMEM((blk, width), BF16),
            pltpu.VMEM((slot_total, blk, blk), BF16),
            pltpu.VMEM((slot_total, blk, blk), BF16),
            pltpu.VMEM((n * blk, width), BF16),
            pltpu.VMEM((relations * rows, n * blk), BF16),
            pltpu.VMEM((relations * rows, 128), F32),
            pltpu.VMEM((relations, width, rows), F32),
            pltpu.VMEM((relations * rows, width), BF16),
            pltpu.VMEM((n, relations, chunk, rows), BF16),
            pltpu.VMEM((n, relations, chunk, rows), BF16),
            pltpu.VMEM((n, relations, chunk, rows), BF16),
            pltpu.VMEM((relations, chunk, width), F32),
            pltpu.VMEM((relations, chunk, width), BF16),
            pltpu.VMEM((relations, chunk, width), BF16),
            pltpu.VMEM((n * blk, relations * rows), BF16),
            pltpu.VMEM((rows, width), F32),
            pltpu.VMEM((groups, half, 2 * share), BF16),
            pltpu.VMEM((groups, half, 2 * share), BF16),
            pltpu.VMEM((half, 2 * share), F32),
            pltpu.VMEM((half, 2 * share), F32),
            pltpu.VMEM((1, 2 * share), F32),
            pltpu.VMEM((groups, half, 2 * share), BF16),
            pltpu.VMEM((n, rows, width), BF16),
            pltpu.VMEM((relations * rows, width), BF16),
            pltpu.VMEM((n, *grid, quarter, width), BF16),
            pltpu.VMEM((n, 2, 2, quarter, width // 2) if square else (groups, n, quarter, width), BF16),
            pltpu.VMEM((n, 2, quarter, width // 2), BF16),
            pltpu.VMEM((n, 2, quarter, width // 2), BF16),
            pltpu.VMEM((n, quarter, width), BF16),
            pltpu.VMEM((n, quarter, width), BF16),
            pltpu.VMEM((chips - 2, 2, quarter, width), BF16),
            pltpu.VMEM((chips - 2, quarter, width), BF16),
            pltpu.VMEM((chips - 2, sections, quarter, width), BF16),
            pltpu.VMEM((2, sections, quarter, width), BF16),
            dma((4,)), dma((2,)), dma((13,)), dma, dma, dma, dma, dma((chips - 2,)), dma((chips - 2,)), dma((2,)), dma((2,)), dma((2,)),
            dma((n, 2)), dma((n, 2, 2)),
            dma((4,)), dma((4,)), dma((n,)), dma((n,)), dma,
            dma((chips,)), dma((chips,)), dma((chips,)),
        ],
        compiler_params=pltpu.CompilerParams(
            collective_id=0, has_side_effects=True, vmem_limit_bytes=60 << 20
        ),
        name="layer",
    )(
        source_blocks, tile_count, tile_slot,
        features.reshape(sections, groups, quarter, width), cotangent, bias,
        tile_values.reshape(relations, rows * slot_total, blk), weights,
    )
    results = (out, grad_w, grad_f)
    out, grad_w, grad_f = pl.pallas_call(
        hand_over,
        out_shape=tuple(jax.ShapeDtypeStruct(x.shape, x.dtype) for x in results),
        in_specs=[vmem] * 3,
        out_specs=(anywhere,) * 3,
        scratch_shapes=[dma((3,))],
        compiler_params=pltpu.CompilerParams(vmem_limit_bytes=4 << 20),
        name="hand_over",
    )(*results)
    return (out.T, grad_w, grad_f)


def solution(mesh):
    placed = (
        P("tgt", None),
        P("rel", None, None),
        P(),
        P("tgt", None),
        P("rel", "tgt", None, None),
        P("rel", "tgt"),
        P("rel", "tgt", None),
        P(),
    )
    return jax.shard_map(
        functools.partial(per_device, mesh.shape["tgt"], mesh.shape["rel"]),
        mesh=mesh,
        in_specs=placed,
        out_specs=(P("tgt", "rel"), P("rel", "tgt", None), P("tgt", "rel", None)),
        check_vma=False,
    )
```

```python
import functools

import jax
import jax.numpy as jnp
from jax import lax
from jax.experimental import pallas as pl
from jax.experimental.pallas import tpu as pltpu
from jax.sharding import PartitionSpec as P

MESH = pl.DeviceIdType.MESH
F32 = jnp.float32
BF16 = jnp.bfloat16


def aligned(start, size, multiple):
    return pl.ds(pl.multiple_of(start, multiple), size)


def is_one(condition):
    return condition.astype(jnp.int32).astype(F32)


def pack(value, first, width):
    half = value.shape[0] // 2
    return jnp.concatenate(
        [value[:half, first : first + width], value[half:, first : first + width]], axis=1
    )


def drain(view, semaphore):
    pltpu.make_async_copy(view, view, semaphore).wait()


def kernel(
    n, groups,
    table, counts, slots,
    feat_hbm, cot_hbm, bias, values_hbm, weights_hbm,
    out, grad_w, grad_f,
    weights, values, feat, cot, gathered, partner_staged, masked, masked_t, fetched, adj, scale, turned_scratch, msg, msg_t, msg_all, msg_end, end_sum, end_send, end_recv, adj_t, pre,
    pre_send, pre_recv, cot_own, active, bias_own, gp_all, gp_full, gm,
    part, part_recv, relay, relay_recv, part_sum, part_back, inbox, crossed, gathered_sum, collected,
    load_sem, pair_sem, sent_sem, spread_sem, back_sem, end_sem, help_sem, inbox_sem, crossed_sem, collect_sem, slab_sem, cross_slab_sem,
    a_recv, b_recv, p_recv, g_recv, d_recv, r_recv, msg_sem, line_sem, other_sem, across_sem,
):
    me = lax.axis_index("tgt")
    grp = lax.axis_index("rel")
    sections, _, quarter, width = feat.shape
    blk = quarter * groups
    rows = sections * blk
    relations = weights.shape[0]
    slot_total = slots.shape[2]
    share = width // groups
    chips = n // 2
    chip, core = me // 2, lax.rem(me, 2)

    def tgt(j):
        return lax.rem(chip + j // 2, chips) * 2 + lax.rem(core + lax.rem(j, 2), 2)

    below, above_me = chip, chips - 1 - chip
    both = jnp.minimum(below, above_me)
    assisted = chips == 4 or chips > 5
    last = chips - 1
    is_end = (chip == 0) | (chip == last)
    agent_low, agent_high = 2, last - 2
    soon = chips == 4
    sliced = soon and groups == 4
    outward = jnp.where(chip == 1, 2, 1)
    outer_chip = jnp.where(chip == 1, 0, last)
    helped = jnp.where(chip == agent_low, 0, last)
    is_agent = (chip == agent_low) | (chip == agent_high)

    def near(j):
        k = j // 2 - 1
        two_sided = jnp.where(lax.rem(k, 2) == 0, chip + k // 2 + 1, chip - k // 2 - 1)
        distance = k - both + 1
        one_sided = jnp.where(above_me > below, chip + distance, chip - distance)
        return jnp.where(k < 2 * both, two_sided, one_sided) * 2 + lax.rem(core + lax.rem(j, 2), 2)

    partner = chip * 2 + 1 - core
    row, column = grp // 2, lax.rem(grp, 2)
    beside = row * 2 + 1 - column
    above = (1 - row) * 2 + column

    square = groups == 4

    def rel(i):
        if square:
            return (grp, beside, above, (1 - row) * 2 + 1 - column)[i]
        return lax.rem(grp + i, groups)

    load_w = pltpu.make_async_copy(weights_hbm, weights, load_sem.at[0])
    load_v = pltpu.make_async_copy(values_hbm, values, load_sem.at[1])
    load_f = pltpu.make_async_copy(feat_hbm, feat, load_sem.at[2])
    load_c = pltpu.make_async_copy(cot_hbm, cot, load_sem.at[3])
    load_f.start()
    load_v.start()
    load_w.start()
    load_c.start()

    barrier = pltpu.get_barrier_semaphore()

    @pl.loop(1, n)
    def _(j):
        pl.semaphore_signal(barrier, inc=1, device_id=(grp, tgt(j)), device_id_type=MESH)

    for i in range(1, groups):
        pl.semaphore_signal(barrier, inc=1, device_id=(rel(i), me), device_id_type=MESH)

    def whole_block(t):
        total = jnp.zeros((blk, width), F32)
        for k in range(sections):
            total = total + feat[k].reshape(blk, width).astype(F32) * is_one(table[t, me] == k)
        return total.astype(BF16)

    pl.semaphore_wait(barrier, n - 1 + groups - 1)

    cut = width // 2

    def columns(h):
        return aligned(h * cut, cut, 128)

    def climb_rows(o, h, source):
        return pltpu.make_async_remote_copy(
            src_ref=source, dst_ref=gathered.at[o, :, :, columns(h)],
            send_sem=sent_sem.at[0], recv_sem=a_recv.at[o, h],
            device_id=(grp, jnp.minimum(chip + 1, chips - 1) * 2 + core), device_id_type=MESH,
        )

    def descend_rows(o, h, source):
        return pltpu.make_async_remote_copy(
            src_ref=source, dst_ref=gathered.at[o, :, :, columns(h)],
            send_sem=sent_sem.at[0], recv_sem=a_recv.at[o, h],
            device_id=(grp, jnp.maximum(chip - 1, 0) * 2 + core), device_id_type=MESH,
        )

    def across_rows(o, h):
        return pltpu.make_async_remote_copy(
            src_ref=gathered.at[o, :, :, columns(h)], dst_ref=gathered.at[o, :, :, columns(h)],
            send_sem=sent_sem.at[0], recv_sem=a_recv.at[o, h],
            device_id=(grp, partner), device_id_type=MESH,
        )

    fetch_pair = pltpu.make_async_remote_copy(
        src_ref=partner_staged, dst_ref=fetched.at[aligned(me * blk, blk, blk), :],
        send_sem=pair_sem.at[0], recv_sem=pair_sem.at[1],
        device_id=(grp, partner), device_id_type=MESH,
    )

    def leap_rows(z, h):
        return pltpu.make_async_remote_copy(
            src_ref=feat_hbm.at[:, grp, :, columns(h)], dst_ref=gathered.at[me, :, :, columns(h)],
            send_sem=sent_sem.at[0], recv_sem=a_recv.at[me, h],
            device_id=(grp, z * 2 + core), device_id_type=MESH,
        )

    for h in range(2):
        @pl.when(chip < chips - 1)
        def _():
            climb_rows(me, h, feat_hbm.at[:, grp, :, columns(h)]).start()

        @pl.when(chip > 0)
        def _():
            descend_rows(me, h, feat_hbm.at[:, grp, :, columns(h)]).start()

    @pl.loop(0, chips)
    def _(z):
        @pl.when((z > chip + 2) | (z < chip - 2))
        def _():
            for h in range(2):
                leap_rows(z, h).start()

    load_f.wait()
    partner_staged[...] = whole_block(partner)
    fetch_pair.start()
    fetched[aligned(me * blk, blk, blk), :] = whole_block(me)

    sent = range(4) if square else range(groups - 1)

    def spread(j, h, way):
        if square:
            size = quarter if way < 2 else quarter // 2
            source = (grp, grp, beside, above)[way]
            extra = quarter // 2 if way == 3 else 0
            peer = (beside, above, above, beside)[way]
        else:
            size, source, extra, peer = quarter, grp, 0, rel(way + 1)
        rows_at = aligned(near(j) * blk + source * quarter + extra, size, size)
        return pltpu.make_async_remote_copy(
            src_ref=fetched.at[rows_at, columns(h)], dst_ref=fetched.at[rows_at, columns(h)],
            send_sem=sent_sem.at[1],
            recv_sem=b_recv.at[j, h] if square and way < 2 else spread_sem,
            device_id=(peer, me), device_id_type=MESH,
        )

    first_hop = sent[:2] if square else sent

    def event(e):
        inner = lax.rem(e, 4)
        paired = e < 4 * both
        k = jnp.where(paired, e // 4 * 2 + 1 + lax.rem(inner, 2), e // 2 + 1)
        return k, jnp.where(paired, inner // 2, lax.rem(e, 2))

    def pass_on(e, side):
        k, h = event(e)
        j = 2 * k + side
        if not square:
            return
        drain(fetched.at[: 2 * quarter, columns(h)], b_recv.at[j, h])
        spread(j, h, 2).start()
        spread(j, h, 3).start()

    def placed(j, h):
        o = near(j)
        total = jnp.zeros((quarter, cut), F32)
        for k in range(sections):
            total = total + gathered[o, k, :, columns(h)].astype(F32) * is_one(table[me, o] == k)
        fetched[aligned(o * blk + grp * quarter, quarter, quarter), columns(h)] = total.astype(BF16)
        for way in first_hop:
            spread(j, h, way).start()

    def arrive(e):
        k, h = event(e)
        o = near(2 * k)
        across_rows(o, h).wait_recv()

        @pl.when((o // 2 == chip - 1) & (chip < chips - 1))
        def _():
            climb_rows(o, h, gathered.at[o, :, :, columns(h)]).start()

        @pl.when((o // 2 == chip + 1) & (chip > 0))
        def _():
            descend_rows(o, h, gathered.at[o, :, :, columns(h)]).start()

        across_rows(o, h).start()
        placed(2 * k, h)

    def arrive_across(e):
        k, h = event(e)
        across_rows(near(2 * k + 1), h).wait_recv()
        placed(2 * k + 1, h)

    load_v.wait()

    def adjacency(b):
        r, q = b // sections, lax.rem(b, sections)
        count = counts[r, q]
        total = jnp.zeros((blk, blk), F32)
        for s in range(slot_total):
            start = (q * blk * slot_total) + s
            tile = values[r, pl.ds(start, blk, stride=slot_total), :].astype(F32) * is_one(s < count)
            masked[s] = tile.astype(BF16)
            masked_t[s] = tile.T.astype(BF16)
            total = total + tile
        degree = jnp.sum(total, axis=1, keepdims=True)
        root = 1.0 / jnp.sqrt(jnp.maximum(degree, 1.0))
        scale[aligned(b * blk, blk, blk), :] = jnp.broadcast_to(root, (blk, 128))

        @pl.loop(0, n)
        def _(o):
            entry = jnp.zeros((blk, blk), BF16)
            entry_t = jnp.zeros((blk, blk), BF16)
            for s in range(slot_total):
                here = jnp.full((blk, blk), is_one(slots[r, q, s] == o), F32).astype(BF16)
                entry = entry + masked[s] * here
                entry_t = entry_t + masked_t[s] * here
            adj[aligned(b * blk, blk, blk), aligned(o * blk, blk, blk)] = entry
            adj_t[aligned(o * blk, blk, blk), aligned(b * blk, blk, blk)] = entry_t

    blocks = relations * sections

    @pl.loop(0, blocks // 2)
    def _(b):
        adjacency(b)

    events = 2 * (chips - 1)
    arrive(0)
    arrive(1)

    @pl.loop(0, blocks // 2)
    def _(b):
        adjacency(blocks // 2 + b)
        arrive_across(b)
        arrive(2 + b)

    @pl.loop(blocks // 2 + 2, events)
    def _(e):
        arrive(e)
        arrive_across(e - 2)

    pass_on(0, 0)
    arrive_across(events - 2)
    pass_on(0, 1)
    arrive_across(events - 1)

    @pl.loop(1, events)
    def _(e):
        pass_on(e, 0)
        pass_on(e, 1)

    load_w.wait()
    fetch_pair.wait_recv()

    late = n - 2 if square else (n - 2) * (groups - 1)
    drain(fetched.at[: late * quarter, :], spread_sem)

    tile_width = 256
    chunk = width // n
    for c in range(width // tile_width):
        at = slice(c * tile_width, (c + 1) * tile_width)
        acc = jnp.dot(adj[...], fetched[:, at], preferred_element_type=F32) * scale[:, 0:1]
        msg[:, at] = acc.astype(BF16)
        for r in range(relations):
            turned_scratch[r, at, :] = acc[r * rows : (r + 1) * rows, :].T

    for r in range(relations):
        msg_t[:, r] = turned_scratch[r].reshape(n, chunk, rows).astype(BF16)

    def send_messages(target, z, landing, semaphore):
        return pltpu.make_async_remote_copy(
            src_ref=msg_t.at[target], dst_ref=landing.at[me],
            send_sem=sent_sem.at[4], recv_sem=semaphore,
            device_id=(grp, z * 2 + lax.rem(target, 2)), device_id_type=MESH,
        )

    def start_messages(j):
        target = near(j)
        z = target // 2
        if not assisted:
            send_messages(target, z, msg_all, msg_sem).start()
            return
        away = ((z == 0) & (chip >= agent_low)) | ((z == last) & (chip <= agent_high))

        @pl.when(jnp.logical_not(away))
        def _():
            send_messages(target, z, msg_all, msg_sem).start()

        agent = jnp.where(z == 0, agent_low, agent_high)

        @pl.when(away & jnp.logical_not((agent == chip) & (lax.rem(target, 2) == core)))
        def _():
            send_messages(target, agent, msg_end, end_sem).start()

    @pl.loop(4, n)
    def _(j):
        start_messages(n + 3 - j)

    def start_next_messages():
        start_messages(2)
        start_messages(3)

    pl.when(jnp.logical_not(is_end))(start_next_messages)

    send_messages(partner, chip, msg_all, msg_sem).start()
    msg_all[me] = msg_t[me]
    if assisted:
        msg_end[me] = msg_t[helped * 2 + core]

    @pl.loop(0, width // tile_width)
    def _(c):
        at = aligned(c * tile_width, tile_width, tile_width)
        total = None
        for r in range(relations):
            part_r = jnp.dot(
                msg[r * rows : (r + 1) * rows, :], weights[r, :, at], preferred_element_type=F32
            )
            total = part_r if total is None else total + part_r
        pre[:, at] = total

    whole = pre[...]
    for k in range(groups):
        pre_send[k] = pack(whole, k * share, share).astype(BF16)

    pieces = 4
    piece_rows = rows // 2 // pieces

    def reduce_pre(i, p):
        at = slice(p * piece_rows, (p + 1) * piece_rows)
        return pltpu.make_async_remote_copy(
            src_ref=pre_send.at[rel(i), at, :], dst_ref=pre_recv.at[i, at, :],
            send_sem=sent_sem.at[2], recv_sem=p_recv.at[p],
            device_id=(rel(i), me), device_id_type=MESH,
        )

    for p in range(pieces):
        for i in range(1, groups):
            reduce_pre(i, p).start()

    load_c.wait()
    for k in range(groups):
        @pl.when(grp == k)
        def _():
            cot_own[...] = pack(cot[...].astype(F32), k * share, share)
            piece = bias[...].reshape(1, width)[:, k * share : (k + 1) * share]
            bias_own[...] = jnp.concatenate([piece, piece], axis=1)

    def gather_gp(i, p):
        at = slice(p * piece_rows, (p + 1) * piece_rows)
        return pltpu.make_async_remote_copy(
            src_ref=gp_all.at[grp, at, :], dst_ref=gp_all.at[grp, at, :],
            send_sem=sent_sem.at[3], recv_sem=g_recv.at[p],
            device_id=(rel(i), me), device_id_type=MESH,
        )

    for p in range(pieces):
        at = slice(p * piece_rows, (p + 1) * piece_rows)
        total = pre_send[grp, at, :].astype(F32)
        drain(pre_recv.at[1:groups, at, :], p_recv.at[p])
        for i in range(1, groups):
            total = total + pre_recv[i, at, :].astype(F32)
        pre_act = total + bias_own[...]
        sigmoid = jax.nn.sigmoid(pre_act)
        derivative = sigmoid * (1.0 + pre_act * (1.0 - sigmoid))
        gp_all[grp, at, :] = (cot_own[at, :] * derivative).astype(BF16)
        for i in range(1, groups):
            gather_gp(i, p).start()
        active[at, :] = pre_act * sigmoid

    upright = active[...].T
    for h in range(2):
        out[:, h * (rows // 2) : (h + 1) * (rows // 2)] = upright[h * share : (h + 1) * share].astype(BF16)

    half = rows // 2
    for p in range(pieces):
        at = slice(p * piece_rows, (p + 1) * piece_rows)
        drain(pre_recv.at[1:groups, at, :], g_recv.at[p])
        for h in range(2):
            gp_full[me, h * half + p * piece_rows : h * half + (p + 1) * piece_rows, :] = jnp.concatenate(
                [gp_all[k, at, h * share : (h + 1) * share].astype(F32) for k in range(groups)], axis=1
            ).astype(BF16)

    if square:
        span, mine, other = half, jnp.where(core == 0, column, row), jnp.where(core == 0, beside, above)
    else:
        span, mine, other = rows, 0, grp

    def piece_of(o, part_of):
        return gp_full.at[o, aligned(part_of * span, span, span), :]

    def climb_gp(o):
        return pltpu.make_async_remote_copy(
            src_ref=piece_of(o, mine), dst_ref=piece_of(o, mine),
            send_sem=sent_sem.at[5], recv_sem=line_sem.at[o // 2],
            device_id=(grp, jnp.minimum(chip + 1, chips - 1) * 2 + core), device_id_type=MESH,
        )

    def descend_gp(o):
        return pltpu.make_async_remote_copy(
            src_ref=piece_of(o, mine), dst_ref=piece_of(o, mine),
            send_sem=sent_sem.at[5], recv_sem=line_sem.at[o // 2],
            device_id=(grp, jnp.maximum(chip - 1, 0) * 2 + core), device_id_type=MESH,
        )

    def exchange_gp(o):
        return pltpu.make_async_remote_copy(
            src_ref=piece_of(o, mine), dst_ref=piece_of(o, mine),
            send_sem=sent_sem.at[8], recv_sem=other_sem.at[o // 2],
            device_id=(other, me), device_id_type=MESH,
        )

    def across_gp(o, part_of):
        return pltpu.make_async_remote_copy(
            src_ref=piece_of(o, part_of), dst_ref=piece_of(o, part_of),
            send_sem=sent_sem.at[9], recv_sem=across_sem.at[o // 2],
            device_id=(grp, partner), device_id_type=MESH,
        )

    whole_end = assisted and square
    next_in = jnp.where(chip == 0, 1, last - 1)

    def slab(o, c):
        return gp_full.at[o, :, columns(c)]

    def across_slab(o, c):
        return pltpu.make_async_remote_copy(
            src_ref=slab(o, c), dst_ref=slab(o, c),
            send_sem=sent_sem.at[9], recv_sem=cross_slab_sem.at[c],
            device_id=(grp, partner), device_id_type=MESH,
        )

    def beside_end(o):
        return ((o // 2 == 0) & (chip == 1)) | ((o // 2 == last) & (chip == last - 1))

    along = jnp.logical_not(is_end) if sliced else chip >= 0

    @pl.when(along & (chip < chips - 1))
    def _():
        climb_gp(me).start()

    @pl.when(along & (chip > 0))
    def _():
        descend_gp(me).start()

    if sliced:
        @pl.when(is_end)
        def _():
            for c in range(2):
                pltpu.make_async_remote_copy(
                    src_ref=slab(me, c), dst_ref=slab(me, c),
                    send_sem=sent_sem.at[5], recv_sem=slab_sem.at[c],
                    device_id=(grp, next_in * 2 + core), device_id_type=MESH,
                ).start()
    elif whole_end:
        @pl.when(is_end)
        def _():
            pltpu.make_async_remote_copy(
                src_ref=piece_of(me, 1 - mine), dst_ref=piece_of(me, 1 - mine),
                send_sem=sent_sem.at[5], recv_sem=other_sem.at[chip],
                device_id=(grp, next_in * 2 + core), device_id_type=MESH,
            ).start()

    for h in range(rows // span):
        across_gp(me, h).start()


    def gp_arrives(k):
        o = near(2 * k)
        climb_gp(o).wait_recv()

        @pl.when((o < me) & (chip < last - assisted))
        def _():
            climb_gp(o).start()

        @pl.when((o > me) & (chip > 0 + assisted))
        def _():
            descend_gp(o).start()

        if whole_end:
            @pl.when(jnp.logical_not(beside_end(o)))
            def _():
                exchange_gp(o).start()
        elif square:
            exchange_gp(o).start()
        across_gp(o, mine).start()

    def gp_completes(k):
        if square:
            o = near(2 * k)
            pltpu.make_async_remote_copy(
                src_ref=piece_of(o, 1 - mine), dst_ref=piece_of(o, 1 - mine),
                send_sem=sent_sem.at[8], recv_sem=other_sem.at[o // 2],
                device_id=(other, me), device_id_type=MESH,
            ).wait_recv()
            across_gp(o, 1 - mine).start()

    def gp_crossed(o):
        drain(gp_full.at[o], across_sem.at[o // 2])

    def weigh(o):
        chunk = width // n
        if chunk % 16 == 0:
            product = jnp.dot(
                msg_all[o].reshape(relations * chunk, rows), gp_full[o], preferred_element_type=F32
            )
            grad_w[...] = grad_w[...] + product.reshape(relations, chunk, width)
        else:
            for r in range(relations):
                grad_w[r] = grad_w[r] + jnp.dot(msg_all[o, r], gp_full[o], preferred_element_type=F32)

    def weigh_end(o):
        for r in range(relations):
            end_sum[r] = end_sum[r] + jnp.dot(msg_end[o, r], gp_full[o], preferred_element_type=F32)

    grad_w[...] = jnp.zeros(grad_w.shape, F32)
    end_sum[...] = jnp.zeros(end_sum.shape, F32)
    help_end = pltpu.make_async_remote_copy(
        src_ref=end_send, dst_ref=end_recv,
        send_sem=sent_sem.at[11], recv_sem=help_sem,
        device_id=(grp, helped * 2 + core), device_id_type=MESH,
    )

    @pl.loop(0, width // tile_width)
    def _(c):
        at = aligned(c * tile_width, tile_width, tile_width)
        for r in range(relations):
            rows_r = slice(r * rows, (r + 1) * rows)
            grads = lax.dot_general(
                gp_full[me], weights[r, at, :],
                (((1,), (1,)), ((), ())), preferred_element_type=F32,
            )
            gm[rows_r, at] = (grads * scale[rows_r, 0:1]).astype(BF16)

    lower, higher = slice(0, cut), slice(cut, width)

    def far(j):
        return near(n - j + 2 * lax.rem(j, 2))

    def reduce_part(o, i):
        if square:
            source = part.at[o, :, 1 - column, :, lower] if i == 1 else part.at[o, 1 - row, :, :, higher]
            target, peer = part_recv.at[o, i - 1], (beside, above)[i - 1]
        else:
            source, target, peer = part.at[o, rel(i)], part_recv.at[i, o], rel(i)
        return pltpu.make_async_remote_copy(
            src_ref=source, dst_ref=target,
            send_sem=sent_sem.at[6], recv_sem=d_recv.at[o],
            device_id=(peer, me), device_id_type=MESH,
        )

    def relay_part(o, w):
        return pltpu.make_async_remote_copy(
            src_ref=relay.at[o, w], dst_ref=relay_recv.at[o, w],
            send_sem=sent_sem.at[10], recv_sem=r_recv.at[o],
            device_id=((above, beside)[w], me), device_id_type=MESH,
        )

    def start_parts(z):
        product = jnp.dot(
            adj_t[aligned(z * 2 * blk, 2 * blk, blk), :], gm[...], preferred_element_type=F32
        )
        for v in range(2):
            o = z * 2 + v
            part[o] = product[v * blk : (v + 1) * blk].astype(BF16).reshape(part.shape[1:])
            for i in range(1, 3 if square else groups):
                reduce_part(o, i).start()

    @pl.loop(1, chips)
    def _(e):
        start_parts(near(n - 2 * e) // 2)

    far_chips = chips - 2
    is_inner = (chip == 1) | (chip == last - 1)
    low_side = chip <= 1

    def crosses(o, source):
        return ((source <= 1) & (o // 2 >= 2)) | ((source >= last - 1) & (o // 2 <= last - 2))

    def hand(o, device, landing, semaphore):
        return pltpu.make_async_remote_copy(
            src_ref=part_sum.at[o], dst_ref=landing,
            send_sem=sent_sem.at[7], recv_sem=semaphore,
            device_id=(grp, device), device_id_type=MESH,
        )

    def give_back(j):
        o = far(j)
        if not assisted:
            hand(o, o, part_back.at[me], back_sem).start()
            return
        slot = jnp.where(low_side, jnp.maximum(o // 2 - 2, 0), jnp.minimum(o // 2, far_chips - 1))
        odd = lax.rem(o, 2)
        over = crosses(o, chip)

        @pl.when(over & is_end)
        def _():
            hand(o, next_in * 2 + odd, inbox.at[slot, core], inbox_sem.at[slot]).start()

        @pl.when(over & is_inner & (odd != core))
        def _():
            hand(o, partner, crossed.at[slot], crossed_sem.at[slot]).start()

        @pl.when(jnp.logical_not(over & (is_end | is_inner)))
        def _():
            hand(o, o, part_back.at[me], back_sem).start()

    def collect(slot):
        z = jnp.where(low_side, slot + 2, slot)
        side = jnp.where(low_side, 0, 1)
        return pltpu.make_async_remote_copy(
            src_ref=gathered_sum.at[slot], dst_ref=collected.at[side],
            send_sem=sent_sem.at[12], recv_sem=collect_sem.at[side],
            device_id=(grp, z * 2 + core), device_id_type=MESH,
        )

    def sum_for_far_side(first=0, past=far_chips):
        outer = jnp.where(low_side, 0, last)

        @pl.loop(first, past)
        def _(i):
            slot = jnp.where(low_side, far_chips - 1 - i, i)
            drain(crossed.at[slot], crossed_sem.at[slot])
            drain(inbox.at[slot], inbox_sem.at[slot])
            o = jnp.where(low_side, slot + 2, slot) * 2 + core
            terms = (
                (me, part_sum[o].astype(F32)),
                (partner, crossed[slot].astype(F32)),
                (outer * 2, inbox[slot, 0].astype(F32)),
                (outer * 2 + 1, inbox[slot, 1].astype(F32)),
            )
            for k in range(sections):
                total = None
                for t, term in terms:
                    kept = term * is_one(table[t, o] == k)
                    total = kept if total is None else total + kept
                gathered_sum[slot, k] = total.astype(BF16)
            collect(slot).start()

    def relayed(o):
        if square:
            drain(part_recv.at[o], d_recv.at[o])
            up = part[o, 1 - row, column, :, lower].astype(F32) + part_recv[o, 0, 1 - row].astype(F32)
            relay[o, 0] = up.astype(BF16)
            relay_part(o, 0).start()
            aside = part[o, row, 1 - column, :, higher].astype(F32) + part_recv[o, 1, 1 - column].astype(F32)
            relay[o, 1] = aside.astype(BF16)
            relay_part(o, 1).start()

    def reduced(o):
        if square:
            drain(relay_recv.at[o], r_recv.at[o])
            first = part[o, row, column, :, lower].astype(F32) + part_recv[o, 0, row].astype(F32)
            second = part[o, row, column, :, higher].astype(F32) + part_recv[o, 1, column].astype(F32)
            first = first + relay_recv[o, 0].astype(F32)
            second = second + relay_recv[o, 1].astype(F32)
            return jnp.concatenate([first, second], axis=1).astype(BF16)
        total = part[o, grp].astype(F32)
        drain(part_recv.at[1:groups, o], d_recv.at[o])
        for i in range(1, groups):
            total = total + part_recv[i, o].astype(F32)
        return total.astype(BF16)

    def send_reduced(j):
        part_sum[far(j)] = reduced(far(j))
        give_back(j)

    relays = both > 0
    weigh(me)

    def slab_arrives(c):
        drain(slab(outer_chip * 2 + core, c), slab_sem.at[c])
        outer = outer_chip * 2 + core
        across_slab(outer, c).start()
        ahead = gp_full.at[outer, aligned(mine * span, span, span), columns(c)]
        pltpu.make_async_remote_copy(
            src_ref=ahead, dst_ref=ahead,
            send_sem=sent_sem.at[5], recv_sem=line_sem.at[outer_chip],
            device_id=(grp, jnp.where(chip == 1, 2, last - 2) * 2 + core), device_id_type=MESH,
        ).start()

    def help_slab(c):
        other = outer_chip * 2 + 1 - core
        drain(slab(other, c), cross_slab_sem.at[c])
        for r in range(relations):
            total = None
            for o in (me, partner, outer_chip * 2 + core, other):
                product = jnp.dot(msg_end[o, r], gp_full[o, :, c * cut : (c + 1) * cut], preferred_element_type=F32)
                total = product if total is None else total + product
            end_send[r, :, c * cut : (c + 1) * cut] = total.astype(BF16)
        pltpu.make_async_remote_copy(
            src_ref=end_send.at[:, :, columns(c)], dst_ref=end_recv.at[:, :, columns(c)],
            send_sem=sent_sem.at[11], recv_sem=help_sem,
            device_id=(grp, helped * 2 + core), device_id_type=MESH,
        ).start()

    if sliced:
        @pl.when(is_end)
        def _():
            gp_arrives(1)
            relayed(far(2))
            relayed(far(3))
            start_next_messages()
            relayed(far(4))
            relayed(far(5))

        @pl.when(jnp.logical_not(is_end))
        def _():
            gp_arrives(3 - outward)
            slab_arrives(0)
            relayed(far(2))
            relayed(far(3))
            gp_crossed(partner)
            drain(msg_end.at[: 2 * (chips - 2) - 1], end_sem)
            help_slab(0)
            slab_arrives(1)
            relayed(far(4))
            relayed(far(5))
            help_slab(1)
    else:
        gp_arrives(1)

        @pl.when(relays)
        def _():
            gp_arrives(2)

        @pl.loop(2, n - 2)
        def _(j):
            relayed(far(j))

    start_parts(chip)

    sides = jnp.where(helped == 0, last - chip, chip)

    def beyond(i):
        return jnp.where(helped == 0, chip + 1, chip - 1 - (sides - 1)) + i

    def complete(k):
        gp_completes(k)
        gp_crossed(near(2 * k + 1))

    if assisted and soon and not sliced:
        @pl.when(is_agent)
        def _():
            complete(outward)
            gp_crossed(partner)

    def help_out():
        drain(msg_end.at[: 2 * (chips - 2) - 1], end_sem)
        weigh_end(me)
        weigh_end(partner)

        @pl.loop(0, sides)
        def _(i):
            weigh_end(beyond(i) * 2)
            weigh_end(beyond(i) * 2 + 1)

        end_send[...] = end_sum[...].astype(BF16)
        help_end.start()

    if assisted and soon and not sliced:
        pl.when(is_agent)(help_out)

    if not sliced:
        pl.when(is_end)(start_next_messages)
    if not assisted:
        @pl.when(jnp.logical_not(relays))
        def _():
            gp_arrives(2)

    relayed(far(n - 2))
    relayed(far(n - 1))

    if not sliced:
        @pl.when(relays)
        def _():
            @pl.loop(3, chips)
            def _(k):
                gp_arrives(k)


    @pl.loop(2, n - 2)
    def _(j):
        send_reduced(j)

    relayed(partner)
    relayed(me)
    send_reduced(n - 2)
    send_reduced(n - 1)

    if sliced:
        @pl.when(relays)
        def _():
            sum_for_far_side(0, 1)
            gp_arrives(3)

    if not assisted:
        @pl.when(jnp.logical_not(relays))
        def _():
            @pl.loop(3, chips)
            def _(k):
                gp_arrives(k)

    if assisted:
        pl.when(is_inner)(functools.partial(sum_for_far_side, 1 if sliced else 0))

    if assisted:
        @pl.when(is_end)
        def _():
            drain(msg_all.at[:3], msg_sem)

        @pl.when(jnp.logical_not(is_end))
        def _():
            drain(msg_all.at[: n - 1], msg_sem)
    else:
        drain(msg_all.at[: n - 1], msg_sem)

    if sliced:
        @pl.when(is_end)
        def _():
            gp_completes(1)
            gp_crossed(partner)
            weigh(partner)
            weigh(near(2))

        @pl.when(jnp.logical_not(is_end))
        def _():
            inward = 3 - outward

            @pl.loop(0, 3)
            def _(i):
                weigh(jnp.where(i == 0, partner, near(2 * outward + jnp.maximum(i - 1, 0))))

            gp_completes(inward)
            weigh(near(2 * inward))
            gp_crossed(near(2 * inward + 1))
            weigh(near(2 * inward + 1))
            gp_completes(3)

    part_sum[partner] = reduced(partner)
    give_partner = pltpu.make_async_remote_copy(
        src_ref=part_sum.at[partner], dst_ref=part_back.at[me],
        send_sem=sent_sem.at[7], recv_sem=back_sem,
        device_id=(grp, partner), device_id_type=MESH,
    )
    give_partner.start()
    part_back[me] = reduced(me)

    if sliced:
        @pl.when(is_end)
        def _():
            gp_crossed(near(3))
            weigh(near(3))

        @pl.when(jnp.logical_not(is_end))
        def _():
            weigh(near(6))
            gp_crossed(near(7))
            weigh(near(7))
    else:
        reach = jnp.where(is_end, 2, chips) if assisted else chips
        waited = jnp.where(is_agent, outward, 0) if assisted and soon else 0

        @pl.loop(1, reach)
        def _(k):
            @pl.when(k != waited)
            def _():
                gp_completes(k)

        @pl.loop(1, reach)
        def _(k):
            @pl.when(k != waited)
            def _():
                gp_crossed(near(2 * k + 1))

        if assisted and soon:
            @pl.when(is_end)
            def _():
                gp_crossed(partner)
        else:
            gp_crossed(partner)

        weigh(partner)

        @pl.loop(1, reach)
        def _(k):
            weigh(near(2 * k))
            weigh(near(2 * k + 1))

        if assisted and not soon:
            pl.when(is_agent)(help_out)

    for k in range(sections):
        grad_f[k] = jnp.zeros((quarter, width), F32)

    if assisted:
        for z in range(chips):
            direct = n - 1 - 4 * (z >= 2) - 4 * (z <= last - 2)

            @pl.when(chip == z)
            def _():
                drain(part_sum.at[:direct], back_sem)
    else:
        drain(part_sum.at[: n - 1], back_sem)

    @pl.loop(0, n)
    def _(t):
        def add():
            wanted = table[t, me]
            addend = part_back[t].astype(F32)
            for k in range(sections):
                grad_f[k] = grad_f[k] + addend * is_one(wanted == k)

        if assisted:
            pl.when(jnp.logical_not(crosses(me, t // 2)))(add)
        else:
            add()

    if assisted:
        for side, has in ((0, chip >= 2), (1, chip <= last - 2)):
            @pl.when(has)
            def _():
                drain(collected.at[side], collect_sem.at[side])
                grad_f[...] = grad_f[...] + collected[side].astype(F32)

        @pl.when(is_end)
        def _():
            drain(end_recv, help_sem)
            grad_w[...] = grad_w[...] + end_recv[...].astype(F32)

    fetch_pair.wait_send()
    for z in range(chips):
        near_by = (z > 0) + (z < chips - 1)
        relayed = 2 * (0 < z < chips - 1)
        far = sum(abs(y - z) > 2 for y in range(chips))

        @pl.when(chip == z)
        def _():
            drain(gathered.at[: near_by + relayed + far + chips - 1], sent_sem.at[0])

    drain(fetched.at[: (n - 2) * (groups - 1) * quarter, :], sent_sem.at[1])
    drain(pre_recv.at[1:groups], sent_sem.at[2])
    drain(pre_recv.at[1:groups], sent_sem.at[3])
    if assisted:
        @pl.when(is_agent)
        def _():
            drain(msg_all.at[: n - 2], sent_sem.at[4])
            drain(end_send, sent_sem.at[11])

        @pl.when(jnp.logical_not(is_agent))
        def _():
            drain(msg_all.at[: n - 1], sent_sem.at[4])
    else:
        drain(msg_all.at[: n - 1], sent_sem.at[4])

    for z in range(chips):
        at_end = z in (0, last)
        climbs = z * (z + 1 <= last - assisted) + (z < last)
        descents = (last - z) * (z - 1 >= 0 + assisted) + (z > 0)
        climbs, descents = (climbs if z < last else 0), (descents if z > 0 else 0)
        if at_end:
            climbs, descents = int(z == 0), int(z == last)
        known = 1 if at_end and assisted else last
        doubled = int(at_end and assisted and square)
        swapped = known - (assisted and z in (1, last - 1))

        @pl.when(chip == z)
        def _():
            if square:
                drain(fetched.at[: (climbs + descents + doubled) * span, :], sent_sem.at[5])
                drain(fetched.at[: swapped * span, :], sent_sem.at[8])
            else:
                drain(gp_full.at[: climbs + descents], sent_sem.at[5])
            drain(gp_full.at[: known + 1], sent_sem.at[9])

    if square:
        drain(part_recv, sent_sem.at[6])
        drain(relay_recv, sent_sem.at[10])
    else:
        drain(part_recv.at[1:groups], sent_sem.at[6])
    if assisted:
        @pl.when(is_inner)
        def _():
            drain(part_sum.at[: n - 1 - far_chips], sent_sem.at[7])
            drain(gathered_sum, sent_sem.at[12])

        @pl.when(jnp.logical_not(is_inner))
        def _():
            drain(part_sum.at[: n - 1], sent_sem.at[7])
    else:
        drain(part_sum.at[: n - 1], sent_sem.at[7])


def hand_over(*refs):
    copies = [pltpu.make_async_copy(refs[k], refs[3 + k], refs[6].at[k]) for k in range(3)]
    for copy in copies:
        copy.start()
    for copy in copies:
        copy.wait()


def per_device(
    n, groups,
    features, weights, bias, cotangent, tile_values, tile_count, tile_slot, source_blocks,
):
    rows, width = features.shape
    relations, _, slot_total, blk = tile_values.shape
    sections = rows // blk
    quarter, share, chunk, chips = blk // groups, width // groups, width // n, n // 2
    half = rows // 2
    square = groups == 4
    grid = (2, 2) if square else (groups,)
    vmem = pl.BlockSpec(memory_space=pltpu.VMEM)
    smem = pl.BlockSpec(memory_space=pltpu.SMEM)
    anywhere = pl.BlockSpec(memory_space=pl.ANY)
    hbm = pl.BlockSpec(memory_space=pltpu.HBM)
    dma = pltpu.SemaphoreType.DMA
    out, grad_w, grad_f = pl.pallas_call(
        functools.partial(kernel, n, groups),
        out_shape=(
            pltpu.VMEM((share, rows), BF16),
            pltpu.VMEM((relations, chunk, width), F32),
            pltpu.VMEM((sections, quarter, width), F32),
        ),
        in_specs=[smem, smem, smem, hbm, hbm, vmem, hbm, hbm],
        out_specs=(vmem, vmem, vmem),
        scratch_shapes=[
            pltpu.VMEM((relations, width, width), BF16),
            pltpu.VMEM((relations, rows * slot_total, blk), jnp.int32),
            pltpu.VMEM((sections, groups, quarter, width), BF16),
            pltpu.VMEM((rows, width), BF16),
            pltpu.VMEM((n, sections, quarter, width), BF16),
            pltpu.VMEM((blk, width), BF16),
            pltpu.VMEM((slot_total, blk, blk), BF16),
            pltpu.VMEM((slot_total, blk, blk), BF16),
            pltpu.VMEM((n * blk, width), BF16),
            pltpu.VMEM((relations * rows, n * blk), BF16),
            pltpu.VMEM((relations * rows, 128), F32),
            pltpu.VMEM((relations, width, rows), F32),
            pltpu.VMEM((relations * rows, width), BF16),
            pltpu.VMEM((n, relations, chunk, rows), BF16),
            pltpu.VMEM((n, relations, chunk, rows), BF16),
            pltpu.VMEM((n, relations, chunk, rows), BF16),
            pltpu.VMEM((relations, chunk, width), F32),
            pltpu.VMEM((relations, chunk, width), BF16),
            pltpu.VMEM((relations, chunk, width), BF16),
            pltpu.VMEM((n * blk, relations * rows), BF16),
            pltpu.VMEM((rows, width), F32),
            pltpu.VMEM((groups, half, 2 * share), BF16),
            pltpu.VMEM((groups, half, 2 * share), BF16),
            pltpu.VMEM((half, 2 * share), F32),
            pltpu.VMEM((half, 2 * share), F32),
            pltpu.VMEM((1, 2 * share), F32),
            pltpu.VMEM((groups, half, 2 * share), BF16),
            pltpu.VMEM((n, rows, width), BF16),
            pltpu.VMEM((relations * rows, width), BF16),
            pltpu.VMEM((n, *grid, quarter, width), BF16),
            pltpu.VMEM((n, 2, 2, quarter, width // 2) if square else (groups, n, quarter, width), BF16),
            pltpu.VMEM((n, 2, quarter, width // 2), BF16),
            pltpu.VMEM((n, 2, quarter, width // 2), BF16),
            pltpu.VMEM((n, quarter, width), BF16),
            pltpu.VMEM((n, quarter, width), BF16),
            pltpu.VMEM((chips - 2, 2, quarter, width), BF16),
            pltpu.VMEM((chips - 2, quarter, width), BF16),
            pltpu.VMEM((chips - 2, sections, quarter, width), BF16),
            pltpu.VMEM((2, sections, quarter, width), BF16),
            dma((4,)), dma((2,)), dma((13,)), dma, dma, dma, dma, dma((chips - 2,)), dma((chips - 2,)), dma((2,)), dma((2,)), dma((2,)),
            dma((n, 2)), dma((n, 2)),
            dma((4,)), dma((4,)), dma((n,)), dma((n,)), dma,
            dma((chips,)), dma((chips,)), dma((chips,)),
        ],
        compiler_params=pltpu.CompilerParams(
            collective_id=0, has_side_effects=True, vmem_limit_bytes=60 << 20
        ),
        name="layer",
    )(
        source_blocks, tile_count, tile_slot,
        features.reshape(sections, groups, quarter, width), cotangent, bias,
        tile_values.reshape(relations, rows * slot_total, blk), weights,
    )
    results = (out, grad_w, grad_f)
    out, grad_w, grad_f = pl.pallas_call(
        hand_over,
        out_shape=tuple(jax.ShapeDtypeStruct(x.shape, x.dtype) for x in results),
        in_specs=[vmem] * 3,
        out_specs=(anywhere,) * 3,
        scratch_shapes=[dma((3,))],
        compiler_params=pltpu.CompilerParams(vmem_limit_bytes=4 << 20),
        name="hand_over",
    )(*results)
    return (out.T, grad_w, grad_f)


def solution(mesh):
    placed = (
        P("tgt", None),
        P("rel", None, None),
        P(),
        P("tgt", None),
        P("rel", "tgt", None, None),
        P("rel", "tgt"),
        P("rel", "tgt", None),
        P(),
    )
    return jax.shard_map(
        functools.partial(per_device, mesh.shape["tgt"], mesh.shape["rel"]),
        mesh=mesh,
        in_specs=placed,
        out_specs=(P("tgt", "rel"), P("rel", "tgt", None), P("tgt", "rel", None)),
        check_vma=False,
    )
```

```python
import functools

import jax
import jax.numpy as jnp
from jax import lax
from jax.experimental import pallas as pl
from jax.experimental.pallas import tpu as pltpu
from jax.sharding import PartitionSpec as P

MESH = pl.DeviceIdType.MESH
F32 = jnp.float32
BF16 = jnp.bfloat16


def aligned(start, size, multiple):
    return pl.ds(pl.multiple_of(start, multiple), size)


def is_one(condition):
    return condition.astype(jnp.int32).astype(F32)


def pack(value, first, width):
    half = value.shape[0] // 2
    return jnp.concatenate(
        [value[:half, first : first + width], value[half:, first : first + width]], axis=1
    )


def drain(view, semaphore):
    pltpu.make_async_copy(view, view, semaphore).wait()


def kernel(
    n, groups,
    table, counts, slots,
    feat_hbm, cot_hbm, bias, values_hbm, weights_hbm,
    out, grad_w, grad_f,
    weights, values, feat, cot, gathered, partner_staged, masked, masked_t, fetched, adj, scale, turned_scratch, msg, msg_t, msg_all, msg_end, end_sum, end_send, end_recv, adj_t, pre,
    pre_send, pre_recv, cot_own, active, bias_own, gp_all, gp_full, gm,
    part, part_recv, relay, relay_recv, part_sum, part_back, inbox, crossed, gathered_sum, collected,
    load_sem, pair_sem, sent_sem, spread_sem, back_sem, end_sem, help_sem, inbox_sem, crossed_sem, collect_sem, slab_sem, cross_slab_sem,
    a_recv, b_recv, p_recv, g_recv, d_recv, r_recv, msg_sem, line_sem, other_sem, across_sem,
):
    me = lax.axis_index("tgt")
    grp = lax.axis_index("rel")
    sections, _, quarter, width = feat.shape
    blk = quarter * groups
    rows = sections * blk
    relations = weights.shape[0]
    slot_total = slots.shape[2]
    share = width // groups
    chips = n // 2
    chip, core = me // 2, lax.rem(me, 2)

    def tgt(j):
        return lax.rem(chip + j // 2, chips) * 2 + lax.rem(core + lax.rem(j, 2), 2)

    below, above_me = chip, chips - 1 - chip
    both = jnp.minimum(below, above_me)
    assisted = chips == 4 or chips > 5
    last = chips - 1
    is_end = (chip == 0) | (chip == last)
    agent_low, agent_high = 2, last - 2
    soon = chips == 4
    sliced = soon and groups == 4
    outward = jnp.where(chip == 1, 2, 1)
    outer_chip = jnp.where(chip == 1, 0, last)
    helped = jnp.where(chip == agent_low, 0, last)
    is_agent = (chip == agent_low) | (chip == agent_high)

    def near(j):
        k = j // 2 - 1
        two_sided = jnp.where(lax.rem(k, 2) == 0, chip + k // 2 + 1, chip - k // 2 - 1)
        distance = k - both + 1
        one_sided = jnp.where(above_me > below, chip + distance, chip - distance)
        return jnp.where(k < 2 * both, two_sided, one_sided) * 2 + lax.rem(core + lax.rem(j, 2), 2)

    partner = chip * 2 + 1 - core
    row, column = grp // 2, lax.rem(grp, 2)
    beside = row * 2 + 1 - column
    above = (1 - row) * 2 + column

    square = groups == 4

    def rel(i):
        if square:
            return (grp, beside, above, (1 - row) * 2 + 1 - column)[i]
        return lax.rem(grp + i, groups)

    load_w = pltpu.make_async_copy(weights_hbm, weights, load_sem.at[0])
    load_v = pltpu.make_async_copy(values_hbm, values, load_sem.at[1])
    load_f = pltpu.make_async_copy(feat_hbm, feat, load_sem.at[2])
    load_c = pltpu.make_async_copy(cot_hbm, cot, load_sem.at[3])
    load_v.start()
    load_f.start()
    load_w.start()
    load_c.start()

    barrier = pltpu.get_barrier_semaphore()

    @pl.loop(1, n)
    def _(j):
        pl.semaphore_signal(barrier, inc=1, device_id=(grp, tgt(j)), device_id_type=MESH)

    for i in range(1, groups):
        pl.semaphore_signal(barrier, inc=1, device_id=(rel(i), me), device_id_type=MESH)

    def whole_block(t):
        total = jnp.zeros((blk, width), F32)
        for k in range(sections):
            total = total + feat[k].reshape(blk, width).astype(F32) * is_one(table[t, me] == k)
        return total.astype(BF16)

    pl.semaphore_wait(barrier, n - 1 + groups - 1)

    cut = width // 2

    def columns(h):
        return aligned(h * cut, cut, 128)

    def climb_rows(o, h, source):
        return pltpu.make_async_remote_copy(
            src_ref=source, dst_ref=gathered.at[o, :, :, columns(h)],
            send_sem=sent_sem.at[0], recv_sem=a_recv.at[o, h],
            device_id=(grp, jnp.minimum(chip + 1, chips - 1) * 2 + core), device_id_type=MESH,
        )

    def descend_rows(o, h, source):
        return pltpu.make_async_remote_copy(
            src_ref=source, dst_ref=gathered.at[o, :, :, columns(h)],
            send_sem=sent_sem.at[0], recv_sem=a_recv.at[o, h],
            device_id=(grp, jnp.maximum(chip - 1, 0) * 2 + core), device_id_type=MESH,
        )

    def across_rows(o, h):
        return pltpu.make_async_remote_copy(
            src_ref=gathered.at[o, :, :, columns(h)], dst_ref=gathered.at[o, :, :, columns(h)],
            send_sem=sent_sem.at[0], recv_sem=a_recv.at[o, h],
            device_id=(grp, partner), device_id_type=MESH,
        )

    fetch_pair = pltpu.make_async_remote_copy(
        src_ref=partner_staged, dst_ref=fetched.at[aligned(me * blk, blk, blk), :],
        send_sem=pair_sem.at[0], recv_sem=pair_sem.at[1],
        device_id=(grp, partner), device_id_type=MESH,
    )

    def leap_rows(z, h):
        return pltpu.make_async_remote_copy(
            src_ref=feat_hbm.at[:, grp, :, columns(h)], dst_ref=gathered.at[me, :, :, columns(h)],
            send_sem=sent_sem.at[0], recv_sem=a_recv.at[me, h],
            device_id=(grp, z * 2 + core), device_id_type=MESH,
        )

    for h in range(2):
        @pl.when(chip < chips - 1)
        def _():
            climb_rows(me, h, feat_hbm.at[:, grp, :, columns(h)]).start()

        @pl.when(chip > 0)
        def _():
            descend_rows(me, h, feat_hbm.at[:, grp, :, columns(h)]).start()

    @pl.loop(0, chips)
    def _(z):
        @pl.when((z > chip + 2) | (z < chip - 2))
        def _():
            for h in range(2):
                leap_rows(z, h).start()

    load_f.wait()
    partner_staged[...] = whole_block(partner)
    fetch_pair.start()
    fetched[aligned(me * blk, blk, blk), :] = whole_block(me)

    sent = range(4) if square else range(groups - 1)

    def spread(j, h, way):
        if square:
            size = quarter if way < 2 else quarter // 2
            source = (grp, grp, beside, above)[way]
            extra = quarter // 2 if way == 3 else 0
            peer = (beside, above, above, beside)[way]
        else:
            size, source, extra, peer = quarter, grp, 0, rel(way + 1)
        rows_at = aligned(near(j) * blk + source * quarter + extra, size, size)
        return pltpu.make_async_remote_copy(
            src_ref=fetched.at[rows_at, columns(h)], dst_ref=fetched.at[rows_at, columns(h)],
            send_sem=sent_sem.at[1],
            recv_sem=b_recv.at[j, h] if square and way < 2 else spread_sem,
            device_id=(peer, me), device_id_type=MESH,
        )

    first_hop = sent[:2] if square else sent

    def event(e):
        inner = lax.rem(e, 4)
        paired = e < 4 * both
        k = jnp.where(paired, e // 4 * 2 + 1 + lax.rem(inner, 2), e // 2 + 1)
        return k, jnp.where(paired, inner // 2, lax.rem(e, 2))

    def pass_on(e, side):
        k, h = event(e)
        j = 2 * k + side
        if not square:
            return
        drain(fetched.at[: 2 * quarter, columns(h)], b_recv.at[j, h])
        spread(j, h, 2).start()
        spread(j, h, 3).start()

    def placed(j, h):
        o = near(j)
        total = jnp.zeros((quarter, cut), F32)
        for k in range(sections):
            total = total + gathered[o, k, :, columns(h)].astype(F32) * is_one(table[me, o] == k)
        fetched[aligned(o * blk + grp * quarter, quarter, quarter), columns(h)] = total.astype(BF16)
        for way in first_hop:
            spread(j, h, way).start()

    def arrive(e):
        k, h = event(e)
        o = near(2 * k)
        across_rows(o, h).wait_recv()

        @pl.when((o // 2 == chip - 1) & (chip < chips - 1))
        def _():
            climb_rows(o, h, gathered.at[o, :, :, columns(h)]).start()

        @pl.when((o // 2 == chip + 1) & (chip > 0))
        def _():
            descend_rows(o, h, gathered.at[o, :, :, columns(h)]).start()

        across_rows(o, h).start()
        placed(2 * k, h)

    def arrive_across(e):
        k, h = event(e)
        across_rows(near(2 * k + 1), h).wait_recv()
        placed(2 * k + 1, h)

    load_v.wait()

    def adjacency(b):
        r, q = b // sections, lax.rem(b, sections)
        count = counts[r, q]
        total = jnp.zeros((blk, blk), F32)
        for s in range(slot_total):
            start = (q * blk * slot_total) + s
            tile = values[r, pl.ds(start, blk, stride=slot_total), :].astype(F32) * is_one(s < count)
            masked[s] = tile.astype(BF16)
            masked_t[s] = tile.T.astype(BF16)
            total = total + tile
        degree = jnp.sum(total, axis=1, keepdims=True)
        root = 1.0 / jnp.sqrt(jnp.maximum(degree, 1.0))
        scale[aligned(b * blk, blk, blk), :] = jnp.broadcast_to(root, (blk, 128))

        @pl.loop(0, n)
        def _(o):
            entry = jnp.zeros((blk, blk), BF16)
            entry_t = jnp.zeros((blk, blk), BF16)
            for s in range(slot_total):
                here = jnp.full((blk, blk), is_one(slots[r, q, s] == o), F32).astype(BF16)
                entry = entry + masked[s] * here
                entry_t = entry_t + masked_t[s] * here
            adj[aligned(b * blk, blk, blk), aligned(o * blk, blk, blk)] = entry
            adj_t[aligned(o * blk, blk, blk), aligned(b * blk, blk, blk)] = entry_t

    blocks = relations * sections

    @pl.loop(0, blocks // 2)
    def _(b):
        adjacency(b)

    events = 2 * (chips - 1)
    arrive(0)
    arrive(1)

    @pl.loop(0, blocks // 2)
    def _(b):
        adjacency(blocks // 2 + b)
        arrive_across(b)
        arrive(2 + b)

    @pl.loop(blocks // 2 + 2, events)
    def _(e):
        arrive(e)
        arrive_across(e - 2)

    pass_on(0, 0)
    arrive_across(events - 2)
    pass_on(0, 1)
    arrive_across(events - 1)

    @pl.loop(1, events)
    def _(e):
        pass_on(e, 0)
        pass_on(e, 1)

    load_w.wait()
    fetch_pair.wait_recv()

    late = n - 2 if square else (n - 2) * (groups - 1)
    drain(fetched.at[: late * quarter, :], spread_sem)

    tile_width = 256
    chunk = width // n
    for c in range(width // tile_width):
        at = slice(c * tile_width, (c + 1) * tile_width)
        acc = jnp.dot(adj[...], fetched[:, at], preferred_element_type=F32) * scale[:, 0:1]
        msg[:, at] = acc.astype(BF16)
        for r in range(relations):
            turned_scratch[r, at, :] = acc[r * rows : (r + 1) * rows, :].T

    for r in range(relations):
        msg_t[:, r] = turned_scratch[r].reshape(n, chunk, rows).astype(BF16)

    def send_messages(target, z, landing, semaphore):
        return pltpu.make_async_remote_copy(
            src_ref=msg_t.at[target], dst_ref=landing.at[me],
            send_sem=sent_sem.at[4], recv_sem=semaphore,
            device_id=(grp, z * 2 + lax.rem(target, 2)), device_id_type=MESH,
        )

    def start_messages(j):
        target = near(j)
        z = target // 2
        if not assisted:
            send_messages(target, z, msg_all, msg_sem).start()
            return
        away = ((z == 0) & (chip >= agent_low)) | ((z == last) & (chip <= agent_high))

        @pl.when(jnp.logical_not(away))
        def _():
            send_messages(target, z, msg_all, msg_sem).start()

        agent = jnp.where(z == 0, agent_low, agent_high)

        @pl.when(away & jnp.logical_not((agent == chip) & (lax.rem(target, 2) == core)))
        def _():
            send_messages(target, agent, msg_end, end_sem).start()

    @pl.loop(4, n)
    def _(j):
        start_messages(n + 3 - j)

    def start_next_messages():
        start_messages(2)
        start_messages(3)

    pl.when(jnp.logical_not(is_end))(start_next_messages)

    send_messages(partner, chip, msg_all, msg_sem).start()

    @pl.loop(0, width // tile_width)
    def _(c):
        at = aligned(c * tile_width, tile_width, tile_width)
        total = None
        for r in range(relations):
            part_r = jnp.dot(
                msg[r * rows : (r + 1) * rows, :], weights[r, :, at], preferred_element_type=F32
            )
            total = part_r if total is None else total + part_r
        pre[:, at] = total

    whole = pre[...]
    for k in range(groups):
        pre_send[k] = pack(whole, k * share, share).astype(BF16)

    pieces = 4
    piece_rows = rows // 2 // pieces

    def reduce_pre(i, p):
        at = slice(p * piece_rows, (p + 1) * piece_rows)
        return pltpu.make_async_remote_copy(
            src_ref=pre_send.at[rel(i), at, :], dst_ref=pre_recv.at[i, at, :],
            send_sem=sent_sem.at[2], recv_sem=p_recv.at[p],
            device_id=(rel(i), me), device_id_type=MESH,
        )

    for p in range(pieces):
        for i in range(1, groups):
            reduce_pre(i, p).start()

    msg_all[me] = msg_t[me]
    if assisted:
        msg_end[me] = msg_t[helped * 2 + core]
    load_c.wait()
    for k in range(groups):
        @pl.when(grp == k)
        def _():
            cot_own[...] = pack(cot[...].astype(F32), k * share, share)
            piece = bias[...].reshape(1, width)[:, k * share : (k + 1) * share]
            bias_own[...] = jnp.concatenate([piece, piece], axis=1)

    def gather_gp(i, p):
        at = slice(p * piece_rows, (p + 1) * piece_rows)
        return pltpu.make_async_remote_copy(
            src_ref=gp_all.at[grp, at, :], dst_ref=gp_all.at[grp, at, :],
            send_sem=sent_sem.at[3], recv_sem=g_recv.at[p],
            device_id=(rel(i), me), device_id_type=MESH,
        )

    for p in range(pieces):
        at = slice(p * piece_rows, (p + 1) * piece_rows)
        total = pre_send[grp, at, :].astype(F32)
        drain(pre_recv.at[1:groups, at, :], p_recv.at[p])
        for i in range(1, groups):
            total = total + pre_recv[i, at, :].astype(F32)
        pre_act = total + bias_own[...]
        sigmoid = jax.nn.sigmoid(pre_act)
        derivative = sigmoid * (1.0 + pre_act * (1.0 - sigmoid))
        gp_all[grp, at, :] = (cot_own[at, :] * derivative).astype(BF16)
        for i in range(1, groups):
            gather_gp(i, p).start()
        active[at, :] = pre_act * sigmoid

    upright = active[...].T
    for h in range(2):
        out[:, h * (rows // 2) : (h + 1) * (rows // 2)] = upright[h * share : (h + 1) * share].astype(BF16)

    half = rows // 2
    for p in range(pieces):
        at = slice(p * piece_rows, (p + 1) * piece_rows)
        drain(pre_recv.at[1:groups, at, :], g_recv.at[p])
        for h in range(2):
            gp_full[me, h * half + p * piece_rows : h * half + (p + 1) * piece_rows, :] = jnp.concatenate(
                [gp_all[k, at, h * share : (h + 1) * share].astype(F32) for k in range(groups)], axis=1
            ).astype(BF16)

    if square:
        span, mine, other = half, jnp.where(core == 0, column, row), jnp.where(core == 0, beside, above)
    else:
        span, mine, other = rows, 0, grp

    def piece_of(o, part_of):
        return gp_full.at[o, aligned(part_of * span, span, span), :]

    def climb_gp(o):
        return pltpu.make_async_remote_copy(
            src_ref=piece_of(o, mine), dst_ref=piece_of(o, mine),
            send_sem=sent_sem.at[5], recv_sem=line_sem.at[o // 2],
            device_id=(grp, jnp.minimum(chip + 1, chips - 1) * 2 + core), device_id_type=MESH,
        )

    def descend_gp(o):
        return pltpu.make_async_remote_copy(
            src_ref=piece_of(o, mine), dst_ref=piece_of(o, mine),
            send_sem=sent_sem.at[5], recv_sem=line_sem.at[o // 2],
            device_id=(grp, jnp.maximum(chip - 1, 0) * 2 + core), device_id_type=MESH,
        )

    def exchange_gp(o):
        return pltpu.make_async_remote_copy(
            src_ref=piece_of(o, mine), dst_ref=piece_of(o, mine),
            send_sem=sent_sem.at[8], recv_sem=other_sem.at[o // 2],
            device_id=(other, me), device_id_type=MESH,
        )

    def across_gp(o, part_of):
        return pltpu.make_async_remote_copy(
            src_ref=piece_of(o, part_of), dst_ref=piece_of(o, part_of),
            send_sem=sent_sem.at[9], recv_sem=across_sem.at[o // 2],
            device_id=(grp, partner), device_id_type=MESH,
        )

    whole_end = assisted and square
    next_in = jnp.where(chip == 0, 1, last - 1)

    def slab(o, c):
        return gp_full.at[o, :, columns(c)]

    def across_slab(o, c):
        return pltpu.make_async_remote_copy(
            src_ref=slab(o, c), dst_ref=slab(o, c),
            send_sem=sent_sem.at[9], recv_sem=cross_slab_sem.at[c],
            device_id=(grp, partner), device_id_type=MESH,
        )

    def beside_end(o):
        return ((o // 2 == 0) & (chip == 1)) | ((o // 2 == last) & (chip == last - 1))

    along = jnp.logical_not(is_end) if sliced else chip >= 0

    @pl.when(along & (chip < chips - 1))
    def _():
        climb_gp(me).start()

    @pl.when(along & (chip > 0))
    def _():
        descend_gp(me).start()

    if sliced:
        @pl.when(is_end)
        def _():
            for c in range(2):
                pltpu.make_async_remote_copy(
                    src_ref=slab(me, c), dst_ref=slab(me, c),
                    send_sem=sent_sem.at[5], recv_sem=slab_sem.at[c],
                    device_id=(grp, next_in * 2 + core), device_id_type=MESH,
                ).start()
    elif whole_end:
        @pl.when(is_end)
        def _():
            pltpu.make_async_remote_copy(
                src_ref=piece_of(me, 1 - mine), dst_ref=piece_of(me, 1 - mine),
                send_sem=sent_sem.at[5], recv_sem=other_sem.at[chip],
                device_id=(grp, next_in * 2 + core), device_id_type=MESH,
            ).start()

    for h in range(rows // span):
        across_gp(me, h).start()


    def gp_arrives(k):
        o = near(2 * k)
        climb_gp(o).wait_recv()

        @pl.when((o < me) & (chip < last - assisted))
        def _():
            climb_gp(o).start()

        @pl.when((o > me) & (chip > 0 + assisted))
        def _():
            descend_gp(o).start()

        if whole_end:
            @pl.when(jnp.logical_not(beside_end(o)))
            def _():
                exchange_gp(o).start()
        elif square:
            exchange_gp(o).start()
        across_gp(o, mine).start()

    def gp_completes(k):
        if square:
            o = near(2 * k)
            pltpu.make_async_remote_copy(
                src_ref=piece_of(o, 1 - mine), dst_ref=piece_of(o, 1 - mine),
                send_sem=sent_sem.at[8], recv_sem=other_sem.at[o // 2],
                device_id=(other, me), device_id_type=MESH,
            ).wait_recv()
            across_gp(o, 1 - mine).start()

    def gp_crossed(o):
        drain(gp_full.at[o], across_sem.at[o // 2])

    def weigh(o):
        chunk = width // n
        if chunk % 16 == 0:
            product = jnp.dot(
                msg_all[o].reshape(relations * chunk, rows), gp_full[o], preferred_element_type=F32
            )
            grad_w[...] = grad_w[...] + product.reshape(relations, chunk, width)
        else:
            for r in range(relations):
                grad_w[r] = grad_w[r] + jnp.dot(msg_all[o, r], gp_full[o], preferred_element_type=F32)

    def weigh_end(o):
        for r in range(relations):
            end_sum[r] = end_sum[r] + jnp.dot(msg_end[o, r], gp_full[o], preferred_element_type=F32)

    grad_w[...] = jnp.zeros(grad_w.shape, F32)
    end_sum[...] = jnp.zeros(end_sum.shape, F32)
    help_end = pltpu.make_async_remote_copy(
        src_ref=end_send, dst_ref=end_recv,
        send_sem=sent_sem.at[11], recv_sem=help_sem,
        device_id=(grp, helped * 2 + core), device_id_type=MESH,
    )

    @pl.loop(0, width // tile_width)
    def _(c):
        at = aligned(c * tile_width, tile_width, tile_width)
        for r in range(relations):
            rows_r = slice(r * rows, (r + 1) * rows)
            grads = lax.dot_general(
                gp_full[me], weights[r, at, :],
                (((1,), (1,)), ((), ())), preferred_element_type=F32,
            )
            gm[rows_r, at] = (grads * scale[rows_r, 0:1]).astype(BF16)

    lower, higher = slice(0, cut), slice(cut, width)

    def far(j):
        return near(n - j + 2 * lax.rem(j, 2))

    def reduce_part(o, i):
        if square:
            source = part.at[o, :, 1 - column, :, lower] if i == 1 else part.at[o, 1 - row, :, :, higher]
            target, peer = part_recv.at[o, i - 1], (beside, above)[i - 1]
        else:
            source, target, peer = part.at[o, rel(i)], part_recv.at[i, o], rel(i)
        return pltpu.make_async_remote_copy(
            src_ref=source, dst_ref=target,
            send_sem=sent_sem.at[6], recv_sem=d_recv.at[o],
            device_id=(peer, me), device_id_type=MESH,
        )

    def relay_part(o, w):
        return pltpu.make_async_remote_copy(
            src_ref=relay.at[o, w], dst_ref=relay_recv.at[o, w],
            send_sem=sent_sem.at[10], recv_sem=r_recv.at[o],
            device_id=((above, beside)[w], me), device_id_type=MESH,
        )

    def start_parts(z):
        product = jnp.dot(
            adj_t[aligned(z * 2 * blk, 2 * blk, blk), :], gm[...], preferred_element_type=F32
        )
        for v in range(2):
            o = z * 2 + v
            part[o] = product[v * blk : (v + 1) * blk].astype(BF16).reshape(part.shape[1:])
            for i in range(1, 3 if square else groups):
                reduce_part(o, i).start()

    @pl.loop(1, chips)
    def _(e):
        start_parts(near(n - 2 * e) // 2)

    far_chips = chips - 2
    is_inner = (chip == 1) | (chip == last - 1)
    low_side = chip <= 1

    def crosses(o, source):
        return ((source <= 1) & (o // 2 >= 2)) | ((source >= last - 1) & (o // 2 <= last - 2))

    def hand(o, device, landing, semaphore):
        return pltpu.make_async_remote_copy(
            src_ref=part_sum.at[o], dst_ref=landing,
            send_sem=sent_sem.at[7], recv_sem=semaphore,
            device_id=(grp, device), device_id_type=MESH,
        )

    def give_back(j):
        o = far(j)
        if not assisted:
            hand(o, o, part_back.at[me], back_sem).start()
            return
        slot = jnp.where(low_side, jnp.maximum(o // 2 - 2, 0), jnp.minimum(o // 2, far_chips - 1))
        odd = lax.rem(o, 2)
        over = crosses(o, chip)

        @pl.when(over & is_end)
        def _():
            hand(o, next_in * 2 + odd, inbox.at[slot, core], inbox_sem.at[slot]).start()

        @pl.when(over & is_inner & (odd != core))
        def _():
            hand(o, partner, crossed.at[slot], crossed_sem.at[slot]).start()

        @pl.when(jnp.logical_not(over & (is_end | is_inner)))
        def _():
            hand(o, o, part_back.at[me], back_sem).start()

    def collect(slot):
        z = jnp.where(low_side, slot + 2, slot)
        side = jnp.where(low_side, 0, 1)
        return pltpu.make_async_remote_copy(
            src_ref=gathered_sum.at[slot], dst_ref=collected.at[side],
            send_sem=sent_sem.at[12], recv_sem=collect_sem.at[side],
            device_id=(grp, z * 2 + core), device_id_type=MESH,
        )

    def sum_for_far_side(first=0, past=far_chips):
        outer = jnp.where(low_side, 0, last)

        @pl.loop(first, past)
        def _(i):
            slot = jnp.where(low_side, far_chips - 1 - i, i)
            drain(crossed.at[slot], crossed_sem.at[slot])
            drain(inbox.at[slot], inbox_sem.at[slot])
            o = jnp.where(low_side, slot + 2, slot) * 2 + core
            terms = (
                (me, part_sum[o].astype(F32)),
                (partner, crossed[slot].astype(F32)),
                (outer * 2, inbox[slot, 0].astype(F32)),
                (outer * 2 + 1, inbox[slot, 1].astype(F32)),
            )
            for k in range(sections):
                total = None
                for t, term in terms:
                    kept = term * is_one(table[t, o] == k)
                    total = kept if total is None else total + kept
                gathered_sum[slot, k] = total.astype(BF16)
            collect(slot).start()

    def relayed(o):
        if square:
            drain(part_recv.at[o], d_recv.at[o])
            up = part[o, 1 - row, column, :, lower].astype(F32) + part_recv[o, 0, 1 - row].astype(F32)
            relay[o, 0] = up.astype(BF16)
            relay_part(o, 0).start()
            aside = part[o, row, 1 - column, :, higher].astype(F32) + part_recv[o, 1, 1 - column].astype(F32)
            relay[o, 1] = aside.astype(BF16)
            relay_part(o, 1).start()

    def reduced(o):
        if square:
            drain(relay_recv.at[o], r_recv.at[o])
            first = part[o, row, column, :, lower].astype(F32) + part_recv[o, 0, row].astype(F32)
            second = part[o, row, column, :, higher].astype(F32) + part_recv[o, 1, column].astype(F32)
            first = first + relay_recv[o, 0].astype(F32)
            second = second + relay_recv[o, 1].astype(F32)
            return jnp.concatenate([first, second], axis=1).astype(BF16)
        total = part[o, grp].astype(F32)
        drain(part_recv.at[1:groups, o], d_recv.at[o])
        for i in range(1, groups):
            total = total + part_recv[i, o].astype(F32)
        return total.astype(BF16)

    def send_reduced(j):
        part_sum[far(j)] = reduced(far(j))
        give_back(j)

    relays = both > 0
    weigh(me)

    def slab_arrives(c):
        drain(slab(outer_chip * 2 + core, c), slab_sem.at[c])
        outer = outer_chip * 2 + core
        across_slab(outer, c).start()
        ahead = gp_full.at[outer, aligned(mine * span, span, span), columns(c)]
        pltpu.make_async_remote_copy(
            src_ref=ahead, dst_ref=ahead,
            send_sem=sent_sem.at[5], recv_sem=line_sem.at[outer_chip],
            device_id=(grp, jnp.where(chip == 1, 2, last - 2) * 2 + core), device_id_type=MESH,
        ).start()

    def help_slab(c):
        other = outer_chip * 2 + 1 - core
        drain(slab(other, c), cross_slab_sem.at[c])
        for r in range(relations):
            total = None
            for o in (me, partner, outer_chip * 2 + core, other):
                product = jnp.dot(msg_end[o, r], gp_full[o, :, c * cut : (c + 1) * cut], preferred_element_type=F32)
                total = product if total is None else total + product
            end_send[r, :, c * cut : (c + 1) * cut] = total.astype(BF16)
        pltpu.make_async_remote_copy(
            src_ref=end_send.at[:, :, columns(c)], dst_ref=end_recv.at[:, :, columns(c)],
            send_sem=sent_sem.at[11], recv_sem=help_sem,
            device_id=(grp, helped * 2 + core), device_id_type=MESH,
        ).start()

    if sliced:
        @pl.when(is_end)
        def _():
            gp_arrives(1)
            relayed(far(2))
            relayed(far(3))
            start_next_messages()
            relayed(far(4))
            relayed(far(5))

        @pl.when(jnp.logical_not(is_end))
        def _():
            gp_arrives(3 - outward)
            slab_arrives(0)
            relayed(far(2))
            relayed(far(3))
            gp_crossed(partner)
            drain(msg_end.at[: 2 * (chips - 2) - 1], end_sem)
            help_slab(0)
            slab_arrives(1)
            relayed(far(4))
            relayed(far(5))
            help_slab(1)
    else:
        gp_arrives(1)

        @pl.when(relays)
        def _():
            gp_arrives(2)

        @pl.loop(2, n - 2)
        def _(j):
            relayed(far(j))

    start_parts(chip)

    sides = jnp.where(helped == 0, last - chip, chip)

    def beyond(i):
        return jnp.where(helped == 0, chip + 1, chip - 1 - (sides - 1)) + i

    def complete(k):
        gp_completes(k)
        gp_crossed(near(2 * k + 1))

    if assisted and soon and not sliced:
        @pl.when(is_agent)
        def _():
            complete(outward)
            gp_crossed(partner)

    def help_out():
        drain(msg_end.at[: 2 * (chips - 2) - 1], end_sem)
        weigh_end(me)
        weigh_end(partner)

        @pl.loop(0, sides)
        def _(i):
            weigh_end(beyond(i) * 2)
            weigh_end(beyond(i) * 2 + 1)

        end_send[...] = end_sum[...].astype(BF16)
        help_end.start()

    if assisted and soon and not sliced:
        pl.when(is_agent)(help_out)

    if not sliced:
        pl.when(is_end)(start_next_messages)
    if not assisted:
        @pl.when(jnp.logical_not(relays))
        def _():
            gp_arrives(2)

    relayed(far(n - 2))
    relayed(far(n - 1))

    if not sliced:
        @pl.when(relays)
        def _():
            @pl.loop(3, chips)
            def _(k):
                gp_arrives(k)


    @pl.loop(2, n - 2)
    def _(j):
        send_reduced(j)

    relayed(partner)
    relayed(me)
    send_reduced(n - 2)
    send_reduced(n - 1)

    if sliced:
        @pl.when(relays)
        def _():
            sum_for_far_side(0, 1)
            gp_arrives(3)

    if not assisted:
        @pl.when(jnp.logical_not(relays))
        def _():
            @pl.loop(3, chips)
            def _(k):
                gp_arrives(k)

    if assisted:
        pl.when(is_inner)(functools.partial(sum_for_far_side, 1 if sliced else 0))

    if assisted:
        @pl.when(is_end)
        def _():
            drain(msg_all.at[:3], msg_sem)

        @pl.when(jnp.logical_not(is_end))
        def _():
            drain(msg_all.at[: n - 1], msg_sem)
    else:
        drain(msg_all.at[: n - 1], msg_sem)

    if sliced:
        @pl.when(is_end)
        def _():
            gp_completes(1)
            gp_crossed(partner)
            weigh(partner)
            weigh(near(2))

        @pl.when(jnp.logical_not(is_end))
        def _():
            inward = 3 - outward

            @pl.loop(0, 3)
            def _(i):
                weigh(jnp.where(i == 0, partner, near(2 * outward + jnp.maximum(i - 1, 0))))

            gp_completes(inward)
            weigh(near(2 * inward))
            gp_crossed(near(2 * inward + 1))
            weigh(near(2 * inward + 1))
            gp_completes(3)

    part_sum[partner] = reduced(partner)
    give_partner = pltpu.make_async_remote_copy(
        src_ref=part_sum.at[partner], dst_ref=part_back.at[me],
        send_sem=sent_sem.at[7], recv_sem=back_sem,
        device_id=(grp, partner), device_id_type=MESH,
    )
    give_partner.start()
    part_back[me] = reduced(me)

    if sliced:
        @pl.when(is_end)
        def _():
            gp_crossed(near(3))
            weigh(near(3))

        @pl.when(jnp.logical_not(is_end))
        def _():
            weigh(near(6))
            gp_crossed(near(7))
            weigh(near(7))
    else:
        reach = jnp.where(is_end, 2, chips) if assisted else chips
        waited = jnp.where(is_agent, outward, 0) if assisted and soon else 0

        @pl.loop(1, reach)
        def _(k):
            @pl.when(k != waited)
            def _():
                gp_completes(k)

        @pl.loop(1, reach)
        def _(k):
            @pl.when(k != waited)
            def _():
                gp_crossed(near(2 * k + 1))

        if assisted and soon:
            @pl.when(is_end)
            def _():
                gp_crossed(partner)
        else:
            gp_crossed(partner)

        weigh(partner)

        @pl.loop(1, reach)
        def _(k):
            weigh(near(2 * k))
            weigh(near(2 * k + 1))

        if assisted and not soon:
            pl.when(is_agent)(help_out)

    for k in range(sections):
        grad_f[k] = jnp.zeros((quarter, width), F32)

    if assisted:
        for z in range(chips):
            direct = n - 1 - 4 * (z >= 2) - 4 * (z <= last - 2)

            @pl.when(chip == z)
            def _():
                drain(part_sum.at[:direct], back_sem)
    else:
        drain(part_sum.at[: n - 1], back_sem)

    @pl.loop(0, n)
    def _(t):
        def add():
            wanted = table[t, me]
            addend = part_back[t].astype(F32)
            for k in range(sections):
                grad_f[k] = grad_f[k] + addend * is_one(wanted == k)

        if assisted:
            pl.when(jnp.logical_not(crosses(me, t // 2)))(add)
        else:
            add()

    if assisted:
        for side, has in ((0, chip >= 2), (1, chip <= last - 2)):
            @pl.when(has)
            def _():
                drain(collected.at[side], collect_sem.at[side])
                grad_f[...] = grad_f[...] + collected[side].astype(F32)

        @pl.when(is_end)
        def _():
            drain(end_recv, help_sem)
            grad_w[...] = grad_w[...] + end_recv[...].astype(F32)

    fetch_pair.wait_send()
    for z in range(chips):
        near_by = (z > 0) + (z < chips - 1)
        relayed = 2 * (0 < z < chips - 1)
        far = sum(abs(y - z) > 2 for y in range(chips))

        @pl.when(chip == z)
        def _():
            drain(gathered.at[: near_by + relayed + far + chips - 1], sent_sem.at[0])

    drain(fetched.at[: (n - 2) * (groups - 1) * quarter, :], sent_sem.at[1])
    drain(pre_recv.at[1:groups], sent_sem.at[2])
    drain(pre_recv.at[1:groups], sent_sem.at[3])
    if assisted:
        @pl.when(is_agent)
        def _():
            drain(msg_all.at[: n - 2], sent_sem.at[4])
            drain(end_send, sent_sem.at[11])

        @pl.when(jnp.logical_not(is_agent))
        def _():
            drain(msg_all.at[: n - 1], sent_sem.at[4])
    else:
        drain(msg_all.at[: n - 1], sent_sem.at[4])

    for z in range(chips):
        at_end = z in (0, last)
        climbs = z * (z + 1 <= last - assisted) + (z < last)
        descents = (last - z) * (z - 1 >= 0 + assisted) + (z > 0)
        climbs, descents = (climbs if z < last else 0), (descents if z > 0 else 0)
        if at_end:
            climbs, descents = int(z == 0), int(z == last)
        known = 1 if at_end and assisted else last
        doubled = int(at_end and assisted and square)
        swapped = known - (assisted and z in (1, last - 1))

        @pl.when(chip == z)
        def _():
            if square:
                drain(fetched.at[: (climbs + descents + doubled) * span, :], sent_sem.at[5])
                drain(fetched.at[: swapped * span, :], sent_sem.at[8])
            else:
                drain(gp_full.at[: climbs + descents], sent_sem.at[5])
            drain(gp_full.at[: known + 1], sent_sem.at[9])

    if square:
        drain(part_recv, sent_sem.at[6])
        drain(relay_recv, sent_sem.at[10])
    else:
        drain(part_recv.at[1:groups], sent_sem.at[6])
    if assisted:
        @pl.when(is_inner)
        def _():
            drain(part_sum.at[: n - 1 - far_chips], sent_sem.at[7])
            drain(gathered_sum, sent_sem.at[12])

        @pl.when(jnp.logical_not(is_inner))
        def _():
            drain(part_sum.at[: n - 1], sent_sem.at[7])
    else:
        drain(part_sum.at[: n - 1], sent_sem.at[7])


def hand_over(*refs):
    copies = [pltpu.make_async_copy(refs[k], refs[3 + k], refs[6].at[k]) for k in range(3)]
    for copy in copies:
        copy.start()
    for copy in copies:
        copy.wait()


def per_device(
    n, groups,
    features, weights, bias, cotangent, tile_values, tile_count, tile_slot, source_blocks,
):
    rows, width = features.shape
    relations, _, slot_total, blk = tile_values.shape
    sections = rows // blk
    quarter, share, chunk, chips = blk // groups, width // groups, width // n, n // 2
    half = rows // 2
    square = groups == 4
    grid = (2, 2) if square else (groups,)
    vmem = pl.BlockSpec(memory_space=pltpu.VMEM)
    smem = pl.BlockSpec(memory_space=pltpu.SMEM)
    anywhere = pl.BlockSpec(memory_space=pl.ANY)
    hbm = pl.BlockSpec(memory_space=pltpu.HBM)
    dma = pltpu.SemaphoreType.DMA
    out, grad_w, grad_f = pl.pallas_call(
        functools.partial(kernel, n, groups),
        out_shape=(
            pltpu.VMEM((share, rows), BF16),
            pltpu.VMEM((relations, chunk, width), F32),
            pltpu.VMEM((sections, quarter, width), F32),
        ),
        in_specs=[smem, smem, smem, hbm, hbm, vmem, hbm, hbm],
        out_specs=(vmem, vmem, vmem),
        scratch_shapes=[
            pltpu.VMEM((relations, width, width), BF16),
            pltpu.VMEM((relations, rows * slot_total, blk), jnp.int32),
            pltpu.VMEM((sections, groups, quarter, width), BF16),
            pltpu.VMEM((rows, width), BF16),
            pltpu.VMEM((n, sections, quarter, width), BF16),
            pltpu.VMEM((blk, width), BF16),
            pltpu.VMEM((slot_total, blk, blk), BF16),
            pltpu.VMEM((slot_total, blk, blk), BF16),
            pltpu.VMEM((n * blk, width), BF16),
            pltpu.VMEM((relations * rows, n * blk), BF16),
            pltpu.VMEM((relations * rows, 128), F32),
            pltpu.VMEM((relations, width, rows), F32),
            pltpu.VMEM((relations * rows, width), BF16),
            pltpu.VMEM((n, relations, chunk, rows), BF16),
            pltpu.VMEM((n, relations, chunk, rows), BF16),
            pltpu.VMEM((n, relations, chunk, rows), BF16),
            pltpu.VMEM((relations, chunk, width), F32),
            pltpu.VMEM((relations, chunk, width), BF16),
            pltpu.VMEM((relations, chunk, width), BF16),
            pltpu.VMEM((n * blk, relations * rows), BF16),
            pltpu.VMEM((rows, width), F32),
            pltpu.VMEM((groups, half, 2 * share), BF16),
            pltpu.VMEM((groups, half, 2 * share), BF16),
            pltpu.VMEM((half, 2 * share), F32),
            pltpu.VMEM((half, 2 * share), F32),
            pltpu.VMEM((1, 2 * share), F32),
            pltpu.VMEM((groups, half, 2 * share), BF16),
            pltpu.VMEM((n, rows, width), BF16),
            pltpu.VMEM((relations * rows, width), BF16),
            pltpu.VMEM((n, *grid, quarter, width), BF16),
            pltpu.VMEM((n, 2, 2, quarter, width // 2) if square else (groups, n, quarter, width), BF16),
            pltpu.VMEM((n, 2, quarter, width // 2), BF16),
            pltpu.VMEM((n, 2, quarter, width // 2), BF16),
            pltpu.VMEM((n, quarter, width), BF16),
            pltpu.VMEM((n, quarter, width), BF16),
            pltpu.VMEM((chips - 2, 2, quarter, width), BF16),
            pltpu.VMEM((chips - 2, quarter, width), BF16),
            pltpu.VMEM((chips - 2, sections, quarter, width), BF16),
            pltpu.VMEM((2, sections, quarter, width), BF16),
            dma((4,)), dma((2,)), dma((13,)), dma, dma, dma, dma, dma((chips - 2,)), dma((chips - 2,)), dma((2,)), dma((2,)), dma((2,)),
            dma((n, 2)), dma((n, 2)),
            dma((4,)), dma((4,)), dma((n,)), dma((n,)), dma,
            dma((chips,)), dma((chips,)), dma((chips,)),
        ],
        compiler_params=pltpu.CompilerParams(
            collective_id=0, has_side_effects=True, vmem_limit_bytes=60 << 20
        ),
        name="layer",
    )(
        source_blocks, tile_count, tile_slot,
        features.reshape(sections, groups, quarter, width), cotangent, bias,
        tile_values.reshape(relations, rows * slot_total, blk), weights,
    )
    results = (out, grad_w, grad_f)
    out, grad_w, grad_f = pl.pallas_call(
        hand_over,
        out_shape=tuple(jax.ShapeDtypeStruct(x.shape, x.dtype) for x in results),
        in_specs=[vmem] * 3,
        out_specs=(anywhere,) * 3,
        scratch_shapes=[dma((3,))],
        compiler_params=pltpu.CompilerParams(vmem_limit_bytes=4 << 20),
        name="hand_over",
    )(*results)
    return (out.T, grad_w, grad_f)


def solution(mesh):
    placed = (
        P("tgt", None),
        P("rel", None, None),
        P(),
        P("tgt", None),
        P("rel", "tgt", None, None),
        P("rel", "tgt"),
        P("rel", "tgt", None),
        P(),
    )
    return jax.shard_map(
        functools.partial(per_device, mesh.shape["tgt"], mesh.shape["rel"]),
        mesh=mesh,
        in_specs=placed,
        out_specs=(P("tgt", "rel"), P("rel", "tgt", None), P("tgt", "rel", None)),
        check_vma=False,
    )
```
